8 devices in a mesh: sp: 8 (over z, y, x, core).
Axes of the slice: x: 2, y: 2, z: 1, core: 2. Of those that a mesh axis runs over, the one named last changes fastest.
Arguments:
- hidden_in: bfloat16 [32, 512, 1024], P(None, 'sp')
- grad_out: bfloat16 [32, 512, 1024], P(None, 'sp')
- positions: int32 [32, 512], P(None, 'sp')
- w_q: bfloat16 [1024, 2048], replicated
- w_k: bfloat16 [1024, 1024], replicated
- w_v: bfloat16 [1024, 1024], replicated
- w_o: bfloat16 [2048, 1024], replicated
- g_in: bfloat16 [1024], replicated
- q_norm: bfloat16 [128], replicated
- k_norm: bfloat16 [128], replicated
Outputs:
- output 1: bfloat16 [32, 512, 1024], P(None, 'sp')
- output 2: bfloat16 [32, 512, 1024], P(None, 'sp')
- output 3: float32 [1024, 2048], replicated
- output 4: float32 [1024, 1024], replicated
- output 5: float32 [1024, 1024], replicated
- output 6: float32 [2048, 1024], replicated
- output 7: float32 [1024], replicated
- output 8: float32 [128], replicated
- output 9: float32 [128], replicated
All inputs are finite; a program needn't handle non-finite values.
Results may differ from the reference program's by a relative error of at most 0.0140917.
Values are sent between devices in bfloat16 or wider.
A program may use at most 1 GiB of HBM per device.

```python
import jax
import jax.numpy as jnp
from jax import lax

BATCH = 32
SEQ_LEN = 512
MODEL_DIM = 1024
HEADS = 16
KV_HEADS = 8
HEAD_DIM = 128
EPSILON = 1e-6
ROPE_THETA = 1000000.0
NEG_LARGE = -1e30


def setup_inputs(seed: int = 0) -> dict:
    keys = jax.random.split(jax.random.key(seed), 11)
    act_shape = (BATCH, SEQ_LEN, MODEL_DIM)
    q_width = HEADS * HEAD_DIM
    kv_width = KV_HEADS * HEAD_DIM
    hidden_in = jax.random.normal(keys[0], act_shape, jnp.float32).astype(jnp.bfloat16)
    grad_out = jax.random.normal(keys[1], act_shape, jnp.float32).astype(jnp.bfloat16)
    pos_steps = jax.random.randint(keys[2], (BATCH, SEQ_LEN), 1, 3)
    pos_start = jax.random.randint(keys[3], (BATCH, 1), 0, SEQ_LEN)
    positions = (pos_start + jnp.cumsum(pos_steps, axis=1) - pos_steps[:, :1]).astype(jnp.int32)
    w_q = (jax.random.normal(keys[4], (MODEL_DIM, q_width), jnp.float32) * MODEL_DIM ** -0.5).astype(jnp.bfloat16)
    w_k = (jax.random.normal(keys[5], (MODEL_DIM, kv_width), jnp.float32) * MODEL_DIM ** -0.5).astype(jnp.bfloat16)
    w_v = (jax.random.normal(keys[6], (MODEL_DIM, kv_width), jnp.float32) * MODEL_DIM ** -0.5).astype(jnp.bfloat16)
    w_o = (jax.random.normal(keys[7], (q_width, MODEL_DIM), jnp.float32) * q_width ** -0.5).astype(jnp.bfloat16)
    g_in = (0.5 + jax.random.uniform(keys[8], (MODEL_DIM,), jnp.float32)).astype(jnp.bfloat16)
    q_norm = (1.0 + 2.0 * jax.random.uniform(keys[9], (HEAD_DIM,), jnp.float32)).astype(jnp.bfloat16)
    k_norm = (1.0 + 2.0 * jax.random.uniform(keys[10], (HEAD_DIM,), jnp.float32)).astype(jnp.bfloat16)
    return {'hidden_in': hidden_in, 'grad_out': grad_out, 'positions': positions, 'w_q': w_q, 'w_k': w_k, 'w_v': w_v, 'w_o': w_o, 'g_in': g_in, 'q_norm': q_norm, 'k_norm': k_norm}


def to_bf16(values):
    return values.astype(jnp.bfloat16).astype(jnp.float32)


def rms_scale(values):
    return values * lax.rsqrt(jnp.mean(values * values, axis=-1, keepdims=True) + EPSILON)


def rope_tables(positions):
    exponents = jnp.arange(0, HEAD_DIM, 2).astype(jnp.float32) / HEAD_DIM
    inv_freq = jnp.power(ROPE_THETA, -exponents)
    angles = positions.astype(jnp.float32)[:, :, None] * inv_freq
    return jnp.cos(angles)[:, :, None, :], jnp.sin(angles)[:, :, None, :]


def rotate_half(values, rope_cos, rope_sin):
    half = values.shape[-1] // 2
    first = values[..., :half]
    second = values[..., half:]
    return jnp.concatenate([first * rope_cos - second * rope_sin, second * rope_cos + first * rope_sin], axis=-1)


def head_attention(head_in):
    q_head, k_head, v_head = head_in
    scores = jnp.einsum('bqd,bkd->bqk', q_head, k_head) * HEAD_DIM ** -0.5
    causal = jnp.arange(SEQ_LEN)[:, None] >= jnp.arange(SEQ_LEN)[None, :]
    scores = jnp.where(causal, scores, NEG_LARGE)
    prob_vals = to_bf16(jax.nn.softmax(scores, axis=-1))
    return jnp.einsum('bqk,bkd->bqd', prob_vals, v_head)


def block_forward(x_in, q_weight, k_weight, v_weight, o_weight, in_gain, q_gain, k_gain, rope_cos, rope_sin):
    tokens = BATCH * SEQ_LEN
    hidden = to_bf16(rms_scale(x_in) * in_gain).reshape(tokens, MODEL_DIM)
    q_proj = jnp.dot(hidden, q_weight, preferred_element_type=jnp.float32).reshape(BATCH, SEQ_LEN, HEADS, HEAD_DIM)
    k_proj = jnp.dot(hidden, k_weight, preferred_element_type=jnp.float32).reshape(BATCH, SEQ_LEN, KV_HEADS, HEAD_DIM)
    v_proj = to_bf16(jnp.dot(hidden, v_weight, preferred_element_type=jnp.float32)).reshape(BATCH, SEQ_LEN, KV_HEADS, HEAD_DIM)
    q_rot = to_bf16(rotate_half(rms_scale(q_proj) * q_gain, rope_cos, rope_sin))
    k_rot = to_bf16(rotate_half(rms_scale(k_proj) * k_gain, rope_cos, rope_sin))
    group = HEADS // KV_HEADS
    k_full = jnp.repeat(k_rot, group, axis=2)
    v_full = jnp.repeat(v_proj, group, axis=2)
    per_head = lax.map(jax.checkpoint(head_attention), (jnp.moveaxis(q_rot, 2, 0), jnp.moveaxis(k_full, 2, 0), jnp.moveaxis(v_full, 2, 0)))
    attended = to_bf16(jnp.moveaxis(per_head, 0, 2)).reshape(tokens, HEADS * HEAD_DIM)
    return x_in + jnp.dot(attended, o_weight, preferred_element_type=jnp.float32).reshape(BATCH, SEQ_LEN, MODEL_DIM)


def reference(hidden_in, grad_out, positions, w_q, w_k, w_v, w_o, g_in, q_norm, k_norm):
    rope_cos, rope_sin = rope_tables(positions)

    def forward(x_in, q_weight, k_weight, v_weight, o_weight, in_gain, q_gain, k_gain):
        return block_forward(x_in, q_weight, k_weight, v_weight, o_weight, in_gain, q_gain, k_gain, rope_cos, rope_sin)

    out_f32, pullback = jax.vjp(forward, hidden_in.astype(jnp.float32), w_q.astype(jnp.float32), w_k.astype(jnp.float32), w_v.astype(jnp.float32), w_o.astype(jnp.float32), g_in.astype(jnp.float32), q_norm.astype(jnp.float32), k_norm.astype(jnp.float32))
    grads_all = pullback(grad_out.astype(jnp.float32))
    return (out_f32.astype(jnp.bfloat16), grads_all[0].astype(jnp.bfloat16), grads_all[1], grads_all[2], grads_all[3], grads_all[4], grads_all[5], grads_all[6], grads_all[7])
```

```python
import functools
import jax
import jax.numpy as jnp
from jax import lax
from jax.experimental import pallas as pl
from jax.experimental.pallas import tpu as pltpu
from jax.sharding import PartitionSpec as P

EPSILON = 1e-6
ROPE_THETA = 1000000.0
NEG_LARGE = -1e30
NT = (((1,), (1,)), ((), ()))
TN = (((0,), (0,)), ((), ()))
ROW_BLOCK = 256


def dot(a, b, dims=(((1,), (0,)), ((), ()))):
    return lax.dot_general(a, b, dims, preferred_element_type=jnp.float32)


def rope_tables(positions, head_dim):
    exponents = jnp.arange(0, head_dim, 2).astype(jnp.float32) / head_dim
    inv_freq = jnp.power(ROPE_THETA, -exponents)
    angles = positions.astype(jnp.float32)[:, :, None] * inv_freq
    cos, sin = jnp.cos(angles), jnp.sin(angles)
    return jnp.concatenate([cos, cos], axis=-1), jnp.concatenate([-sin, sin], axis=-1)


def block_kernel(x_ref, dy_ref, cos_ref, sin_ref, gin_ref, qn_ref, kn_ref, wq_ref, wk_ref, wv_ref, wo_ref,
                 out_ref, gi_ref, h_ref, o_ref, dq_ref, dk_ref, dv_ref, dgin_ref, dqn_ref, dkn_ref,
                 out_acc, dh_acc):
    seq, group = pl.program_id(0), pl.program_id(1)
    groups = pl.num_programs(1)
    head_dim = qn_ref.shape[1]
    per_kv = wq_ref.shape[1] // head_dim
    seq_len = x_ref.shape[1]
    scale = head_dim ** -0.5
    half = head_dim // 2

    @pl.when((seq == 0) & (group == 0))
    def _():
        dgin_ref[...] = jnp.zeros_like(dgin_ref)
        dqn_ref[...] = jnp.zeros_like(dqn_ref)
        dkn_ref[...] = jnp.zeros_like(dkn_ref)

    @pl.when(group == 0)
    def _():
        x = x_ref[0].astype(jnp.float32)
        inv = lax.rsqrt(jnp.mean(x * x, axis=-1, keepdims=True) + EPSILON)
        h_ref[0] = (x * inv * gin_ref[...]).astype(jnp.bfloat16)
        out_acc[...] = jnp.zeros_like(out_acc)
        dh_acc[...] = jnp.zeros_like(dh_acc)

    cos, sin = cos_ref[0], sin_ref[0]

    def norm_rotate(t, gain):
        inv = lax.rsqrt(jnp.mean(t * t, axis=-1, keepdims=True) + EPSILON)
        unit = t * inv
        scaled = unit * gain
        return (scaled * cos + pltpu.roll(scaled, half, 1) * sin).astype(jnp.bfloat16), unit, inv

    def norm_rotate_back(grad, unit, inv, gain):
        d_scaled = grad * cos - pltpu.roll(grad, half, 1) * sin
        d_gain = jnp.sum(d_scaled * unit, axis=0, keepdims=True)
        d_unit = d_scaled * gain
        return inv * (d_unit - unit * jnp.mean(d_unit * unit, axis=-1, keepdims=True)), d_gain

    h = h_ref[0]
    dy = dy_ref[0]
    q_proj = dot(h, wq_ref[...])
    k_proj = dot(h, wk_ref[...])
    v = dot(h, wv_ref[...]).astype(jnp.bfloat16)
    d_o = dot(dy, wo_ref[...], NT).astype(jnp.bfloat16)
    k_rot, k_unit, k_inv = norm_rotate(k_proj, kn_ref[...])

    blocks = seq_len // ROW_BLOCK
    dk_parts = [None] * blocks
    dv_parts = [None] * blocks
    rows_id = lax.broadcasted_iota(jnp.int32, (ROW_BLOCK, ROW_BLOCK), 0)
    cols_id = lax.broadcasted_iota(jnp.int32, (ROW_BLOCK, ROW_BLOCK), 1)
    causal = rows_id >= cols_id
    dqn_sum = None
    for head in range(per_kv):
        lanes = slice(head * head_dim, (head + 1) * head_dim)
        q_rot, q_unit, q_inv = norm_rotate(q_proj[:, lanes], qn_ref[...])
        do_head = d_o[:, lanes]
        dq_rows = []
        o_rows = []
        for i in range(blocks):
            rows = slice(i * ROW_BLOCK, (i + 1) * ROW_BLOCK)
            q_i, do_i = q_rot[rows], do_head[rows]
            s_parts = []
            for j in range(i + 1):
                s = dot(q_i, k_rot[j * ROW_BLOCK:(j + 1) * ROW_BLOCK], NT)
                if j == i:
                    s = jnp.where(causal, s, NEG_LARGE)
                s_parts.append(s)
            top = functools.reduce(jnp.maximum, [jnp.max(s, axis=-1, keepdims=True) for s in s_parts])
            e_parts = [jnp.exp((s - top) * scale) for s in s_parts]
            total = functools.reduce(jnp.add, [jnp.sum(e, axis=-1, keepdims=True) for e in e_parts])
            recip = 1.0 / total
            p_parts = [e * recip for e in e_parts]
            pb_parts = [p.astype(jnp.bfloat16) for p in p_parts]
            o_i = None
            for j in range(i + 1):
                part = dot(pb_parts[j], v[j * ROW_BLOCK:(j + 1) * ROW_BLOCK])
                o_i = part if o_i is None else o_i + part
            o_rows.append(o_i.astype(jnp.bfloat16))
            dp_parts = [dot(do_i, v[j * ROW_BLOCK:(j + 1) * ROW_BLOCK], NT) for j in range(i + 1)]
            delta = functools.reduce(jnp.add, [jnp.sum(p * dp, axis=-1, keepdims=True) for p, dp in zip(p_parts, dp_parts)])
            ds_parts = [(p * (dp - delta)).astype(jnp.bfloat16) for p, dp in zip(p_parts, dp_parts)]
            dq_i = None
            for j in range(i + 1):
                cols = slice(j * ROW_BLOCK, (j + 1) * ROW_BLOCK)
                part = dot(ds_parts[j], k_rot[cols])
                dq_i = part if dq_i is None else dq_i + part
                dk_j = dot(ds_parts[j], q_i, TN)
                dv_j = dot(pb_parts[j], do_i, TN)
                dk_parts[j] = dk_j if dk_parts[j] is None else dk_parts[j] + dk_j
                dv_parts[j] = dv_j if dv_parts[j] is None else dv_parts[j] + dv_j
            dq_rows.append(dq_i)
        o_ref[0, :, lanes] = jnp.concatenate(o_rows, axis=0)
        dq_head, d_gain = norm_rotate_back(jnp.concatenate(dq_rows, axis=0) * scale, q_unit, q_inv, qn_ref[...])
        dqn_sum = d_gain if dqn_sum is None else dqn_sum + d_gain
        dq_ref[0, :, lanes] = dq_head.astype(jnp.bfloat16)
    dqn_ref[...] += dqn_sum
    dk_head, d_gain = norm_rotate_back(jnp.concatenate(dk_parts, axis=0) * scale, k_unit, k_inv, kn_ref[...])
    dkn_ref[...] += d_gain
    dk_ref[0] = dk_head.astype(jnp.bfloat16)
    dv_ref[0] = jnp.concatenate(dv_parts, axis=0).astype(jnp.bfloat16)
    out_acc[...] += dot(o_ref[0], wo_ref[...])
    dh_acc[...] += dot(dq_ref[0], wq_ref[...], NT) + dot(dk_ref[0], wk_ref[...], NT) + dot(dv_ref[0], wv_ref[...], NT)

    @pl.when(group == groups - 1)
    def _():
        x = x_ref[0].astype(jnp.float32)
        out_ref[0] = (x + out_acc[...]).astype(jnp.bfloat16)
        inv = lax.rsqrt(jnp.mean(x * x, axis=-1, keepdims=True) + EPSILON)
        unit = x * inv
        d_norm = dh_acc[...]
        dgin_ref[...] += jnp.sum(d_norm * unit, axis=0, keepdims=True)
        d_unit = d_norm * gin_ref[...]
        grad = inv * (d_unit - unit * jnp.mean(d_unit * unit, axis=-1, keepdims=True))
        gi_ref[0] = (dy_ref[0].astype(jnp.float32) + grad).astype(jnp.bfloat16)


def block_call(x, dy, cos, sin, g_in, q_norm, k_norm, w_q, w_k, w_v, w_o):
    seqs, seq_len, model = x.shape
    head_dim = q_norm.shape[1]
    q_width, kv_width = w_q.shape[1], w_k.shape[1]
    groups = kv_width // head_dim
    q_cols = q_width // groups
    tokens = seqs * seq_len
    row = lambda s, g: (s, 0, 0)
    col = lambda s, g: (s, 0, g)
    fixed = lambda s, g: (0, 0)
    wcol = lambda s, g: (0, g)
    bf = lambda *shape: jax.ShapeDtypeStruct(shape, jnp.bfloat16)
    f32 = lambda *shape: jax.ShapeDtypeStruct(shape, jnp.float32)
    flops = 4 * tokens * model * (q_width * 2 + kv_width * 2) + 12 * tokens * seq_len * q_width
    return pl.pallas_call(
        block_kernel,
        grid=(seqs, groups),
        in_specs=[
            pl.BlockSpec((1, seq_len, model), row),
            pl.BlockSpec((1, seq_len, model), row),
            pl.BlockSpec((1, seq_len, head_dim), row),
            pl.BlockSpec((1, seq_len, head_dim), row),
            pl.BlockSpec((1, model), fixed),
            pl.BlockSpec((1, head_dim), fixed),
            pl.BlockSpec((1, head_dim), fixed),
            pl.BlockSpec((model, q_cols), wcol),
            pl.BlockSpec((model, head_dim), wcol),
            pl.BlockSpec((model, head_dim), wcol),
            pl.BlockSpec((q_cols, model), lambda s, g: (g, 0)),
        ],
        out_specs=[
            pl.BlockSpec((1, seq_len, model), row),
            pl.BlockSpec((1, seq_len, model), row),
            pl.BlockSpec((1, seq_len, model), row),
            pl.BlockSpec((1, seq_len, q_cols), col),
            pl.BlockSpec((1, seq_len, q_cols), col),
            pl.BlockSpec((1, seq_len, head_dim), col),
            pl.BlockSpec((1, seq_len, head_dim), col),
            pl.BlockSpec((1, model), fixed),
            pl.BlockSpec((1, head_dim), fixed),
            pl.BlockSpec((1, head_dim), fixed),
        ],
        out_shape=[
            bf(seqs, seq_len, model), bf(seqs, seq_len, model), bf(seqs, seq_len, model),
            bf(seqs, seq_len, q_width), bf(seqs, seq_len, q_width),
            bf(seqs, seq_len, kv_width), bf(seqs, seq_len, kv_width),
            f32(1, model), f32(1, head_dim), f32(1, head_dim),
        ],
        scratch_shapes=[pltpu.VMEM((seq_len, model), jnp.float32), pltpu.VMEM((seq_len, model), jnp.float32)],
        compiler_params=pltpu.CompilerParams(
            dimension_semantics=("arbitrary", "arbitrary"), vmem_limit_bytes=60 * 1024 * 1024),
        cost_estimate=pl.CostEstimate(flops=flops, bytes_accessed=50_000_000, transcendentals=tokens * seq_len * 8),
        name="block",
    )(x, dy, cos, sin, g_in, q_norm, k_norm, w_q, w_k, w_v, w_o)


def reduce_grad(part, c, x, y):
    bit = {1: c, 2: x, 4: y}

    def swap(values, axis_bit):
        return lax.ppermute(values, 'sp', [(d, d ^ axis_bit) for d in range(8)])

    def split(values, axis_bit):
        n = values.shape[0] // 2
        b = bit[axis_bit]
        mine = lax.dynamic_slice_in_dim(values, b * n, n, 0)
        other = lax.dynamic_slice_in_dim(values, (1 - b) * n, n, 0)
        got = swap(other.astype(jnp.bfloat16), axis_bit)
        return mine + got.astype(jnp.float32)

    def join(values, axis_bit):
        got = swap(values, axis_bit)
        b = bit[axis_bit]
        return jnp.where(b == 0, jnp.concatenate([values, got], 0), jnp.concatenate([got, values], 0))

    half = split(part, 1)
    n = half.shape[0] // 2
    xy = split(split(half[:n], 2), 4).astype(jnp.bfloat16)
    yx = split(split(half[n:], 4), 2).astype(jnp.bfloat16)
    full = jnp.concatenate([join(join(xy, 4), 2), join(join(yx, 2), 4)], 0)
    return join(full, 1).astype(jnp.float32)


def solution(mesh):
    group_size = mesh.shape['sp']
    seq_spec = P(None, 'sp', None)
    replicated = P()

    def shard_body(hidden_in, grad_out, positions, w_q, w_k, w_v, w_o, g_in, q_norm, k_norm):
        batch, seq_dev, model_dim = hidden_in.shape
        head_dim = q_norm.shape[0]
        per_dev = batch // group_size
        seq_len = seq_dev * group_size
        me = lax.axis_index('sp')
        c, xi, yi = me % 2, (me // 2) % 2, me // 4

        pos = lax.all_to_all(positions.reshape(per_dev, group_size, seq_dev), 'sp', 1, 1, tiled=True).reshape(per_dev, seq_len)
        cos, sin = rope_tables(pos, head_dim)
        gains = (g_in.astype(jnp.float32)[None], q_norm.astype(jnp.float32)[None], k_norm.astype(jnp.float32)[None])

        def to_batch(values, j):
            piece = values[j * group_size:(j + 1) * group_size]
            return lax.all_to_all(piece, 'sp', 0, 0, tiled=True).reshape(1, seq_len, model_dim)

        def to_seq(values):
            return lax.all_to_all(values.reshape(group_size, seq_dev, model_dim), 'sp', 0, 0, tiled=True)

        outs = []
        for j in range(per_dev):
            xj, dyj = to_batch(hidden_in, j), to_batch(grad_out, j)
            res = block_call(xj, dyj, cos[j:j + 1], sin[j:j + 1], *gains, w_q, w_k, w_v, w_o)
            outs.append((to_seq(res[0]), to_seq(res[1]), dyj) + tuple(res[2:]))
        hidden_out, grad_in = (jnp.concatenate([o[i] for o in outs], axis=0) for i in range(2))
        dy, h, o, dq, dk, dv = (jnp.concatenate([t[i] for t in outs], axis=0).reshape(per_dev * seq_len, -1) for i in range(2, 8))
        small = [sum(t[i] for t in outs)[0] for i in range(8, 11)]
        grad_wo, grad_wq, grad_wk, grad_wv = (reduce_grad(dot(a, b, TN), c, xi, yi) for a, b in ((o, dy), (h, dq), (h, dk), (h, dv)))
        small = lax.psum(tuple(small), 'sp')
        return (hidden_out, grad_in, grad_wq, grad_wk, grad_wv, grad_wo) + tuple(small)

    return jax.shard_map(shard_body, mesh=mesh,
                         in_specs=(seq_spec, seq_spec, P(None, 'sp'), replicated, replicated, replicated, replicated, replicated, replicated, replicated),
                         out_specs=(seq_spec, seq_spec, replicated, replicated, replicated, replicated, replicated, replicated, replicated),
                         check_vma=False)
```

```python
import functools
import jax
import jax.numpy as jnp
from jax import lax
from jax.experimental import pallas as pl
from jax.experimental.pallas import tpu as pltpu
from jax.sharding import PartitionSpec as P

EPSILON = 1e-6
ROPE_THETA = 1000000.0
NEG_LARGE = -1e30
NT = (((1,), (1,)), ((), ()))
TN = (((0,), (0,)), ((), ()))
ROW_BLOCK = 256
DEVICES = 8
BF16 = jnp.bfloat16
F32 = jnp.float32


def dot(a, b, dims=(((1,), (0,)), ((), ()))):
    return lax.dot_general(a, b, dims, preferred_element_type=F32)


def peer_of(me, step):
    core, x, y = me % 2, (me // 2) % 2, me // 4
    return ((y + step // 4) % 2) * 4 + ((x + (step // 2) % 2) % 2) * 2 + (core + step % 2) % 2


def entry_barrier(me):
    barrier = pltpu.get_barrier_semaphore()
    for step in range(1, DEVICES):
        pl.semaphore_signal(barrier, inc=1, device_id=(peer_of(me, step),), device_id_type=pl.DeviceIdType.MESH)
    pl.semaphore_wait(barrier, DEVICES - 1)


def remote(src, dst, send, recv, device):
    return pltpu.make_async_remote_copy(src_ref=src, dst_ref=dst, send_sem=send, recv_sem=recv,
                                        device_id=(device,), device_id_type=pl.DeviceIdType.MESH)


def block_kernel(x_hbm, dy_hbm, pos_hbm, freq_ref, gin_ref, qn_ref, kn_ref, wq_ref, wk_ref, wv_ref, wo_ref,
                 out_hbm, gi_hbm, ht_ref, dyo_ref, o_ref, dq_ref, dk_ref, dv_ref, dgin_ref, dqn_ref, dkn_ref,
                 xb, dyb, gib, posb, h_ref, cos_ref, sin_ref, out_acc, dh_acc, in_send, in_recv, out_send, out_recv):
    seq, group = pl.program_id(0), pl.program_id(1)
    seqs, groups = pl.num_programs(0), pl.num_programs(1)
    me = lax.axis_index('sp')
    head_dim = qn_ref.shape[1]
    per_kv = wq_ref.shape[1] // head_dim
    seq_len = xb.shape[1]
    piece = seq_len // DEVICES
    scale = head_dim ** -0.5
    half = head_dim // 2

    def rows_of(device):
        return pl.ds(pl.multiple_of(device * piece, piece), piece)

    def incoming(kind, s, step, arrival=False):
        peer = peer_of(me, step)
        src = (x_hbm, dy_hbm, pos_hbm)[kind].at[DEVICES * s + peer]

        def landing(device):
            return posb.at[s, device] if kind == 2 else (xb, dyb)[kind].at[s, rows_of(device)]

        if step == 0:
            return pltpu.make_async_copy(src, landing(me), in_recv.at[kind, s, 0])
        return remote(src, landing(peer if arrival else me), in_send.at[kind, s, step], in_recv.at[kind, s, step], peer)

    def outgoing(kind, s, step, arrival=False):
        peer = peer_of(me, step)
        src = (xb, gib)[kind].at[s, rows_of(peer)]
        dst = (out_hbm, gi_hbm)[kind]
        if step == 0:
            return pltpu.make_async_copy(src, dst.at[DEVICES * s + me], out_recv.at[kind, s, 0])
        return remote(src, dst.at[DEVICES * s + (peer if arrival else me)],
                      out_send.at[kind, s, step], out_recv.at[kind, s, step], peer)

    @pl.when((seq == 0) & (group == 0))
    def _():
        entry_barrier(me)

        def send_all(s, carry):
            for kind in (2, 0, 1):
                for step in (2, 4, 6, 3, 5, 7, 1, 0):
                    incoming(kind, s, step).start()
            return carry

        lax.fori_loop(0, seqs, send_all, 0)
        dgin_ref[...] = jnp.zeros_like(dgin_ref)
        dqn_ref[...] = jnp.zeros_like(dqn_ref)
        dkn_ref[...] = jnp.zeros_like(dkn_ref)

    @pl.when(group == 0)
    def _():
        for kind in (2, 0, 1):
            for step in range(DEVICES):
                arrived = incoming(kind, seq, step, arrival=True)
                if step == 0:
                    arrived.wait()
                else:
                    arrived.wait_recv()
        x = xb[seq].astype(F32)
        inv = lax.rsqrt(jnp.mean(x * x, axis=-1, keepdims=True) + EPSILON)
        h = (x * inv * gin_ref[...]).astype(BF16)
        h_ref[...] = h
        ht_ref[...] = h.T
        dyo_ref[0] = dyb[seq]
        out_acc[...] = jnp.zeros_like(out_acc)
        dh_acc[...] = jnp.zeros_like(dh_acc)
        on_diag = lax.broadcasted_iota(jnp.int32, (piece, head_dim), 0) == lax.broadcasted_iota(jnp.int32, (piece, head_dim), 1)
        low = lax.broadcasted_iota(jnp.int32, (piece, head_dim), 1) < half
        for device in range(DEVICES):
            row = jnp.broadcast_to(posb[seq, device, 0:1, :], (piece, head_dim))
            column = jnp.sum(jnp.where(on_diag, row, 0.0), axis=-1, keepdims=True)
            angles = column * freq_ref[...]
            sin = jnp.sin(angles)
            cos_ref[device * piece:(device + 1) * piece, :] = jnp.cos(angles)
            sin_ref[device * piece:(device + 1) * piece, :] = jnp.where(low, -sin, sin)

    cos, sin = cos_ref[...], sin_ref[...]

    def norm_rotate(t, gain):
        inv = lax.rsqrt(jnp.mean(t * t, axis=-1, keepdims=True) + EPSILON)
        unit = t * inv
        scaled = unit * gain
        return (scaled * cos + pltpu.roll(scaled, half, 1) * sin).astype(BF16), unit, inv

    def norm_rotate_back(grad, unit, inv, gain):
        d_scaled = grad * cos - pltpu.roll(grad, half, 1) * sin
        d_gain = jnp.sum(d_scaled * unit, axis=0, keepdims=True)
        d_unit = d_scaled * gain
        return inv * (d_unit - unit * jnp.mean(d_unit * unit, axis=-1, keepdims=True)), d_gain

    h = h_ref[...]
    q_proj = dot(h, wq_ref[...])
    k_proj = dot(h, wk_ref[...])
    v = dot(h, wv_ref[...]).astype(BF16)
    d_o = dot(dyb[seq], wo_ref[...], NT).astype(BF16)
    k_rot, k_unit, k_inv = norm_rotate(k_proj, kn_ref[...])

    blocks = seq_len // ROW_BLOCK
    dk_parts = [None] * blocks
    dv_parts = [None] * blocks
    rows_id = lax.broadcasted_iota(jnp.int32, (ROW_BLOCK, ROW_BLOCK), 0)
    cols_id = lax.broadcasted_iota(jnp.int32, (ROW_BLOCK, ROW_BLOCK), 1)
    causal = rows_id >= cols_id
    dqn_sum = None
    for head in range(per_kv):
        lanes = slice(head * head_dim, (head + 1) * head_dim)
        q_rot, q_unit, q_inv = norm_rotate(q_proj[:, lanes], qn_ref[...])
        do_head = d_o[:, lanes]
        dq_rows = []
        o_rows = []
        for i in range(blocks):
            rows = slice(i * ROW_BLOCK, (i + 1) * ROW_BLOCK)
            q_i, do_i = q_rot[rows], do_head[rows]
            s_parts = []
            for j in range(i + 1):
                s = dot(q_i, k_rot[j * ROW_BLOCK:(j + 1) * ROW_BLOCK], NT)
                if j == i:
                    s = jnp.where(causal, s, NEG_LARGE)
                s_parts.append(s)
            top = functools.reduce(jnp.maximum, [jnp.max(s, axis=-1, keepdims=True) for s in s_parts])
            e_parts = [jnp.exp((s - top) * scale) for s in s_parts]
            total = functools.reduce(jnp.add, [jnp.sum(e, axis=-1, keepdims=True) for e in e_parts])
            recip = 1.0 / total
            p_parts = [e * recip for e in e_parts]
            pb_parts = [p.astype(BF16) for p in p_parts]
            o_i = None
            for j in range(i + 1):
                part = dot(pb_parts[j], v[j * ROW_BLOCK:(j + 1) * ROW_BLOCK])
                o_i = part if o_i is None else o_i + part
            o_rows.append(o_i.astype(BF16))
            dp_parts = [dot(do_i, v[j * ROW_BLOCK:(j + 1) * ROW_BLOCK], NT) for j in range(i + 1)]
            delta = functools.reduce(jnp.add, [jnp.sum(p * dp, axis=-1, keepdims=True) for p, dp in zip(p_parts, dp_parts)])
            ds_parts = [(p * (dp - delta)).astype(BF16) for p, dp in zip(p_parts, dp_parts)]
            dq_i = None
            for j in range(i + 1):
                cols = slice(j * ROW_BLOCK, (j + 1) * ROW_BLOCK)
                part = dot(ds_parts[j], k_rot[cols])
                dq_i = part if dq_i is None else dq_i + part
                dk_j = dot(ds_parts[j], q_i, TN)
                dv_j = dot(pb_parts[j], do_i, TN)
                dk_parts[j] = dk_j if dk_parts[j] is None else dk_parts[j] + dk_j
                dv_parts[j] = dv_j if dv_parts[j] is None else dv_parts[j] + dv_j
            dq_rows.append(dq_i)
        o_ref[0, :, lanes] = jnp.concatenate(o_rows, axis=0)
        dq_head, d_gain = norm_rotate_back(jnp.concatenate(dq_rows, axis=0) * scale, q_unit, q_inv, qn_ref[...])
        dqn_sum = d_gain if dqn_sum is None else dqn_sum + d_gain
        dq_ref[0, :, lanes] = dq_head.astype(BF16)
    dqn_ref[...] += dqn_sum
    dk_head, d_gain = norm_rotate_back(jnp.concatenate(dk_parts, axis=0) * scale, k_unit, k_inv, kn_ref[...])
    dkn_ref[...] += d_gain
    dk_ref[0] = dk_head.astype(BF16)
    dv_ref[0] = jnp.concatenate(dv_parts, axis=0).astype(BF16)
    out_acc[...] += dot(o_ref[0], wo_ref[...])
    dh_acc[...] += dot(dq_ref[0], wq_ref[...], NT) + dot(dk_ref[0], wk_ref[...], NT) + dot(dv_ref[0], wv_ref[...], NT)

    @pl.when(group == groups - 1)
    def _():
        x = xb[seq].astype(F32)
        inv = lax.rsqrt(jnp.mean(x * x, axis=-1, keepdims=True) + EPSILON)
        unit = x * inv
        xb[seq] = (x + out_acc[...]).astype(BF16)
        d_norm = dh_acc[...]
        dgin_ref[...] += jnp.sum(d_norm * unit, axis=0, keepdims=True)
        d_unit = d_norm * gin_ref[...]
        grad = inv * (d_unit - unit * jnp.mean(d_unit * unit, axis=-1, keepdims=True))
        gib[seq] = (dyb[seq].astype(F32) + grad).astype(BF16)
        for kind in range(2):
            for step in (2, 4, 6, 3, 5, 7, 1, 0):
                outgoing(kind, seq, step).start()

    @pl.when((seq == seqs - 1) & (group == groups - 1))
    def _():
        def drain(s, carry):
            for step in range(1, DEVICES):
                for kind in range(3):
                    incoming(kind, s, step).wait_send()
            for step in range(DEVICES):
                for kind in range(2):
                    if step == 0:
                        outgoing(kind, s, 0).wait()
                    else:
                        outgoing(kind, s, step).wait_send()
                        outgoing(kind, s, step, arrival=True).wait_recv()
            return carry

        lax.fori_loop(0, seqs, drain, 0)


def block_call(x, dy, pos, freq, g_in, q_norm, k_norm, w_q, w_k, w_v, w_o):
    batch, piece, model = x.shape
    seqs, seq_len = batch // DEVICES, piece * DEVICES
    head_dim = q_norm.shape[1]
    q_width, kv_width = w_q.shape[1], w_k.shape[1]
    groups = kv_width // head_dim
    q_cols = q_width // groups
    tokens = seqs * seq_len
    row = lambda s, g: (s, 0, 0)
    col = lambda s, g: (s, 0, g)
    fixed = lambda s, g: (0, 0)
    wcol = lambda s, g: (0, g)
    bf = lambda *shape: jax.ShapeDtypeStruct(shape, BF16)
    f32 = lambda *shape: jax.ShapeDtypeStruct(shape, F32)
    anywhere = pl.BlockSpec(memory_space=pl.ANY)
    flops = 4 * tokens * model * (q_width * 2 + kv_width * 2) + 12 * tokens * seq_len * q_width
    return pl.pallas_call(
        block_kernel,
        grid=(seqs, groups),
        in_specs=[
            anywhere, anywhere, anywhere,
            pl.BlockSpec((1, head_dim), fixed),
            pl.BlockSpec((1, model), fixed),
            pl.BlockSpec((1, head_dim), fixed),
            pl.BlockSpec((1, head_dim), fixed),
            pl.BlockSpec((model, q_cols), wcol),
            pl.BlockSpec((model, head_dim), wcol),
            pl.BlockSpec((model, head_dim), wcol),
            pl.BlockSpec((q_cols, model), lambda s, g: (g, 0)),
        ],
        out_specs=[
            anywhere, anywhere,
            pl.BlockSpec((model, seq_len), lambda s, g: (0, s)),
            pl.BlockSpec((1, seq_len, model), row),
            pl.BlockSpec((1, seq_len, q_cols), col),
            pl.BlockSpec((1, seq_len, q_cols), col),
            pl.BlockSpec((1, seq_len, head_dim), col),
            pl.BlockSpec((1, seq_len, head_dim), col),
            pl.BlockSpec((1, model), fixed),
            pl.BlockSpec((1, head_dim), fixed),
            pl.BlockSpec((1, head_dim), fixed),
        ],
        out_shape=[
            bf(batch, piece, model), bf(batch, piece, model),
            bf(model, tokens), bf(seqs, seq_len, model),
            bf(seqs, seq_len, q_width), bf(seqs, seq_len, q_width),
            bf(seqs, seq_len, kv_width), bf(seqs, seq_len, kv_width),
            f32(1, model), f32(1, head_dim), f32(1, head_dim),
        ],
        scratch_shapes=[
            pltpu.VMEM((seqs, seq_len, model), BF16),
            pltpu.VMEM((seqs, seq_len, model), BF16),
            pltpu.VMEM((seqs, seq_len, model), BF16),
            pltpu.VMEM((seqs, DEVICES, 8, head_dim), F32),
            pltpu.VMEM((seq_len, model), BF16),
            pltpu.VMEM((seq_len, head_dim), F32),
            pltpu.VMEM((seq_len, head_dim), F32),
            pltpu.VMEM((seq_len, model), F32),
            pltpu.VMEM((seq_len, model), F32),
            pltpu.SemaphoreType.DMA((3, seqs, DEVICES)),
            pltpu.SemaphoreType.DMA((3, seqs, DEVICES)),
            pltpu.SemaphoreType.DMA((2, seqs, DEVICES)),
            pltpu.SemaphoreType.DMA((2, seqs, DEVICES)),
        ],
        compiler_params=pltpu.CompilerParams(
            dimension_semantics=("arbitrary", "arbitrary"), vmem_limit_bytes=62 * 1024 * 1024,
            collective_id=0, has_side_effects=True),
        cost_estimate=pl.CostEstimate(flops=flops, bytes_accessed=50_000_000, transcendentals=tokens * seq_len * 8),
        name="block",
    )(x, dy, pos, freq, g_in, q_norm, k_norm, w_q, w_k, w_v, w_o)


def grads_kernel(ht_ref, dy_ref, small_ref, o_hbm, dq_hbm, dk_hbm, dv_hbm,
                 ga_hbm, gb_hbm, small_out,
                 ob, qkvb, s1a, s1b, l1a, l1b, s2a, s2b, l2a, l2b, acc_a, acc_b, ra, rb, smallb,
                 load_sem, pair_send, pair_recv, chip_send, chip_recv, all_send, all_recv, fwd_send, fwd_recv,
                 small_send, small_recv):
    me = lax.axis_index('sp')
    partner = peer_of(me, 1)
    q_cols, head_dim = ob.shape[2], (qkvb.shape[2] - ob.shape[2]) // 2
    chips = l1a.shape[0]

    def peer_group(order):
        return peer_of(me, (1 - order // 2) * 2 + (((order + 1) // 2) % 2) * 4)

    def loads(group, slot):
        wide = pl.ds(pl.multiple_of(group * q_cols, q_cols), q_cols)
        narrow = pl.ds(pl.multiple_of(group * head_dim, head_dim), head_dim)
        return [
            pltpu.make_async_copy(o_hbm.at[:, wide], ob.at[slot], load_sem.at[slot, 0]),
            pltpu.make_async_copy(dq_hbm.at[:, wide], qkvb.at[slot, :, pl.ds(0, q_cols)], load_sem.at[slot, 1]),
            pltpu.make_async_copy(dk_hbm.at[:, narrow], qkvb.at[slot, :, pl.ds(q_cols, head_dim)], load_sem.at[slot, 2]),
            pltpu.make_async_copy(dv_hbm.at[:, narrow], qkvb.at[slot, :, pl.ds(q_cols + head_dim, head_dim)], load_sem.at[slot, 3]),
        ]

    def start(copies):
        for copy in copies:
            copy.start()

    def pair(order):
        return [remote(s1a.at[order], l1a.at[order], pair_send.at[0, order], pair_recv.at[0, order], partner),
                remote(s1b.at[order], l1b.at[order], pair_send.at[1, order], pair_recv.at[1, order], partner)]

    def chip(order, device):
        return [remote(s2a.at[order], l2a.at[order], chip_send.at[0, order], chip_recv.at[0, order], device),
                remote(s2b.at[order], l2b.at[order], chip_send.at[1, order], chip_recv.at[1, order], device)]

    start(loads(peer_of(peer_group(0), 1), 0))
    entry_barrier(me)
    for step in range(1, DEVICES):
        remote(small_ref, smallb.at[me], small_send.at[step], small_recv.at[step], peer_of(me, step)).start()

    def products(slot):
        return dot(ob[slot], dy_ref[...], TN), dot(ht_ref[...], qkvb[slot])

    def body(order, carry):
        mine = peer_group(order)
        other = peer_of(mine, 1)
        start(loads(mine, 1))
        for copy in loads(other, 0):
            copy.wait()
        prod_a, prod_b = products(0)
        s1a[order] = prod_a.astype(BF16)
        s1b[order] = prod_b.astype(BF16)
        start(pair(order))

        @pl.when(order < chips - 1)
        def _():
            start(loads(peer_of(peer_group(order + 1), 1), 0))

        for copy in loads(mine, 1):
            copy.wait()
        prod_a, prod_b = products(1)
        acc_a[...] = prod_a
        acc_b[...] = prod_b
        for copy in pair(order):
            copy.wait_recv()
        sum_a = acc_a[...] + l1a[order].astype(F32)
        sum_b = acc_b[...] + l1b[order].astype(F32)

        @pl.when(order < chips - 1)
        def _():
            s2a[order] = sum_a.astype(BF16)
            s2b[order] = sum_b.astype(BF16)
            start(chip(order, mine))

        @pl.when(order == chips - 1)
        def _():
            acc_a[...] = sum_a
            acc_b[...] = sum_b
        return carry

    lax.fori_loop(0, chips, body, 0)

    for order in range(chips - 1):
        for copy in chip(order, me):
            copy.wait_recv()
    ra[...] = (acc_a[...] + l2a[0].astype(F32) + l2a[1].astype(F32) + l2a[2].astype(F32)).astype(BF16)
    rb[...] = (acc_b[...] + l2b[0].astype(F32) + l2b[1].astype(F32) + l2b[2].astype(F32)).astype(BF16)

    pairs = ((ra, ga_hbm), (rb, gb_hbm))

    def spread(step, arrival=False):
        peer = peer_of(me, step)
        return [remote(src, dst.at[peer if arrival else me], all_send.at[i, step], all_recv.at[i, step], peer)
                for i, (src, dst) in enumerate(pairs)]

    def forward(step, arrival=False):
        owner, theirs = peer_of(me, step), peer_of(partner, step)
        return [remote(dst.at[owner], dst.at[theirs if arrival else owner], fwd_send.at[i, step], fwd_recv.at[i, step], partner)
                for i, (_, dst) in enumerate(pairs)]

    def wait_send(copies):
        for copy in copies:
            copy.wait_send()

    def wait_recv(copies):
        for copy in copies:
            copy.wait_recv()

    local = [pltpu.make_async_copy(src, dst.at[me], all_recv.at[i, 0]) for i, (src, dst) in enumerate(pairs)]
    for step in (2, 4, 6, 1):
        start(spread(step))
    start(local)

    for step in range(1, DEVICES):
        remote(small_ref, smallb.at[peer_of(me, step)], small_send.at[step], small_recv.at[step], me).wait_recv()
    smallb[me] = small_ref[...]
    total = smallb[0]
    for device in range(1, DEVICES):
        total = total + smallb[device]
    small_out[...] = total

    for step in (2, 4, 6):
        for arrived, onward in zip(spread(step, arrival=True), forward(step)):
            arrived.wait_recv()
            onward.start()
    wait_recv(spread(1, arrival=True))
    for copy in local:
        copy.wait()
    for step in (1, 2, 4, 6):
        wait_send(spread(step))
    for step in (2, 4, 6):
        wait_send(forward(step))
        wait_recv(forward(step, arrival=True))
    for order in range(chips):
        wait_send(pair(order))
    for order in range(chips - 1):
        wait_send(chip(order, me))
    for step in range(1, DEVICES):
        remote(small_ref, smallb.at[me], small_send.at[step], small_recv.at[step], me).wait_send()


def grads_call(ht, dy, small, o, dq, dk, dv):
    model, tokens = ht.shape
    groups, chips = DEVICES, DEVICES // 2
    q_cols, head_dim = o.shape[1] // groups, dk.shape[1] // groups
    width = q_cols + 2 * head_dim
    vmem = pl.BlockSpec(memory_space=pltpu.VMEM)
    anywhere = pl.BlockSpec(memory_space=pl.ANY)
    a, b = (q_cols, model), (model, width)
    dma = lambda *shape: pltpu.SemaphoreType.DMA(shape)
    return pl.pallas_call(
        grads_kernel,
        in_specs=[vmem, vmem, vmem, anywhere, anywhere, anywhere, anywhere],
        out_specs=[anywhere, anywhere, vmem],
        out_shape=[jax.ShapeDtypeStruct((groups,) + a, BF16), jax.ShapeDtypeStruct((groups,) + b, BF16),
                   jax.ShapeDtypeStruct(small.shape, F32)],
        scratch_shapes=[
            pltpu.VMEM((2, tokens, q_cols), BF16), pltpu.VMEM((2, tokens, width), BF16),
            pltpu.VMEM((chips,) + a, BF16), pltpu.VMEM((chips,) + b, BF16),
            pltpu.VMEM((chips,) + a, BF16), pltpu.VMEM((chips,) + b, BF16),
            pltpu.VMEM((chips - 1,) + a, BF16), pltpu.VMEM((chips - 1,) + b, BF16),
            pltpu.VMEM((chips - 1,) + a, BF16), pltpu.VMEM((chips - 1,) + b, BF16),
            pltpu.VMEM(a, F32), pltpu.VMEM(b, F32), pltpu.VMEM(a, BF16), pltpu.VMEM(b, BF16),
            pltpu.VMEM((DEVICES,) + small.shape, F32),
            dma(2, 4), dma(2, chips), dma(2, chips), dma(2, chips), dma(2, chips),
            dma(2, DEVICES), dma(2, DEVICES), dma(2, DEVICES), dma(2, DEVICES), dma(DEVICES), dma(DEVICES),
        ],
        compiler_params=pltpu.CompilerParams(vmem_limit_bytes=62 * 1024 * 1024, collective_id=1, has_side_effects=True),
        cost_estimate=pl.CostEstimate(flops=2 * tokens * model * 6144, bytes_accessed=60_000_000, transcendentals=0),
        name="grads",
    )(ht, dy, small, o, dq, dk, dv)


def widen_kernel(ga_ref, gb_ref, wq_ref, wk_ref, wv_ref, wo_ref):
    q_cols, head_dim = wq_ref.shape[1], wk_ref.shape[1]
    wo_ref[...] = ga_ref[0].astype(F32)
    wq_ref[...] = gb_ref[0, :, :q_cols].astype(F32)
    wk_ref[...] = gb_ref[0, :, q_cols:q_cols + head_dim].astype(F32)
    wv_ref[...] = gb_ref[0, :, q_cols + head_dim:].astype(F32)


def widen_call(ga, gb):
    groups, q_cols, model = ga.shape
    head_dim = (gb.shape[2] - q_cols) // 2
    f32 = lambda *shape: jax.ShapeDtypeStruct(shape, F32)
    across = lambda g: (0, g)
    return pl.pallas_call(
        widen_kernel,
        grid=(groups,),
        in_specs=[pl.BlockSpec((1, q_cols, model), lambda g: (g, 0, 0)),
                  pl.BlockSpec((1, model, gb.shape[2]), lambda g: (g, 0, 0))],
        out_specs=[pl.BlockSpec((model, q_cols), across), pl.BlockSpec((model, head_dim), across),
                   pl.BlockSpec((model, head_dim), across), pl.BlockSpec((q_cols, model), lambda g: (g, 0))],
        out_shape=[f32(model, groups * q_cols), f32(model, groups * head_dim), f32(model, groups * head_dim),
                   f32(groups * q_cols, model)],
        compiler_params=pltpu.CompilerParams(dimension_semantics=("arbitrary",)),
        name="widen",
    )(ga, gb)


def solution(mesh):
    seq_spec = P(None, 'sp', None)
    replicated = P()

    def shard_body(hidden_in, grad_out, positions, w_q, w_k, w_v, w_o, g_in, q_norm, k_norm):
        batch, seq_dev, model_dim = hidden_in.shape
        head_dim = q_norm.shape[0]
        exponents = jnp.arange(0, head_dim, 2).astype(F32) / head_dim
        inv_freq = jnp.power(ROPE_THETA, -exponents)
        freq = jnp.concatenate([inv_freq, inv_freq])[None]
        pos = jnp.broadcast_to(jnp.pad(positions.astype(F32), ((0, 0), (0, head_dim - seq_dev)))[:, None, :], (batch, 8, head_dim))
        gains = (g_in.astype(F32)[None], q_norm.astype(F32)[None], k_norm.astype(F32)[None])
        hidden_out, grad_in, ht, dy, o, dq, dk, dv, dgin, dqn, dkn = block_call(
            hidden_in, grad_out, pos, freq, *gains, w_q, w_k, w_v, w_o)
        small = jnp.concatenate([dgin.reshape(-1, head_dim), dqn, dkn, jnp.zeros((6, head_dim), F32)], axis=0)
        flat = lambda t: t.reshape(-1, t.shape[-1])
        ga, gb, small = grads_call(ht, flat(dy), small, flat(o), flat(dq), flat(dk), flat(dv))
        grad_wq, grad_wk, grad_wv, grad_wo = widen_call(ga, gb)
        rows = model_dim // head_dim
        return (hidden_out, grad_in, grad_wq, grad_wk, grad_wv, grad_wo,
                small[:rows].reshape(-1), small[rows], small[rows + 1])

    return jax.shard_map(shard_body, mesh=mesh,
                         in_specs=(seq_spec, seq_spec, P(None, 'sp'), replicated, replicated, replicated, replicated, replicated, replicated, replicated),
                         out_specs=(seq_spec, seq_spec, replicated, replicated, replicated, replicated, replicated, replicated, replicated),
                         check_vma=False)
```

```python
import functools
import jax
import jax.numpy as jnp
from jax import lax
from jax.experimental import pallas as pl
from jax.experimental.pallas import tpu as pltpu
from jax.sharding import PartitionSpec as P

EPSILON = 1e-6
ROPE_THETA = 1000000.0
NEG_LARGE = -1e30
LOG2_E = 1.4426950408889634
NT = (((1,), (1,)), ((), ()))
TN = (((0,), (0,)), ((), ()))
ROW_BLOCK = 256
DEVICES = 8
BF16 = jnp.bfloat16
F32 = jnp.float32


def dot(a, b, dims=(((1,), (0,)), ((), ()))):
    return lax.dot_general(a, b, dims, preferred_element_type=F32)


def peer_of(me, step):
    core, x, y = me % 2, (me // 2) % 2, me // 4
    return ((y + step // 4) % 2) * 4 + ((x + (step // 2) % 2) % 2) * 2 + (core + step % 2) % 2


def entry_barrier(me):
    barrier = pltpu.get_barrier_semaphore()
    for step in range(1, DEVICES):
        pl.semaphore_signal(barrier, inc=1, device_id=(peer_of(me, step),), device_id_type=pl.DeviceIdType.MESH)
    pl.semaphore_wait(barrier, DEVICES - 1)


def remote(src, dst, send, recv, device):
    return pltpu.make_async_remote_copy(src_ref=src, dst_ref=dst, send_sem=send, recv_sem=recv,
                                        device_id=(device,), device_id_type=pl.DeviceIdType.MESH)


def block_kernel(x_hbm, dy_hbm, pos_hbm, wq_hbm, wk_hbm, wv_hbm, wo_hbm, freq_ref, gin_ref, qn_ref, kn_ref,
                 out_hbm, gi_hbm, ht_ref, dyo_ref, o_ref, dq_ref, dk_ref, dv_ref, dgin_ref, dqn_ref, dkn_ref,
                 xb, dyb, gib, posb, wqkv, wo, h_ref, rope_cos, rope_sin, next_cos, next_sin, out_acc, dh_acc,
                 q_next, k_next, v_next, do_next, v_now, do_now, o_now, dqkv_now, o_last, dqkv_last,
                 weight_sem, in_send, in_recv, out_send, out_recv):
    seq, group = pl.program_id(0), pl.program_id(1)
    seqs, groups = pl.num_programs(0), pl.num_programs(1)
    me = lax.axis_index('sp')
    head_dim = qn_ref.shape[1]
    q_cols = o_now.shape[1]
    per_kv = q_cols // head_dim
    seq_len = xb.shape[1]
    piece = seq_len // DEVICES
    scale = head_dim ** -0.5
    half = head_dim // 2
    tiles = [slice(i, i + ROW_BLOCK) for i in range(0, seq_len, ROW_BLOCK)]

    def rows_of(device):
        return pl.ds(pl.multiple_of(device * piece, piece), piece)

    def incoming(kind, s, step, arrival=False):
        peer = peer_of(me, step)
        src = (x_hbm, dy_hbm, pos_hbm)[kind].at[DEVICES * s + peer]

        def landing(device):
            return posb.at[s, device] if kind == 2 else (xb, dyb)[kind].at[s, rows_of(device)]

        if step == 0:
            return pltpu.make_async_copy(src, landing(me), in_recv.at[kind, s, 0])
        return remote(src, landing(peer if arrival else me), in_send.at[kind, s, step], in_recv.at[kind, s, step], peer)

    def outgoing(kind, s, step, arrival=False):
        peer = peer_of(me, step)
        src = (xb, gib)[kind].at[s, rows_of(peer)]
        dst = (out_hbm, gi_hbm)[kind]
        if step == 0:
            return pltpu.make_async_copy(src, dst.at[DEVICES * s + me], out_recv.at[kind, s, 0])
        return remote(src, dst.at[DEVICES * s + (peer if arrival else me)],
                      out_send.at[kind, s, step], out_recv.at[kind, s, step], peer)

    def weight_loads():
        copies = [pltpu.make_async_copy(wo_hbm.at[g * q_cols:(g + 1) * q_cols], wo.at[g], weight_sem.at[3, g]) for g in range(wo.shape[0])]
        for i, src in enumerate((wq_hbm, wk_hbm, wv_hbm)):
            start, size = (0, q_cols, q_cols + head_dim)[i], q_cols if i == 0 else head_dim
            copies += [pltpu.make_async_copy(src.at[:, g * size:(g + 1) * size], wqkv.at[g, :, start:start + size], weight_sem.at[i, g])
                       for g in range(wo.shape[0])]
        return copies

    def arrive(kind, s):
        for step in range(DEVICES):
            if step == 0:
                incoming(kind, s, 0).wait()
            else:
                incoming(kind, s, step, arrival=True).wait_recv()

    def prepare(s):
        arrive(2, s)
        on_diag = lax.broadcasted_iota(jnp.int32, (piece, head_dim), 0) == lax.broadcasted_iota(jnp.int32, (piece, head_dim), 1)
        low = lax.broadcasted_iota(jnp.int32, (piece, head_dim), 1) < half
        for device in range(DEVICES):
            row = jnp.broadcast_to(posb[s, device, 0:1, :], (piece, head_dim))
            column = jnp.sum(jnp.where(on_diag, row, 0.0), axis=-1, keepdims=True)
            angles = column * freq_ref[...]
            sin = jnp.sin(angles)
            next_cos[device * piece:(device + 1) * piece, :] = jnp.cos(angles)
            next_sin[device * piece:(device + 1) * piece, :] = jnp.where(low, -sin, sin)
        arrive(0, s)
        x = xb[s].astype(F32)
        inv = lax.rsqrt(jnp.mean(x * x, axis=-1, keepdims=True) + EPSILON)
        h_ref[...] = (x * inv * gin_ref[...]).astype(BF16)
        arrive(1, s)

    def project(s, g):
        def q_rows(rows):
            q_next[rows] = dot(h_ref[rows], wqkv[g, :, :q_cols])

        def kv_rows(rows):
            kv = dot(h_ref[rows], wqkv[g, :, q_cols:])
            k_next[rows] = kv[:, :head_dim]
            v_next[rows] = kv[:, head_dim:].astype(BF16)

        def do_rows(rows):
            do_next[rows] = dot(dyb[s, rows], wo[g], NT).astype(BF16)

        return [functools.partial(f, rows) for f in (q_rows, kv_rows, do_rows) for rows in tiles]

    def accumulate(g):
        def out_cols(cols):
            out_acc[:, cols] += dot(o_last[...], wo[g, :, cols])

        def dh_cols(cols):
            dh_acc[:, cols] += dot(dqkv_last[...], wqkv[g, cols, :], NT)

        columns = [slice(c, c + 256) for c in range(0, out_acc.shape[1], 256)]
        return [functools.partial(f, cols) for f in (out_cols, dh_cols) for cols in columns]

    def run(products):
        for product in products:
            product()

    def finish(s):
        x = xb[s].astype(F32)
        inv = lax.rsqrt(jnp.mean(x * x, axis=-1, keepdims=True) + EPSILON)
        unit = x * inv
        xb[s] = (x + out_acc[...]).astype(BF16)
        d_norm = dh_acc[...]
        dgin_ref[...] += jnp.sum(d_norm * unit, axis=0, keepdims=True)
        d_unit = d_norm * gin_ref[...]
        grad = inv * (d_unit - unit * jnp.mean(d_unit * unit, axis=-1, keepdims=True))
        gib[s] = (dyb[s].astype(F32) + grad).astype(BF16)
        for kind in range(2):
            for step in (2, 4, 6, 3, 5, 7, 1, 0):
                outgoing(kind, s, step).start()

    @pl.when((seq == 0) & (group == 0))
    def _():
        entry_barrier(me)

        def send_all(s, carry):
            for kind in (2, 0, 1):
                for step in (2, 4, 6, 3, 5, 7, 1, 0):
                    incoming(kind, s, step).start()
            return carry

        lax.fori_loop(0, seqs, send_all, 0)
        for copy in weight_loads():
            copy.start()
        dgin_ref[...] = jnp.zeros_like(dgin_ref)
        dqn_ref[...] = jnp.zeros_like(dqn_ref)
        dkn_ref[...] = jnp.zeros_like(dkn_ref)
        o_now[...] = jnp.zeros_like(o_now)
        dqkv_now[...] = jnp.zeros_like(dqkv_now)
        out_acc[...] = jnp.zeros_like(out_acc)
        dh_acc[...] = jnp.zeros_like(dh_acc)
        for copy in weight_loads():
            copy.wait()
        prepare(0)
        run(project(0, 0))

    @pl.when(group == 0)
    def _():
        rope_cos[...] = next_cos[...]
        rope_sin[...] = next_sin[...]
        ht_ref[...] = h_ref[...].T
        dyo_ref[0] = dyb[seq]

    last_group = group == groups - 1

    @pl.when(last_group & (seq < seqs - 1))
    def _():
        prepare(seq + 1)

    cos, sin = rope_cos[...], rope_sin[...]

    def norm_rotate(t, gain):
        inv = lax.rsqrt(jnp.mean(t * t, axis=-1, keepdims=True) + EPSILON)
        unit = t * inv
        scaled = unit * gain
        return (scaled * cos + pltpu.roll(scaled, half, 1) * sin).astype(BF16), unit, inv

    def norm_rotate_back(grad, unit, inv, gain):
        d_scaled = grad * cos - pltpu.roll(grad, half, 1) * sin
        d_gain = jnp.sum(d_scaled * unit, axis=0, keepdims=True)
        d_unit = d_scaled * gain
        return inv * (d_unit - unit * jnp.mean(d_unit * unit, axis=-1, keepdims=True)), d_gain

    v_now[...] = v_next[...]
    do_now[...] = do_next[...]
    o_last[...] = o_now[...]
    dqkv_last[...] = dqkv_now[...]

    ahead = project(jnp.minimum(seq + last_group.astype(jnp.int32), seqs - 1), (group + 1) % groups)
    behind = accumulate((group + groups - 1) % groups)
    lanes = [slice(head * head_dim, (head + 1) * head_dim) for head in range(per_kv)]
    stacked = per_kv * ROW_BLOCK
    rows_id = lax.broadcasted_iota(jnp.int32, (stacked, ROW_BLOCK), 0) % ROW_BLOCK
    causal = rows_id >= lax.broadcasted_iota(jnp.int32, (stacked, ROW_BLOCK), 1)
    blocks = len(tiles)

    run(behind[:6])
    k_rot, k_unit, k_inv = norm_rotate(k_next[...], kn_ref[...])
    q_parts = [norm_rotate(q_next[:, lane], qn_ref[...]) for lane in lanes]
    q_tile = [jnp.concatenate([part[0][tile] for part in q_parts], axis=0) for tile in tiles]
    do_tile = [jnp.concatenate([do_now[tile, lane] for lane in lanes], axis=0) for tile in tiles]

    def scores(i):
        s_parts = [dot(q_tile[i], k_rot[tiles[j]], NT) for j in range(i + 1)]
        s_parts[i] = jnp.where(causal, s_parts[i], NEG_LARGE)
        return s_parts

    def softmax(s_parts):
        top = functools.reduce(jnp.maximum, [jnp.max(s, axis=-1, keepdims=True) for s in s_parts])
        e_parts = [jnp.exp2((s - top) * (scale * LOG2_E)) for s in s_parts]
        recip = 1.0 / functools.reduce(jnp.add, [jnp.sum(e, axis=-1, keepdims=True) for e in e_parts])
        p_parts = [e * recip for e in e_parts]
        return p_parts, [p.astype(BF16) for p in p_parts]

    def softmax_back(p_parts, dp_parts):
        delta = functools.reduce(jnp.add, [jnp.sum(p * dp, axis=-1, keepdims=True) for p, dp in zip(p_parts, dp_parts)])
        return [(p * (dp - delta)).astype(BF16) for p, dp in zip(p_parts, dp_parts)]

    def rows_sum(parts, values):
        return functools.reduce(jnp.add, [dot(part, values[tiles[j]]) for j, part in enumerate(parts)])

    def store_output(i, o_i):
        for head, lane in enumerate(lanes):
            o_head = o_i[head * ROW_BLOCK:(head + 1) * ROW_BLOCK].astype(BF16)
            o_ref[0, tiles[i], lane] = o_head
            o_now[tiles[i], lane] = o_head

    fill = [ahead[0:2], behind[6:7], behind[7:8] + ahead[2:3], ahead[3:4]]
    s_all = [scores(i) for i in range(blocks)]
    dp_all = [[dot(do_tile[i], v_now[tiles[j]], NT) for j in range(i + 1)] for i in range(blocks)]
    dk_parts, dv_parts, dq_tile = [None] * blocks, [None] * blocks, []
    for i in range(blocks):
        p_parts, pb_parts = softmax(s_all[i])
        run(fill[2 * i])
        store_output(i, rows_sum(pb_parts, v_now))
        for j in range(i + 1):
            dv_j = dot(pb_parts[j], do_tile[i], TN)
            dv_parts[j] = dv_j if dv_parts[j] is None else dv_parts[j] + dv_j
        ds_parts = softmax_back(p_parts, dp_all[i])
        run(fill[2 * i + 1])
        dq_tile.append(rows_sum(ds_parts, k_rot))
        for j in range(i + 1):
            dk_j = dot(ds_parts[j], q_tile[i], TN)
            dk_parts[j] = dk_j if dk_parts[j] is None else dk_parts[j] + dk_j
    run(ahead[4:])
    for head, lane in enumerate(lanes):
        dq_head = jnp.concatenate([dq[head * ROW_BLOCK:(head + 1) * ROW_BLOCK] for dq in dq_tile], axis=0)
        dq_head, d_gain = norm_rotate_back(dq_head * scale, q_parts[head][1], q_parts[head][2], qn_ref[...])
        dqn_ref[...] += d_gain
        dq_head = dq_head.astype(BF16)
        dq_ref[0, :, lane] = dq_head
        dqkv_now[:, lane] = dq_head
    dk_head, d_gain = norm_rotate_back(jnp.concatenate(dk_parts, axis=0) * scale, k_unit, k_inv, kn_ref[...])
    dkn_ref[...] += d_gain
    dk_head = dk_head.astype(BF16)
    dk_ref[0] = dk_head
    dqkv_now[:, q_cols:q_cols + head_dim] = dk_head
    dv_head = jnp.concatenate(dv_parts, axis=0).astype(BF16)
    dv_ref[0] = dv_head
    dqkv_now[:, q_cols + head_dim:] = dv_head

    @pl.when((group == 0) & (seq > 0))
    def _():
        finish(seq - 1)
        out_acc[...] = jnp.zeros_like(out_acc)
        dh_acc[...] = jnp.zeros_like(dh_acc)

    @pl.when((seq == seqs - 1) & last_group)
    def _():
        o_last[...] = o_now[...]
        dqkv_last[...] = dqkv_now[...]
        run(accumulate(groups - 1))
        finish(seqs - 1)

        def drain(s, carry):
            for step in range(1, DEVICES):
                for kind in range(3):
                    incoming(kind, s, step).wait_send()
            for step in range(DEVICES):
                for kind in range(2):
                    if step == 0:
                        outgoing(kind, s, 0).wait()
                    else:
                        outgoing(kind, s, step).wait_send()
                        outgoing(kind, s, step, arrival=True).wait_recv()
            return carry

        lax.fori_loop(0, seqs, drain, 0)


def block_call(x, dy, pos, freq, g_in, q_norm, k_norm, w_q, w_k, w_v, w_o):
    batch, piece, model = x.shape
    seqs, seq_len = batch // DEVICES, piece * DEVICES
    head_dim = q_norm.shape[1]
    q_width, kv_width = w_q.shape[1], w_k.shape[1]
    groups = kv_width // head_dim
    q_cols = q_width // groups
    tokens = seqs * seq_len
    width = q_cols + 2 * head_dim
    row = lambda s, g: (s, 0, 0)
    col = lambda s, g: (s, 0, g)
    fixed = lambda s, g: (0, 0)
    bf = lambda *shape: jax.ShapeDtypeStruct(shape, BF16)
    f32 = lambda *shape: jax.ShapeDtypeStruct(shape, F32)
    anywhere = pl.BlockSpec(memory_space=pl.ANY)
    flops = 4 * tokens * model * (q_width * 2 + kv_width * 2) + 12 * tokens * seq_len * q_width
    vb = lambda *shape: pltpu.VMEM(shape, BF16)
    vf = lambda *shape: pltpu.VMEM(shape, F32)
    return pl.pallas_call(
        block_kernel,
        grid=(seqs, groups),
        in_specs=[
            anywhere, anywhere, anywhere, anywhere, anywhere, anywhere, anywhere,
            pl.BlockSpec((1, head_dim), fixed),
            pl.BlockSpec((1, model), fixed),
            pl.BlockSpec((1, head_dim), fixed),
            pl.BlockSpec((1, head_dim), fixed),
        ],
        out_specs=[
            anywhere, anywhere,
            pl.BlockSpec((model, seq_len), lambda s, g: (0, s)),
            pl.BlockSpec((1, seq_len, model), row),
            pl.BlockSpec((1, seq_len, q_cols), col),
            pl.BlockSpec((1, seq_len, q_cols), col),
            pl.BlockSpec((1, seq_len, head_dim), col),
            pl.BlockSpec((1, seq_len, head_dim), col),
            pl.BlockSpec((1, model), fixed),
            pl.BlockSpec((1, head_dim), fixed),
            pl.BlockSpec((1, head_dim), fixed),
        ],
        out_shape=[
            bf(batch, piece, model), bf(batch, piece, model),
            bf(model, tokens), bf(seqs, seq_len, model),
            bf(seqs, seq_len, q_width), bf(seqs, seq_len, q_width),
            bf(seqs, seq_len, kv_width), bf(seqs, seq_len, kv_width),
            f32(1, model), f32(1, head_dim), f32(1, head_dim),
        ],
        scratch_shapes=[
            vb(seqs, seq_len, model), vb(seqs, seq_len, model), vb(seqs, seq_len, model),
            vf(seqs, DEVICES, 8, head_dim),
            vb(groups, model, width), vb(groups, q_cols, model),
            vb(seq_len, model),
            vf(seq_len, head_dim), vf(seq_len, head_dim), vf(seq_len, head_dim), vf(seq_len, head_dim),
            vf(seq_len, model), vf(seq_len, model),
            vf(seq_len, q_cols), vf(seq_len, head_dim), vb(seq_len, head_dim), vb(seq_len, q_cols),
            vb(seq_len, head_dim), vb(seq_len, q_cols),
            vb(seq_len, q_cols), vb(seq_len, width), vb(seq_len, q_cols), vb(seq_len, width),
            pltpu.SemaphoreType.DMA((4, groups)),
            pltpu.SemaphoreType.DMA((3, seqs, DEVICES)),
            pltpu.SemaphoreType.DMA((3, seqs, DEVICES)),
            pltpu.SemaphoreType.DMA((2, seqs, DEVICES)),
            pltpu.SemaphoreType.DMA((2, seqs, DEVICES)),
        ],
        compiler_params=pltpu.CompilerParams(
            dimension_semantics=("arbitrary", "arbitrary"), vmem_limit_bytes=62 * 1024 * 1024,
            collective_id=0, has_side_effects=True),
        cost_estimate=pl.CostEstimate(flops=flops, bytes_accessed=50_000_000, transcendentals=tokens * seq_len * 8),
        name="block",
    )(x, dy, pos, w_q, w_k, w_v, w_o, freq, g_in, q_norm, k_norm)


def grads_kernel(ht_ref, dy_ref, small_ref, o_hbm, dq_hbm, dk_hbm, dv_hbm,
                 ga_hbm, gb_hbm, small_out,
                 ob, qkvb, s1a, s1b, l1a, l1b, s2a, s2b, l2a, l2b, acc_a, acc_b, ra, rb, smallb,
                 load_sem, pair_send, pair_recv, chip_send, chip_recv, all_send, all_recv, fwd_send, fwd_recv,
                 small_send, small_recv):
    me = lax.axis_index('sp')
    partner = peer_of(me, 1)
    q_cols, head_dim = ob.shape[2], (qkvb.shape[2] - ob.shape[2]) // 2
    chips = l1a.shape[0]

    def peer_group(order):
        return peer_of(me, (1 - order // 2) * 2 + (((order + 1) // 2) % 2) * 4)

    def loads(group, slot):
        wide = pl.ds(pl.multiple_of(group * q_cols, q_cols), q_cols)
        narrow = pl.ds(pl.multiple_of(group * head_dim, head_dim), head_dim)
        return [
            pltpu.make_async_copy(o_hbm.at[:, wide], ob.at[slot], load_sem.at[slot, 0]),
            pltpu.make_async_copy(dq_hbm.at[:, wide], qkvb.at[slot, :, pl.ds(0, q_cols)], load_sem.at[slot, 1]),
            pltpu.make_async_copy(dk_hbm.at[:, narrow], qkvb.at[slot, :, pl.ds(q_cols, head_dim)], load_sem.at[slot, 2]),
            pltpu.make_async_copy(dv_hbm.at[:, narrow], qkvb.at[slot, :, pl.ds(q_cols + head_dim, head_dim)], load_sem.at[slot, 3]),
        ]

    def start(copies):
        for copy in copies:
            copy.start()

    def pair(order):
        return [remote(s1a.at[order], l1a.at[order], pair_send.at[0, order], pair_recv.at[0, order], partner),
                remote(s1b.at[order], l1b.at[order], pair_send.at[1, order], pair_recv.at[1, order], partner)]

    def chip(order, device):
        return [remote(s2a.at[order], l2a.at[order], chip_send.at[0, order], chip_recv.at[0, order], device),
                remote(s2b.at[order], l2b.at[order], chip_send.at[1, order], chip_recv.at[1, order], device)]

    start(loads(peer_of(peer_group(0), 1), 0))
    entry_barrier(me)
    for step in range(1, DEVICES):
        remote(small_ref, smallb.at[me], small_send.at[step], small_recv.at[step], peer_of(me, step)).start()

    def products(slot):
        return dot(ob[slot], dy_ref[...], TN), dot(ht_ref[...], qkvb[slot])

    def body(order, carry):
        mine = peer_group(order)
        other = peer_of(mine, 1)
        start(loads(mine, 1))
        for copy in loads(other, 0):
            copy.wait()
        prod_a, prod_b = products(0)
        s1a[order] = prod_a.astype(BF16)
        s1b[order] = prod_b.astype(BF16)
        start(pair(order))

        @pl.when(order < chips - 1)
        def _():
            start(loads(peer_of(peer_group(order + 1), 1), 0))

        for copy in loads(mine, 1):
            copy.wait()
        prod_a, prod_b = products(1)
        acc_a[...] = prod_a
        acc_b[...] = prod_b
        for copy in pair(order):
            copy.wait_recv()
        sum_a = acc_a[...] + l1a[order].astype(F32)
        sum_b = acc_b[...] + l1b[order].astype(F32)

        @pl.when(order < chips - 1)
        def _():
            s2a[order] = sum_a.astype(BF16)
            s2b[order] = sum_b.astype(BF16)
            start(chip(order, mine))

        @pl.when(order == chips - 1)
        def _():
            acc_a[...] = sum_a
            acc_b[...] = sum_b
        return carry

    lax.fori_loop(0, chips, body, 0)

    for order in range(chips - 1):
        for copy in chip(order, me):
            copy.wait_recv()
    ra[...] = (acc_a[...] + l2a[0].astype(F32) + l2a[1].astype(F32) + l2a[2].astype(F32)).astype(BF16)
    rb[...] = (acc_b[...] + l2b[0].astype(F32) + l2b[1].astype(F32) + l2b[2].astype(F32)).astype(BF16)

    pairs = ((ra, ga_hbm), (rb, gb_hbm))

    def spread(step, arrival=False):
        peer = peer_of(me, step)
        return [remote(src, dst.at[peer if arrival else me], all_send.at[i, step], all_recv.at[i, step], peer)
                for i, (src, dst) in enumerate(pairs)]

    def forward(step, arrival=False):
        owner, theirs = peer_of(me, step), peer_of(partner, step)
        return [remote(dst.at[owner], dst.at[theirs if arrival else owner], fwd_send.at[i, step], fwd_recv.at[i, step], partner)
                for i, (_, dst) in enumerate(pairs)]

    def wait_send(copies):
        for copy in copies:
            copy.wait_send()

    def wait_recv(copies):
        for copy in copies:
            copy.wait_recv()

    local = [pltpu.make_async_copy(src, dst.at[me], all_recv.at[i, 0]) for i, (src, dst) in enumerate(pairs)]
    for step in (2, 4, 6, 1):
        start(spread(step))
    start(local)

    for step in range(1, DEVICES):
        remote(small_ref, smallb.at[peer_of(me, step)], small_send.at[step], small_recv.at[step], me).wait_recv()
    smallb[me] = small_ref[...]
    total = smallb[0]
    for device in range(1, DEVICES):
        total = total + smallb[device]
    small_out[...] = total

    for step in (2, 4, 6):
        for arrived, onward in zip(spread(step, arrival=True), forward(step)):
            arrived.wait_recv()
            onward.start()
    wait_recv(spread(1, arrival=True))
    for copy in local:
        copy.wait()
    for step in (1, 2, 4, 6):
        wait_send(spread(step))
    for step in (2, 4, 6):
        wait_send(forward(step))
        wait_recv(forward(step, arrival=True))
    for order in range(chips):
        wait_send(pair(order))
    for order in range(chips - 1):
        wait_send(chip(order, me))
    for step in range(1, DEVICES):
        remote(small_ref, smallb.at[me], small_send.at[step], small_recv.at[step], me).wait_send()


def grads_call(ht, dy, small, o, dq, dk, dv):
    model, tokens = ht.shape
    groups, chips = DEVICES, DEVICES // 2
    q_cols, head_dim = o.shape[1] // groups, dk.shape[1] // groups
    width = q_cols + 2 * head_dim
    vmem = pl.BlockSpec(memory_space=pltpu.VMEM)
    anywhere = pl.BlockSpec(memory_space=pl.ANY)
    a, b = (q_cols, model), (model, width)
    dma = lambda *shape: pltpu.SemaphoreType.DMA(shape)
    return pl.pallas_call(
        grads_kernel,
        in_specs=[vmem, vmem, vmem, anywhere, anywhere, anywhere, anywhere],
        out_specs=[anywhere, anywhere, vmem],
        out_shape=[jax.ShapeDtypeStruct((groups,) + a, BF16), jax.ShapeDtypeStruct((groups,) + b, BF16),
                   jax.ShapeDtypeStruct(small.shape, F32)],
        scratch_shapes=[
            pltpu.VMEM((2, tokens, q_cols), BF16), pltpu.VMEM((2, tokens, width), BF16),
            pltpu.VMEM((chips,) + a, BF16), pltpu.VMEM((chips,) + b, BF16),
            pltpu.VMEM((chips,) + a, BF16), pltpu.VMEM((chips,) + b, BF16),
            pltpu.VMEM((chips - 1,) + a, BF16), pltpu.VMEM((chips - 1,) + b, BF16),
            pltpu.VMEM((chips - 1,) + a, BF16), pltpu.VMEM((chips - 1,) + b, BF16),
            pltpu.VMEM(a, F32), pltpu.VMEM(b, F32), pltpu.VMEM(a, BF16), pltpu.VMEM(b, BF16),
            pltpu.VMEM((DEVICES,) + small.shape, F32),
            dma(2, 4), dma(2, chips), dma(2, chips), dma(2, chips), dma(2, chips),
            dma(2, DEVICES), dma(2, DEVICES), dma(2, DEVICES), dma(2, DEVICES), dma(DEVICES), dma(DEVICES),
        ],
        compiler_params=pltpu.CompilerParams(vmem_limit_bytes=62 * 1024 * 1024, collective_id=1, has_side_effects=True),
        cost_estimate=pl.CostEstimate(flops=2 * tokens * model * 6144, bytes_accessed=60_000_000, transcendentals=0),
        name="grads",
    )(ht, dy, small, o, dq, dk, dv)


def widen_kernel(ga_ref, gb_ref, wq_ref, wk_ref, wv_ref, wo_ref):
    q_cols, head_dim = wq_ref.shape[1], wk_ref.shape[1]
    wo_ref[...] = ga_ref[0].astype(F32)
    wq_ref[...] = gb_ref[0, :, :q_cols].astype(F32)
    wk_ref[...] = gb_ref[0, :, q_cols:q_cols + head_dim].astype(F32)
    wv_ref[...] = gb_ref[0, :, q_cols + head_dim:].astype(F32)


def widen_call(ga, gb):
    groups, q_cols, model = ga.shape
    head_dim = (gb.shape[2] - q_cols) // 2
    f32 = lambda *shape: jax.ShapeDtypeStruct(shape, F32)
    across = lambda g: (0, g)
    return pl.pallas_call(
        widen_kernel,
        grid=(groups,),
        in_specs=[pl.BlockSpec((1, q_cols, model), lambda g: (g, 0, 0)),
                  pl.BlockSpec((1, model, gb.shape[2]), lambda g: (g, 0, 0))],
        out_specs=[pl.BlockSpec((model, q_cols), across), pl.BlockSpec((model, head_dim), across),
                   pl.BlockSpec((model, head_dim), across), pl.BlockSpec((q_cols, model), lambda g: (g, 0))],
        out_shape=[f32(model, groups * q_cols), f32(model, groups * head_dim), f32(model, groups * head_dim),
                   f32(groups * q_cols, model)],
        compiler_params=pltpu.CompilerParams(dimension_semantics=("arbitrary",)),
        name="widen",
    )(ga, gb)


def solution(mesh):
    seq_spec = P(None, 'sp', None)
    replicated = P()

    def shard_body(hidden_in, grad_out, positions, w_q, w_k, w_v, w_o, g_in, q_norm, k_norm):
        batch, seq_dev, model_dim = hidden_in.shape
        head_dim = q_norm.shape[0]
        exponents = jnp.arange(0, head_dim, 2).astype(F32) / head_dim
        inv_freq = jnp.power(ROPE_THETA, -exponents)
        freq = jnp.concatenate([inv_freq, inv_freq])[None]
        pos = jnp.broadcast_to(jnp.pad(positions.astype(F32), ((0, 0), (0, head_dim - seq_dev)))[:, None, :], (batch, 8, head_dim))
        gains = (g_in.astype(F32)[None], q_norm.astype(F32)[None], k_norm.astype(F32)[None])
        hidden_out, grad_in, ht, dy, o, dq, dk, dv, dgin, dqn, dkn = block_call(
            hidden_in, grad_out, pos, freq, *gains, w_q, w_k, w_v, w_o)
        small = jnp.concatenate([dgin.reshape(-1, head_dim), dqn, dkn, jnp.zeros((6, head_dim), F32)], axis=0)
        flat = lambda t: t.reshape(-1, t.shape[-1])
        ga, gb, small = grads_call(ht, flat(dy), small, flat(o), flat(dq), flat(dk), flat(dv))
        grad_wq, grad_wk, grad_wv, grad_wo = widen_call(ga, gb)
        rows = model_dim // head_dim
        return (hidden_out, grad_in, grad_wq, grad_wk, grad_wv, grad_wo,
                small[:rows].reshape(-1), small[rows], small[rows + 1])

    return jax.shard_map(shard_body, mesh=mesh,
                         in_specs=(seq_spec, seq_spec, P(None, 'sp'), replicated, replicated, replicated, replicated, replicated, replicated, replicated),
                         out_specs=(seq_spec, seq_spec, replicated, replicated, replicated, replicated, replicated, replicated, replicated),
                         check_vma=False)
```

```python
import functools
import jax
import jax.numpy as jnp
from jax import lax
from jax.experimental import pallas as pl
from jax.experimental.pallas import tpu as pltpu
from jax.sharding import PartitionSpec as P

EPSILON = 1e-6
ROPE_THETA = 1000000.0
NEG_LARGE = -1e30
LOG2_E = 1.4426950408889634
NT = (((1,), (1,)), ((), ()))
TN = (((0,), (0,)), ((), ()))
ROW_BLOCK = 256
DEVICES = 8
BF16 = jnp.bfloat16
F32 = jnp.float32


def dot(a, b, dims=(((1,), (0,)), ((), ()))):
    return lax.dot_general(a, b, dims, preferred_element_type=F32)


def peer_of(me, step):
    core, x, y = me % 2, (me // 2) % 2, me // 4
    return ((y + step // 4) % 2) * 4 + ((x + (step // 2) % 2) % 2) * 2 + (core + step % 2) % 2


def entry_barrier(me):
    barrier = pltpu.get_barrier_semaphore()
    for step in range(1, DEVICES):
        pl.semaphore_signal(barrier, inc=1, device_id=(peer_of(me, step),), device_id_type=pl.DeviceIdType.MESH)
    pl.semaphore_wait(barrier, DEVICES - 1)


def remote(src, dst, send, recv, device):
    return pltpu.make_async_remote_copy(src_ref=src, dst_ref=dst, send_sem=send, recv_sem=recv,
                                        device_id=(device,), device_id_type=pl.DeviceIdType.MESH)


def block_kernel(x_hbm, dy_hbm, pos_hbm, wq_hbm, wk_hbm, wv_hbm, wo_hbm, gains_ref,
                 out_hbm, gi_hbm, ga_hbm, gb_hbm, o_hbm, dqkv_hbm, small_out,
                 xb, dyb, gib, posb, wqkv, wo, h_ref, ht_ref, rope_cos, rope_sin, next_cos, next_sin, out_acc, dh_acc,
                 q_next, k_next, v_next, do_next, v_now, do_now, o_now, dqkv_now, o_last, dqkv_last, o_stage, dqkv_stage,
                 dgin_ref, dqn_ref, dkn_ref, small, smallb, ob, qkvb, l1a, l1b, t_a, t_b, l2a, l2b,
                 weight_sem, in_send, in_recv, out_send, out_recv, store_sem, load_sem, pair_send, pair_recv,
                 turn_send, turn_recv, chip_send, chip_recv, all_send, all_recv, small_send, small_recv):
    seq, group = pl.program_id(0), pl.program_id(1)
    seqs, groups = pl.num_programs(0), pl.num_programs(1)
    me = lax.axis_index('sp')
    head_dim, model = dqn_ref.shape[1], dgin_ref.shape[1]
    gin_ref = gains_ref.at[:, pl.ds(0, model)]
    qn_ref, kn_ref, freq_ref = (gains_ref.at[:, pl.ds(model + i * head_dim, head_dim)] for i in range(3))
    q_cols = o_now.shape[1]
    per_kv = q_cols // head_dim
    seq_len = xb.shape[1]
    piece = seq_len // DEVICES
    scale = head_dim ** -0.5
    half = head_dim // 2
    tiles = [slice(i, i + ROW_BLOCK) for i in range(0, seq_len, ROW_BLOCK)]

    def rows_of(device):
        return pl.ds(pl.multiple_of(device * piece, piece), piece)

    def incoming(kind, s, step, arrival=False):
        peer = peer_of(me, step)
        src = (x_hbm, dy_hbm, pos_hbm)[kind].at[DEVICES * s + peer]

        def landing(device):
            return posb.at[s, device] if kind == 2 else (xb, dyb)[kind].at[s, rows_of(device)]

        if step == 0:
            return pltpu.make_async_copy(src, landing(me), in_recv.at[kind, s, 0])
        return remote(src, landing(peer if arrival else me), in_send.at[kind, s, step], in_recv.at[kind, s, step], peer)

    def outgoing(kind, s, step, arrival=False):
        peer = peer_of(me, step)
        src = xb.at[s, rows_of(peer)] if kind == 0 else gib.at[s % 2, rows_of(peer)]
        dst = (out_hbm, gi_hbm)[kind]
        if step == 0:
            return pltpu.make_async_copy(src, dst.at[DEVICES * s + me], out_recv.at[kind, s, 0])
        return remote(src, dst.at[DEVICES * s + (peer if arrival else me)],
                      out_send.at[kind, s, step], out_recv.at[kind, s, step], peer)

    def sent(kind, s):
        outgoing(kind, s, 0).wait()
        for step in range(1, DEVICES):
            outgoing(kind, s, step).wait_send()

    def weight_loads():
        copies = [pltpu.make_async_copy(wo_hbm.at[g * q_cols:(g + 1) * q_cols], wo.at[g], weight_sem.at[3, g]) for g in range(wo.shape[0])]
        for i, src in enumerate((wq_hbm, wk_hbm, wv_hbm)):
            start, size = (0, q_cols, q_cols + head_dim)[i], q_cols if i == 0 else head_dim
            copies += [pltpu.make_async_copy(src.at[:, g * size:(g + 1) * size], wqkv.at[g, :, start:start + size], weight_sem.at[i, g])
                       for g in range(wo.shape[0])]
        return copies

    def arrive(kind, s):
        for step in range(DEVICES):
            if step == 0:
                incoming(kind, s, 0).wait()
            else:
                incoming(kind, s, step, arrival=True).wait_recv()

    def prepare(s):
        arrive(2, s)
        on_diag = lax.broadcasted_iota(jnp.int32, (piece, head_dim), 0) == lax.broadcasted_iota(jnp.int32, (piece, head_dim), 1)
        low = lax.broadcasted_iota(jnp.int32, (piece, head_dim), 1) < half
        half_count = DEVICES // 2

        def column(device):
            row = jnp.broadcast_to(posb[s, device, 0:1, :], (piece, head_dim))
            return jnp.sum(jnp.where(on_diag, row, 0.0), axis=-1, keepdims=True)

        for device in range(half_count):
            angles = jnp.where(low, column(device), column(device + half_count)) * freq_ref[...]
            cos, sin = jnp.cos(angles), jnp.sin(angles)
            cos_turned, sin_turned = pltpu.roll(cos, half, 1), pltpu.roll(sin, half, 1)
            first = slice(device * piece, (device + 1) * piece)
            second = slice((device + half_count) * piece, (device + half_count + 1) * piece)
            next_cos[first, :] = jnp.where(low, cos, cos_turned)
            next_sin[first, :] = jnp.where(low, -sin, sin_turned)
            next_cos[second, :] = jnp.where(low, cos_turned, cos)
            next_sin[second, :] = jnp.where(low, -sin_turned, sin)
        arrive(0, s)
        x = xb[s].astype(F32)
        inv = lax.rsqrt(jnp.mean(x * x, axis=-1, keepdims=True) + EPSILON)
        h_ref[...] = (x * inv * gin_ref[...]).astype(BF16)
        arrive(1, s)

    def project(s, g):
        def q_rows(rows):
            q_next[rows] = dot(h_ref[rows], wqkv[g, :, :q_cols])

        def kv_rows(rows):
            kv = dot(h_ref[rows], wqkv[g, :, q_cols:])
            k_next[rows] = kv[:, :head_dim]
            v_next[rows] = kv[:, head_dim:].astype(BF16)

        def do_rows(rows):
            do_next[rows] = dot(dyb[s, rows], wo[g], NT).astype(BF16)

        return [functools.partial(f, rows) for f in (q_rows, kv_rows, do_rows) for rows in tiles]

    def accumulate(g):
        def out_cols(cols):
            out_acc[:, cols] += dot(o_last[...], wo[g, :, cols])

        def dh_cols(cols):
            dh_acc[:, cols] += dot(dqkv_last[...], wqkv[g, cols, :], NT)

        columns = [slice(c, c + 256) for c in range(0, out_acc.shape[1], 256)]
        return [functools.partial(f, cols) for f in (out_cols, dh_cols) for cols in columns]

    def run(products):
        for product in products:
            product()

    def finish(s):
        x = xb[s].astype(F32)
        inv = lax.rsqrt(jnp.mean(x * x, axis=-1, keepdims=True) + EPSILON)
        unit = x * inv
        xb[s] = (x + out_acc[...]).astype(BF16)
        d_norm = dh_acc[...]
        dgin_ref[...] += jnp.sum(d_norm * unit, axis=0, keepdims=True)
        d_unit = d_norm * gin_ref[...]
        grad = inv * (d_unit - unit * jnp.mean(d_unit * unit, axis=-1, keepdims=True))

        @pl.when(s >= 2)
        def _():
            sent(1, s - 2)

        gib[s % 2] = (dyb[s].astype(F32) + grad).astype(BF16)
        for kind in range(2):
            for step in (2, 4, 6, 3, 5, 7, 1, 0):
                outgoing(kind, s, step).start()

    @pl.when((seq == 0) & (group == 0))
    def _():
        entry_barrier(me)

        def send_all(s, carry):
            for kind in (2, 0, 1):
                for step in (2, 4, 6, 3, 5, 7, 1, 0):
                    incoming(kind, s, step).start()
            return carry

        lax.fori_loop(0, seqs, send_all, 0)
        for copy in weight_loads():
            copy.start()
        dgin_ref[...] = jnp.zeros_like(dgin_ref)
        dqn_ref[...] = jnp.zeros_like(dqn_ref)
        dkn_ref[...] = jnp.zeros_like(dkn_ref)
        o_now[...] = jnp.zeros_like(o_now)
        dqkv_now[...] = jnp.zeros_like(dqkv_now)
        out_acc[...] = jnp.zeros_like(out_acc)
        dh_acc[...] = jnp.zeros_like(dh_acc)
        for copy in weight_loads():
            copy.wait()
        prepare(0)
        run(project(0, 0))

    @pl.when(group == 0)
    def _():
        rope_cos[...] = next_cos[...]
        rope_sin[...] = next_sin[...]
        ht_ref[:, pl.ds(pl.multiple_of(seq * seq_len, seq_len), seq_len)] = h_ref[...].T

    last_group = group == groups - 1

    @pl.when(last_group & (seq < seqs - 1))
    def _():
        prepare(seq + 1)

    cos, sin = rope_cos[...], rope_sin[...]

    def norm_rotate(t, gain):
        inv = lax.rsqrt(jnp.mean(t * t, axis=-1, keepdims=True) + EPSILON)
        unit = t * inv
        scaled = unit * gain
        return (scaled * cos + pltpu.roll(scaled, half, 1) * sin).astype(BF16), unit, inv

    def norm_rotate_back(grad, unit, inv, gain):
        d_scaled = grad * cos - pltpu.roll(grad, half, 1) * sin
        d_gain = jnp.sum(d_scaled * unit, axis=0, keepdims=True)
        d_unit = d_scaled * gain
        return inv * (d_unit - unit * jnp.mean(d_unit * unit, axis=-1, keepdims=True)), d_gain

    step_id = seq * groups + group
    slot = step_id % 2

    def stores(step):
        g, rows = step % groups, pl.ds(pl.multiple_of((step // groups) * seq_len, seq_len), seq_len)
        return [pltpu.make_async_copy(o_stage.at[step % 2], o_hbm.at[g, rows], store_sem.at[0, step % 2]),
                pltpu.make_async_copy(dqkv_stage.at[step % 2], dqkv_hbm.at[g, rows], store_sem.at[1, step % 2])]

    @pl.when(step_id >= 2)
    def _():
        for copy in stores(step_id - 2):
            copy.wait()

    @pl.when(step_id >= 1)
    def _():
        for copy in stores(step_id - 1):
            copy.start()

    v_now[...] = v_next[...]
    do_now[...] = do_next[...]
    o_last[...] = o_now[...]
    dqkv_last[...] = dqkv_now[...]

    ahead = project(jnp.minimum(seq + last_group.astype(jnp.int32), seqs - 1), (group + 1) % groups)
    behind = accumulate((group + groups - 1) % groups)
    lanes = [slice(head * head_dim, (head + 1) * head_dim) for head in range(per_kv)]
    stacked = per_kv * ROW_BLOCK
    rows_id = lax.broadcasted_iota(jnp.int32, (stacked, ROW_BLOCK), 0) % ROW_BLOCK
    causal = rows_id >= lax.broadcasted_iota(jnp.int32, (stacked, ROW_BLOCK), 1)
    blocks = len(tiles)

    run(behind[:6])
    k_rot, k_unit, k_inv = norm_rotate(k_next[...], kn_ref[...])
    q_parts = [norm_rotate(q_next[:, lane], qn_ref[...]) for lane in lanes]
    q_tile = [jnp.concatenate([part[0][tile] for part in q_parts], axis=0) for tile in tiles]
    do_tile = [jnp.concatenate([do_now[tile, lane] for lane in lanes], axis=0) for tile in tiles]

    def scores(i):
        s_parts = [dot(q_tile[i], k_rot[tiles[j]], NT) for j in range(i + 1)]
        s_parts[i] = jnp.where(causal, s_parts[i], NEG_LARGE)
        return s_parts

    def softmax(s_parts):
        top = functools.reduce(jnp.maximum, [jnp.max(s, axis=-1, keepdims=True) for s in s_parts])
        e_parts = [jnp.exp2((s - top) * (scale * LOG2_E)) for s in s_parts]
        recip = 1.0 / functools.reduce(jnp.add, [jnp.sum(e, axis=-1, keepdims=True) for e in e_parts])
        p_parts = [e * recip for e in e_parts]
        return p_parts, [p.astype(BF16) for p in p_parts]

    def softmax_back(p_parts, dp_parts):
        delta = functools.reduce(jnp.add, [jnp.sum(p * dp, axis=-1, keepdims=True) for p, dp in zip(p_parts, dp_parts)])
        return [(p * (dp - delta)).astype(BF16) for p, dp in zip(p_parts, dp_parts)]

    def rows_sum(parts, values):
        return functools.reduce(jnp.add, [dot(part, values[tiles[j]]) for j, part in enumerate(parts)])

    def store_output(i, o_i):
        for head, lane in enumerate(lanes):
            o_head = o_i[head * ROW_BLOCK:(head + 1) * ROW_BLOCK].astype(BF16)
            o_stage[slot, tiles[i], lane] = o_head
            o_now[tiles[i], lane] = o_head

    fill = [ahead[0:2], behind[6:7], behind[7:8] + ahead[2:3], ahead[3:4]]
    s_all = [scores(i) for i in range(blocks)]
    dp_all = [[dot(do_tile[i], v_now[tiles[j]], NT) for j in range(i + 1)] for i in range(blocks)]
    dk_parts, dv_parts, dq_tile = [None] * blocks, [None] * blocks, []
    for i in range(blocks):
        p_parts, pb_parts = softmax(s_all[i])
        run(fill[2 * i])
        store_output(i, rows_sum(pb_parts, v_now))
        for j in range(i + 1):
            dv_j = dot(pb_parts[j], do_tile[i], TN)
            dv_parts[j] = dv_j if dv_parts[j] is None else dv_parts[j] + dv_j
        ds_parts = softmax_back(p_parts, dp_all[i])
        run(fill[2 * i + 1])
        dq_tile.append(rows_sum(ds_parts, k_rot))
        for j in range(i + 1):
            dk_j = dot(ds_parts[j], q_tile[i], TN)
            dk_parts[j] = dk_j if dk_parts[j] is None else dk_parts[j] + dk_j
    run(ahead[4:])
    for head, lane in enumerate(lanes):
        dq_head = jnp.concatenate([dq[head * ROW_BLOCK:(head + 1) * ROW_BLOCK] for dq in dq_tile], axis=0)
        dq_head, d_gain = norm_rotate_back(dq_head * scale, q_parts[head][1], q_parts[head][2], qn_ref[...])
        dqn_ref[...] += d_gain
        dq_head = dq_head.astype(BF16)
        dqkv_stage[slot, :, lane] = dq_head
        dqkv_now[:, lane] = dq_head
    dk_head, d_gain = norm_rotate_back(jnp.concatenate(dk_parts, axis=0) * scale, k_unit, k_inv, kn_ref[...])
    dkn_ref[...] += d_gain
    dk_head = dk_head.astype(BF16)
    dqkv_stage[slot, :, q_cols:q_cols + head_dim] = dk_head
    dqkv_now[:, q_cols:q_cols + head_dim] = dk_head
    dv_head = jnp.concatenate(dv_parts, axis=0).astype(BF16)
    dqkv_stage[slot, :, q_cols + head_dim:] = dv_head
    dqkv_now[:, q_cols + head_dim:] = dv_head

    @pl.when((group == 0) & (seq > 0))
    def _():
        finish(seq - 1)
        out_acc[...] = jnp.zeros_like(out_acc)
        dh_acc[...] = jnp.zeros_like(dh_acc)

    @pl.when((seq == seqs - 1) & last_group)
    def _():
        o_last[...] = o_now[...]
        dqkv_last[...] = dqkv_now[...]
        run(accumulate(groups - 1))
        finish(seqs - 1)
        for copy in stores(step_id - 1):
            copy.wait()
        for copy in stores(step_id):
            copy.start()
        for copy in stores(step_id):
            copy.wait()
        reduce_gradients(me, (ga_hbm, gb_hbm), o_hbm, dqkv_hbm, small_out, dyb, ht_ref, wo, wqkv,
                         dgin_ref, dqn_ref, dkn_ref, small, smallb, ob, qkvb, (l1a, l1b), (t_a, t_b), (l2a, l2b), (out_acc, dh_acc),
                         load_sem, pair_send, pair_recv, turn_send, turn_recv, chip_send, chip_recv,
                         all_send, all_recv, small_send, small_recv)

        def drain(s, carry):
            for step in range(1, DEVICES):
                for kind in range(3):
                    incoming(kind, s, step).wait_send()
                for kind in range(2):
                    outgoing(kind, s, step, arrival=True).wait_recv()
            sent(0, s)
            return carry

        lax.fori_loop(0, seqs, drain, 0)
        for s in range(2):
            sent(1, seqs - 2 + s)


def start(copies):
    for copy in copies:
        copy.start()


def wait_send(copies):
    for copy in copies:
        copy.wait_send()


def wait_recv(copies):
    for copy in copies:
        copy.wait_recv()


X, Y, DIAG, PARTNER = 2, 4, 6, 1


def reduce_gradients(me, gathered, o_hbm, dqkv_hbm, small_out, dyb, ht_ref, wo, wqkv,
                     dgin_ref, dqn_ref, dkn_ref, small, smallb, ob, qkvb, pair_in, turn_in, chip_in, acc,
                     load_sem, pair_send, pair_recv, turn_send, turn_recv, chip_send, chip_recv,
                     all_send, all_recv, small_send, small_recv):
    partner = peer_of(me, PARTNER)
    chips = 4
    stage = (wo, wqkv)
    sizes = [ref.shape[1] // 2 for ref in stage]
    result = 2 * chips - 1

    def half_of(i, half):
        return pl.ds(half * sizes[i], sizes[i])

    def own(i, half):
        cols = stage[i].shape[2]
        return acc[i].at[pl.ds(half * sizes[i], sizes[i])] if i == 0 else acc[i].at[:, pl.ds(half * cols, cols)]

    small[...] = jnp.zeros_like(small)
    lanes = dqn_ref.shape[1]
    rows = dgin_ref.shape[1] // lanes
    for row in range(rows):
        small[row:row + 1] = dgin_ref[:, row * lanes:(row + 1) * lanes]
    small[rows:rows + 1] = dqn_ref[...]
    small[rows + 1:rows + 2] = dkn_ref[...]

    def small_copy(step, arrival=False):
        peer = peer_of(me, step)
        return remote(small, smallb.at[peer if arrival else me], small_send.at[step], small_recv.at[step], peer)

    def peer_group(order):
        return peer_of(me, (1 - order // 2) * X + ((order + 1) % 2) * Y)

    def loads(group, slot):
        return [pltpu.make_async_copy(o_hbm.at[group], ob.at[slot], load_sem.at[0, slot]),
                pltpu.make_async_copy(dqkv_hbm.at[group], qkvb.at[slot], load_sem.at[1, slot])]

    def wait(copies):
        for copy in copies:
            copy.wait()

    def pair(order):
        return [remote(stage[i].at[order], pair_in[i].at[order % 2], pair_send.at[i, order], pair_recv.at[i, order], partner) for i in range(2)]

    def turn(half):
        return [remote(stage[i].at[chips, half_of(i, half)], turn_in[i].at[half], turn_send.at[i, half], turn_recv.at[i, half],
                       peer_of(me, (X, Y)[half])) for i in range(2)]

    def chip(axis, half):
        return [remote(stage[i].at[chips + 1 + axis, half_of(i, half)], chip_in[i].at[axis, half_of(i, half)],
                       chip_send.at[i, axis, half], chip_recv.at[i, axis, half], peer_of(me, (X, Y)[axis])) for i in range(2)]

    def join_turn(axis, half):
        wait_recv(turn(half))
        for i in range(2):
            part = stage[i][chips + 1 + axis, half * sizes[i]:(half + 1) * sizes[i]].astype(F32)
            stage[i][chips + 1 + axis, half * sizes[i]:(half + 1) * sizes[i]] = (part + turn_in[i][half].astype(F32)).astype(BF16)
        start(chip(axis, half))

    start(loads(peer_of(peer_group(0), PARTNER), 0))
    for step in range(1, DEVICES):
        small_copy(step).start()

    def products(slot):
        tokens = dyb.shape[0] * dyb.shape[1]
        return dot(ob[slot], dyb[...].reshape(tokens, dyb.shape[2]), TN), dot(ht_ref[...], qkvb[slot])

    def body(order, carry):
        mine = peer_group(order)
        other = peer_of(mine, PARTNER)
        start(loads(mine, 1))
        wait(loads(other, 0))
        for i, product in enumerate(products(0)):
            stage[i][order] = product.astype(BF16)
        start(pair(order))

        @pl.when(order < chips - 1)
        def _():
            start(loads(peer_of(peer_group(order + 1), PARTNER), 0))

        wait(loads(mine, 1))
        for i, product in enumerate(products(1)):
            for half in range(2):
                own(i, half)[...] = product[half * sizes[i]:(half + 1) * sizes[i]]
        wait_recv(pair(order))

        @pl.when(order < chips - 1)
        def _():
            for i in range(2):
                for half in range(2):
                    part = slice(half * sizes[i], (half + 1) * sizes[i])
                    stage[i][chips + order, part] = (own(i, half)[...] + pair_in[i][order % 2, part].astype(F32)).astype(BF16)

        @pl.when(order == 0)
        def _():
            start(turn(0))
            start(turn(1))

        @pl.when(order == 1)
        def _():
            start(chip(0, 0))

        @pl.when(order == 2)
        def _():
            start(chip(1, 1))
            join_turn(0, 1)
            join_turn(1, 0)
        return carry

    lax.fori_loop(0, chips, body, 0)

    def spread(half, slot, arrival=False):
        x, y, diag = (peer_of(me, step) for step in (X, Y, DIAG))
        target = (x, y, (y, x)[half], partner, partner, partner, partner)[slot]
        owner = (me, me, (x, y)[half], me, x, y, diag)[slot]
        sender = (x, y, diag, partner, peer_of(partner, X), peer_of(partner, Y), peer_of(partner, DIAG))[slot]
        copies = []
        for i in range(2):
            part = half_of(i, half)
            src = stage[i].at[result, part] if slot in (0, 1, 3) else gathered[i].at[owner, part]
            copies.append(remote(src, gathered[i].at[sender if arrival else owner, part],
                                 all_send.at[i, half, slot], all_recv.at[i, half, slot], target))
        return copies

    for half in range(2):
        for axis in range(2):
            wait_recv(chip(axis, half))
        for i in range(2):
            part = slice(half * sizes[i], (half + 1) * sizes[i])
            total = own(i, half)[...] + pair_in[i][(chips - 1) % 2, part].astype(F32) + chip_in[i][0, part].astype(F32) + chip_in[i][1, part].astype(F32)
            stage[i][result, part] = total.astype(BF16)
        for slot in ((0, 1, 3), (1, 0, 3))[half]:
            start(spread(half, slot))
    local = [pltpu.make_async_copy(stage[i].at[result], gathered[i].at[me], load_sem.at[i, 0]) for i in range(2)]
    start(local)

    for step in range(1, DEVICES):
        small_copy(step, arrival=True).wait_recv()
    smallb[me] = small[...]
    sums = smallb[0]
    for device in range(1, DEVICES):
        sums = sums + smallb[device]
    small_out[...] = sums

    for half, slot, onward in ((0, 0, (2, 4)), (1, 1, (2, 5)), (1, 0, (4,)), (0, 1, (5,)), (0, 2, (6,)), (1, 2, (6,))):
        wait_recv(spread(half, slot, arrival=True))
        for forward in onward:
            start(spread(half, forward))
    wait(local)
    for half in range(2):
        for slot in (3, 4, 5, 6):
            wait_recv(spread(half, slot, arrival=True))
        for slot in range(7):
            wait_send(spread(half, slot))
        wait_send(turn(half))
        for axis in range(2):
            wait_send(chip(axis, half))
    for order in range(chips):
        wait_send(pair(order))
    for step in range(1, DEVICES):
        small_copy(step).wait_send()


def block_call(x, dy, pos, gains, w_q, w_k, w_v, w_o, head_dim):
    batch, piece, model = x.shape
    seqs, seq_len = batch // DEVICES, piece * DEVICES
    q_width, kv_width = w_q.shape[1], w_k.shape[1]
    groups = kv_width // head_dim
    q_cols = q_width // groups
    tokens = seqs * seq_len
    width = q_cols + 2 * head_dim
    fixed = lambda s, g: (0, 0)
    bf = lambda *shape: jax.ShapeDtypeStruct(shape, BF16)
    f32 = lambda *shape: jax.ShapeDtypeStruct(shape, F32)
    anywhere = pl.BlockSpec(memory_space=pl.ANY)
    flops = 4 * tokens * model * (q_width * 2 + kv_width * 2) + 12 * tokens * seq_len * q_width
    vb = lambda *shape: pltpu.VMEM(shape, BF16)
    vf = lambda *shape: pltpu.VMEM(shape, F32)
    dma = lambda *shape: pltpu.SemaphoreType.DMA(shape)
    return pl.pallas_call(
        block_kernel,
        grid=(seqs, groups),
        in_specs=[
            anywhere, anywhere, anywhere, anywhere, anywhere, anywhere, anywhere,
            pl.BlockSpec(gains.shape, fixed),
        ],
        out_specs=[anywhere] * 6 + [pl.BlockSpec((16, head_dim), fixed)],
        out_shape=[
            bf(batch, piece, model), bf(batch, piece, model),
            bf(groups, q_cols, model), bf(groups, model, width),
            bf(groups, tokens, q_cols), bf(groups, tokens, width),
            f32(16, head_dim),
        ],
        scratch_shapes=[
            vb(seqs, seq_len, model), vb(seqs, seq_len, model), vb(2, seq_len, model),
            vf(seqs, DEVICES, 8, head_dim),
            vb(groups, model, width), vb(groups, q_cols, model),
            vb(seq_len, model), vb(model, tokens),
            vf(seq_len, head_dim), vf(seq_len, head_dim), vf(seq_len, head_dim), vf(seq_len, head_dim),
            vf(seq_len, model), vf(seq_len, model),
            vf(seq_len, q_cols), vf(seq_len, head_dim), vb(seq_len, head_dim), vb(seq_len, q_cols),
            vb(seq_len, head_dim), vb(seq_len, q_cols),
            vb(seq_len, q_cols), vb(seq_len, width), vb(seq_len, q_cols), vb(seq_len, width),
            vb(2, seq_len, q_cols), vb(2, seq_len, width),
            vf(1, model), vf(1, head_dim), vf(1, head_dim), vf(16, head_dim), vf(DEVICES, 16, head_dim),
            vb(2, tokens, q_cols), vb(2, tokens, width),
            vb(2, q_cols, model), vb(2, model, width),
            vb(2, q_cols // 2, model), vb(2, model // 2, width),
            vb(2, q_cols, model), vb(2, model, width),
            pltpu.SemaphoreType.DMA((4, groups)),
            pltpu.SemaphoreType.DMA((3, seqs, DEVICES)),
            pltpu.SemaphoreType.DMA((3, seqs, DEVICES)),
            pltpu.SemaphoreType.DMA((2, seqs, DEVICES)),
            pltpu.SemaphoreType.DMA((2, seqs, DEVICES)),
            dma(2, 2), dma(2, 2), dma(2, 4), dma(2, 4), dma(2, 2), dma(2, 2), dma(2, 2, 2), dma(2, 2, 2),
            dma(2, 2, 7), dma(2, 2, 7), dma(DEVICES), dma(DEVICES),
        ],
        compiler_params=pltpu.CompilerParams(
            dimension_semantics=("arbitrary", "arbitrary"), vmem_limit_bytes=67_000_000,
            collective_id=0, has_side_effects=True),
        cost_estimate=pl.CostEstimate(flops=flops, bytes_accessed=50_000_000, transcendentals=tokens * seq_len * 8),
        name="block",
    )(x, dy, pos, w_q, w_k, w_v, w_o, gains)


def widen_kernel(ga_ref, gb_ref, small_ref, wq_ref, wk_ref, wv_ref, wo_ref, dgin_ref, dqn_ref, dkn_ref):
    @pl.when(pl.program_id(0) == 0)
    def _():
        lanes = small_ref.shape[1]
        rows = dgin_ref.shape[1] // lanes
        for row in range(rows):
            dgin_ref[:, row * lanes:(row + 1) * lanes] = small_ref[row:row + 1]
        dqn_ref[...] = small_ref[rows:rows + 1]
        dkn_ref[...] = small_ref[rows + 1:rows + 2]

    q_cols, head_dim = wq_ref.shape[1], wk_ref.shape[1]
    wo_ref[...] = ga_ref[0].astype(F32)
    wq_ref[...] = gb_ref[0, :, :q_cols].astype(F32)
    wk_ref[...] = gb_ref[0, :, q_cols:q_cols + head_dim].astype(F32)
    wv_ref[...] = gb_ref[0, :, q_cols + head_dim:].astype(F32)


def widen_call(ga, gb, small):
    groups, q_cols, model = ga.shape
    head_dim = (gb.shape[2] - q_cols) // 2
    f32 = lambda *shape: jax.ShapeDtypeStruct(shape, F32)
    across = lambda g: (0, g)
    return pl.pallas_call(
        widen_kernel,
        grid=(groups,),
        in_specs=[pl.BlockSpec((1, q_cols, model), lambda g: (g, 0, 0)),
                  pl.BlockSpec((1, model, gb.shape[2]), lambda g: (g, 0, 0)),
                  pl.BlockSpec(small.shape, lambda g: (0, 0))],
        out_specs=[pl.BlockSpec((model, q_cols), across), pl.BlockSpec((model, head_dim), across),
                   pl.BlockSpec((model, head_dim), across), pl.BlockSpec((q_cols, model), lambda g: (g, 0))]
        + [pl.BlockSpec((1, n), lambda g: (0, 0)) for n in (model, head_dim, head_dim)],
        out_shape=[f32(model, groups * q_cols), f32(model, groups * head_dim), f32(model, groups * head_dim),
                   f32(groups * q_cols, model), f32(1, model), f32(1, head_dim), f32(1, head_dim)],
        compiler_params=pltpu.CompilerParams(dimension_semantics=("arbitrary",)),
        name="widen",
    )(ga, gb, small)


def solution(mesh):
    seq_spec = P(None, 'sp', None)
    replicated = P()

    def shard_body(hidden_in, grad_out, positions, w_q, w_k, w_v, w_o, g_in, q_norm, k_norm):
        batch, seq_dev, model_dim = hidden_in.shape
        head_dim = q_norm.shape[0]
        exponents = jnp.arange(0, head_dim, 2).astype(F32) / head_dim
        inv_freq = jnp.power(ROPE_THETA, -exponents)
        gains = jnp.concatenate([g_in.astype(F32), q_norm.astype(F32), k_norm.astype(F32), inv_freq, inv_freq])[None]
        pos = jnp.broadcast_to(jnp.pad(positions.astype(F32), ((0, 0), (0, head_dim - seq_dev)))[:, None, :], (batch, 8, head_dim))
        hidden_out, grad_in, ga, gb, _, _, small = block_call(hidden_in, grad_out, pos, gains, w_q, w_k, w_v, w_o, head_dim)
        grad_wq, grad_wk, grad_wv, grad_wo, dgin, dqn, dkn = widen_call(ga, gb, small)
        return hidden_out, grad_in, grad_wq, grad_wk, grad_wv, grad_wo, dgin[0], dqn[0], dkn[0]

    return jax.shard_map(shard_body, mesh=mesh,
                         in_specs=(seq_spec, seq_spec, P(None, 'sp'), replicated, replicated, replicated, replicated, replicated, replicated, replicated),
                         out_specs=(seq_spec, seq_spec, replicated, replicated, replicated, replicated, replicated, replicated, replicated),
                         check_vma=False)
```

```python
import functools
import jax
import jax.numpy as jnp
from jax import lax
from jax.experimental import pallas as pl
from jax.experimental.pallas import tpu as pltpu
from jax.sharding import PartitionSpec as P

EPSILON = 1e-6
ROPE_THETA = 1000000.0
NEG_LARGE = -1e30
LOG2_E = 1.4426950408889634
NT = (((1,), (1,)), ((), ()))
TN = (((0,), (0,)), ((), ()))
ROW_BLOCK = 256
DEVICES = 8
BF16 = jnp.bfloat16
F32 = jnp.float32


def dot(a, b, dims=(((1,), (0,)), ((), ()))):
    return lax.dot_general(a, b, dims, preferred_element_type=F32)


def peer_of(me, step):
    core, x, y = me % 2, (me // 2) % 2, me // 4
    return ((y + step // 4) % 2) * 4 + ((x + (step // 2) % 2) % 2) * 2 + (core + step % 2) % 2


X, Y, DIAG, PARTNER = 2, 4, 6, 1


def chip_peer(me, order):
    return peer_of(me, (1 - order // 2) * X + ((order + 1) % 2) * Y)


def group_at(me, place):
    return peer_of(chip_peer(me, place // 2), 1 - place % 2)


def entry_barrier(me):
    barrier = pltpu.get_barrier_semaphore()
    for step in range(1, DEVICES):
        pl.semaphore_signal(barrier, inc=1, device_id=(peer_of(me, step),), device_id_type=pl.DeviceIdType.MESH)
    pl.semaphore_wait(barrier, DEVICES - 1)


def remote(src, dst, send, recv, device):
    return pltpu.make_async_remote_copy(src_ref=src, dst_ref=dst, send_sem=send, recv_sem=recv,
                                        device_id=(device,), device_id_type=pl.DeviceIdType.MESH)


def block_kernel(x_hbm, dy_hbm, pos_hbm, wq_hbm, wk_hbm, wv_hbm, wo_hbm, gains_ref,
                 out_hbm, gi_hbm, ga_hbm, gb_hbm, o_hbm, dqkv_hbm, small_out,
                 xb, dyb, gib, posb, wqkv, wo, h_ref, ht_ref, rope_cos, rope_sin, next_cos, next_sin, out_acc, dh_acc,
                 q_next, k_next, v_next, do_next, v_now, do_now, o_now, dqkv_now, o_last, dqkv_last, o_stage, dqkv_stage,
                 dgin_ref, dqn_ref, dkn_ref, small, smallb, ob, qkvb, l1a, l1b, t_a, t_b, l2a, l2b,
                 weight_sem, in_send, in_recv, out_send, out_recv, store_sem, load_sem, pair_send, pair_recv,
                 turn_send, turn_recv, chip_send, chip_recv, all_send, all_recv, small_send, small_recv):
    seq, group = pl.program_id(0), pl.program_id(1)
    seqs, groups = pl.num_programs(0), pl.num_programs(1)
    me = lax.axis_index('sp')
    head_dim, model = dqn_ref.shape[1], dgin_ref.shape[1]
    gin_ref = gains_ref.at[:, pl.ds(0, model)]
    qn_ref, kn_ref, freq_ref = (gains_ref.at[:, pl.ds(model + i * head_dim, head_dim)] for i in range(3))
    q_cols = o_now.shape[1]
    per_kv = q_cols // head_dim
    seq_len = xb.shape[1]
    piece = seq_len // DEVICES
    scale = head_dim ** -0.5
    half = head_dim // 2
    tiles = [slice(i, i + ROW_BLOCK) for i in range(0, seq_len, ROW_BLOCK)]

    def rows_of(device):
        return pl.ds(pl.multiple_of(device * piece, piece), piece)

    def incoming(kind, s, step, arrival=False):
        peer = peer_of(me, step)
        src = (x_hbm, dy_hbm, pos_hbm)[kind].at[DEVICES * s + peer]

        def landing(device):
            return posb.at[s, device] if kind == 2 else (xb, dyb)[kind].at[s, rows_of(device)]

        if step == 0:
            return pltpu.make_async_copy(src, landing(me), in_recv.at[kind, s, 0])
        return remote(src, landing(peer if arrival else me), in_send.at[kind, s, step], in_recv.at[kind, s, step], peer)

    def outgoing(kind, s, step, arrival=False):
        peer = peer_of(me, step)
        src = xb.at[s, rows_of(peer)] if kind == 0 else gib.at[s % 2, rows_of(peer)]
        dst = (out_hbm, gi_hbm)[kind]
        if step == 0:
            return pltpu.make_async_copy(src, dst.at[DEVICES * s + me], out_recv.at[kind, s, 0])
        return remote(src, dst.at[DEVICES * s + (peer if arrival else me)],
                      out_send.at[kind, s, step], out_recv.at[kind, s, step], peer)

    def sent(kind, s):
        outgoing(kind, s, 0).wait()
        for step in range(1, DEVICES):
            outgoing(kind, s, step).wait_send()

    def weight_loads():
        copies = []
        for place in range(DEVICES):
            g = group_at(me, place)
            wide = pl.ds(pl.multiple_of(g * q_cols, q_cols), q_cols)
            narrow = pl.ds(pl.multiple_of(g * head_dim, head_dim), head_dim)
            parts = ((wq_hbm.at[:, wide], wqkv.at[place, :, pl.ds(0, q_cols)]),
                     (wk_hbm.at[:, narrow], wqkv.at[place, :, pl.ds(q_cols, head_dim)]),
                     (wv_hbm.at[:, narrow], wqkv.at[place, :, pl.ds(q_cols + head_dim, head_dim)]),
                     (wo_hbm.at[wide], wo.at[place]))
            copies += [pltpu.make_async_copy(src, dst, weight_sem.at[i, place]) for i, (src, dst) in enumerate(parts)]
        return copies

    def arrive(kind, s):
        for step in range(DEVICES):
            if step == 0:
                incoming(kind, s, 0).wait()
            else:
                incoming(kind, s, step, arrival=True).wait_recv()

    def prepare(s):
        arrive(2, s)
        on_diag = lax.broadcasted_iota(jnp.int32, (piece, head_dim), 0) == lax.broadcasted_iota(jnp.int32, (piece, head_dim), 1)
        low = lax.broadcasted_iota(jnp.int32, (piece, head_dim), 1) < half
        half_count = DEVICES // 2

        def column(device):
            row = jnp.broadcast_to(posb[s, device, 0:1, :], (piece, head_dim))
            return jnp.sum(jnp.where(on_diag, row, 0.0), axis=-1, keepdims=True)

        for device in range(half_count):
            angles = jnp.where(low, column(device), column(device + half_count)) * freq_ref[...]
            cos, sin = jnp.cos(angles), jnp.sin(angles)
            cos_turned, sin_turned = pltpu.roll(cos, half, 1), pltpu.roll(sin, half, 1)
            first = slice(device * piece, (device + 1) * piece)
            second = slice((device + half_count) * piece, (device + half_count + 1) * piece)
            next_cos[first, :] = jnp.where(low, cos, cos_turned)
            next_sin[first, :] = jnp.where(low, -sin, sin_turned)
            next_cos[second, :] = jnp.where(low, cos_turned, cos)
            next_sin[second, :] = jnp.where(low, -sin_turned, sin)
        arrive(0, s)
        x = xb[s].astype(F32)
        inv = lax.rsqrt(jnp.mean(x * x, axis=-1, keepdims=True) + EPSILON)
        h_ref[...] = (x * inv * gin_ref[...]).astype(BF16)
        arrive(1, s)

    def project(s, g):
        def q_rows(rows):
            q_next[rows] = dot(h_ref[rows], wqkv[g, :, :q_cols])

        def kv_rows(rows):
            kv = dot(h_ref[rows], wqkv[g, :, q_cols:])
            k_next[rows] = kv[:, :head_dim]
            v_next[rows] = kv[:, head_dim:].astype(BF16)

        def do_rows(rows):
            do_next[rows] = dot(dyb[s, rows], wo[g], NT).astype(BF16)

        return [functools.partial(f, rows) for f in (q_rows, kv_rows, do_rows) for rows in tiles]

    def accumulate(g):
        def out_cols(cols):
            out_acc[:, cols] += dot(o_last[...], wo[g, :, cols])

        def dh_cols(cols):
            dh_acc[:, cols] += dot(dqkv_last[...], wqkv[g, cols, :], NT)

        columns = [slice(c, c + 256) for c in range(0, out_acc.shape[1], 256)]
        return [functools.partial(f, cols) for f in (out_cols, dh_cols) for cols in columns]

    def run(products):
        for product in products:
            product()

    def finish(s):
        x = xb[s].astype(F32)
        inv = lax.rsqrt(jnp.mean(x * x, axis=-1, keepdims=True) + EPSILON)
        unit = x * inv
        xb[s] = (x + out_acc[...]).astype(BF16)
        d_norm = dh_acc[...]
        dgin_ref[...] += jnp.sum(d_norm * unit, axis=0, keepdims=True)
        d_unit = d_norm * gin_ref[...]
        grad = inv * (d_unit - unit * jnp.mean(d_unit * unit, axis=-1, keepdims=True))

        @pl.when(s >= 2)
        def _():
            sent(1, s - 2)

        gib[s % 2] = (dyb[s].astype(F32) + grad).astype(BF16)
        for kind in range(2):
            for step in (2, 4, 6, 3, 5, 7, 1, 0):
                outgoing(kind, s, step).start()

    @pl.when((seq == 0) & (group == 0))
    def _():
        entry_barrier(me)

        def send_all(s, carry):
            for kind in (2, 0, 1):
                for step in (2, 4, 6, 3, 5, 7, 1, 0):
                    incoming(kind, s, step).start()
            return carry

        lax.fori_loop(0, seqs, send_all, 0)
        for copy in weight_loads():
            copy.start()
        dgin_ref[...] = jnp.zeros_like(dgin_ref)
        dqn_ref[...] = jnp.zeros_like(dqn_ref)
        dkn_ref[...] = jnp.zeros_like(dkn_ref)
        o_now[...] = jnp.zeros_like(o_now)
        dqkv_now[...] = jnp.zeros_like(dqkv_now)
        out_acc[...] = jnp.zeros_like(out_acc)
        dh_acc[...] = jnp.zeros_like(dh_acc)
        for copy in weight_loads():
            copy.wait()
        prepare(0)
        run(project(0, 0))

    @pl.when(group == 0)
    def _():
        rope_cos[...] = next_cos[...]
        rope_sin[...] = next_sin[...]
        ht_ref[:, pl.ds(pl.multiple_of(seq * seq_len, seq_len), seq_len)] = h_ref[...].T

    last_group = group == groups - 1

    @pl.when(last_group & (seq < seqs - 1))
    def _():
        prepare(seq + 1)

    cos, sin = rope_cos[...], rope_sin[...]

    def norm_rotate(t, gain):
        inv = lax.rsqrt(jnp.mean(t * t, axis=-1, keepdims=True) + EPSILON)
        unit = t * inv
        scaled = unit * gain
        return (scaled * cos + pltpu.roll(scaled, half, 1) * sin).astype(BF16), unit, inv

    def norm_rotate_back(grad, unit, inv, gain):
        d_scaled = grad * cos - pltpu.roll(grad, half, 1) * sin
        d_gain = jnp.sum(d_scaled * unit, axis=0, keepdims=True)
        d_unit = d_scaled * gain
        return inv * (d_unit - unit * jnp.mean(d_unit * unit, axis=-1, keepdims=True)), d_gain

    step_id = seq * groups + group
    slot = step_id % 2

    def stores(step):
        g, rows = step % groups, pl.ds(pl.multiple_of((step // groups) * seq_len, seq_len), seq_len)
        return [pltpu.make_async_copy(o_stage.at[step % 2], o_hbm.at[g, rows], store_sem.at[0, step % 2]),
                pltpu.make_async_copy(dqkv_stage.at[step % 2], dqkv_hbm.at[g, rows], store_sem.at[1, step % 2])]

    stored = (seqs - 1) * groups

    @pl.when((step_id >= 2) & (step_id - 2 < stored))
    def _():
        for copy in stores(step_id - 2):
            copy.wait()

    @pl.when((step_id >= 1) & (step_id - 1 < stored))
    def _():
        for copy in stores(step_id - 1):
            copy.start()

    v_now[...] = v_next[...]
    do_now[...] = do_next[...]
    o_last[...] = o_now[...]
    dqkv_last[...] = dqkv_now[...]

    ahead = project(jnp.minimum(seq + last_group.astype(jnp.int32), seqs - 1), (group + 1) % groups)
    behind = accumulate((group + groups - 1) % groups)
    lanes = [slice(head * head_dim, (head + 1) * head_dim) for head in range(per_kv)]
    stacked = per_kv * ROW_BLOCK
    rows_id = lax.broadcasted_iota(jnp.int32, (stacked, ROW_BLOCK), 0) % ROW_BLOCK
    causal = rows_id >= lax.broadcasted_iota(jnp.int32, (stacked, ROW_BLOCK), 1)
    blocks = len(tiles)

    run(behind[:6])
    k_rot, k_unit, k_inv = norm_rotate(k_next[...], kn_ref[...])
    q_parts = [norm_rotate(q_next[:, lane], qn_ref[...]) for lane in lanes]
    q_tile = [jnp.concatenate([part[0][tile] for part in q_parts], axis=0) for tile in tiles]
    do_tile = [jnp.concatenate([do_now[tile, lane] for lane in lanes], axis=0) for tile in tiles]

    def scores(i):
        s_parts = [dot(q_tile[i], k_rot[tiles[j]], NT) for j in range(i + 1)]
        s_parts[i] = jnp.where(causal, s_parts[i], NEG_LARGE)
        return s_parts

    def softmax(s_parts):
        top = functools.reduce(jnp.maximum, [jnp.max(s, axis=-1, keepdims=True) for s in s_parts])
        e_parts = [jnp.exp2((s - top) * (scale * LOG2_E)) for s in s_parts]
        recip = 1.0 / functools.reduce(jnp.add, [jnp.sum(e, axis=-1, keepdims=True) for e in e_parts])
        p_parts = [e * recip for e in e_parts]
        return p_parts, [p.astype(BF16) for p in p_parts]

    def softmax_back(p_parts, dp_parts):
        delta = functools.reduce(jnp.add, [jnp.sum(p * dp, axis=-1, keepdims=True) for p, dp in zip(p_parts, dp_parts)])
        return [(p * (dp - delta)).astype(BF16) for p, dp in zip(p_parts, dp_parts)]

    def rows_sum(parts, values):
        return functools.reduce(jnp.add, [dot(part, values[tiles[j]]) for j, part in enumerate(parts)])

    def store_output(i, o_i):
        for head, lane in enumerate(lanes):
            o_head = o_i[head * ROW_BLOCK:(head + 1) * ROW_BLOCK].astype(BF16)
            o_stage[slot, tiles[i], lane] = o_head
            o_now[tiles[i], lane] = o_head

    fill = [ahead[0:2], behind[6:7], behind[7:8] + ahead[2:3], ahead[3:4]]
    dp_all = [[dot(do_tile[i], v_now[tiles[j]], NT) for j in range(i + 1)] for i in range(blocks)]
    s_all = [scores(i) for i in range(blocks)]
    dk_parts, dv_parts, dq_tile = [None] * blocks, [None] * blocks, []
    for i in range(blocks):
        p_parts, pb_parts = softmax(s_all[i])
        run(fill[2 * i])
        store_output(i, rows_sum(pb_parts, v_now))
        for j in range(i + 1):
            dv_j = dot(pb_parts[j], do_tile[i], TN)
            dv_parts[j] = dv_j if dv_parts[j] is None else dv_parts[j] + dv_j
        ds_parts = softmax_back(p_parts, dp_all[i])
        run(fill[2 * i + 1])
        dq_tile.append(rows_sum(ds_parts, k_rot))
        for j in range(i + 1):
            dk_j = dot(ds_parts[j], q_tile[i], TN)
            dk_parts[j] = dk_j if dk_parts[j] is None else dk_parts[j] + dk_j
    run(ahead[4:])
    for head, lane in enumerate(lanes):
        dq_head = jnp.concatenate([dq[head * ROW_BLOCK:(head + 1) * ROW_BLOCK] for dq in dq_tile], axis=0)
        dq_head, d_gain = norm_rotate_back(dq_head * scale, q_parts[head][1], q_parts[head][2], qn_ref[...])
        dqn_ref[...] += d_gain
        dq_head = dq_head.astype(BF16)
        dqkv_stage[slot, :, lane] = dq_head
        dqkv_now[:, lane] = dq_head
    dk_head, d_gain = norm_rotate_back(jnp.concatenate(dk_parts, axis=0) * scale, k_unit, k_inv, kn_ref[...])
    dkn_ref[...] += d_gain
    dk_head = dk_head.astype(BF16)
    dqkv_stage[slot, :, q_cols:q_cols + head_dim] = dk_head
    dqkv_now[:, q_cols:q_cols + head_dim] = dk_head
    dv_head = jnp.concatenate(dv_parts, axis=0).astype(BF16)
    dqkv_stage[slot, :, q_cols + head_dim:] = dv_head
    dqkv_now[:, q_cols + head_dim:] = dv_head

    @pl.when((group == 0) & (seq > 0))
    def _():
        finish(seq - 1)
        out_acc[...] = jnp.zeros_like(out_acc)
        dh_acc[...] = jnp.zeros_like(dh_acc)

    reducer = GradientReducer(me, (ga_hbm, gb_hbm), o_hbm, dqkv_hbm, small_out, dyb, ht_ref, wo, wqkv,
                              dgin_ref, dqn_ref, dkn_ref, small, smallb, ob, qkvb, o_now, dqkv_now, (l1a, l1b), (t_a, t_b), (l2a, l2b),
                              load_sem, pair_send, pair_recv, turn_send, turn_recv, chip_send, chip_recv,
                              all_send, all_recv, small_send, small_recv)
    last_seq = seq == seqs - 1

    @pl.when(last_seq & (group == 0))
    def _():
        start(reducer.loads(0))

    @pl.when(last_seq & (group < groups - 1))
    def _():
        reducer.step(group)

    @pl.when(last_seq & last_group)
    def _():
        o_last[...] = o_now[...]
        dqkv_last[...] = dqkv_now[...]
        run(accumulate(groups - 1))
        finish(seqs - 1)
        reducer.step(groups - 1)
        reducer.finish()

        def drain(s, carry):
            for step in range(1, DEVICES):
                for kind in range(3):
                    incoming(kind, s, step).wait_send()
                for kind in range(2):
                    outgoing(kind, s, step, arrival=True).wait_recv()
            sent(0, s)
            return carry

        lax.fori_loop(0, seqs, drain, 0)
        for s in range(2):
            sent(1, seqs - 2 + s)


def start(copies):
    for copy in copies:
        copy.start()


def wait_send(copies):
    for copy in copies:
        copy.wait_send()


def wait_recv(copies):
    for copy in copies:
        copy.wait_recv()


class GradientReducer:
    def __init__(self, me, gathered, o_hbm, dqkv_hbm, small_out, dyb, ht_ref, wo, wqkv, dgin_ref, dqn_ref, dkn_ref,
                 small, smallb, ob, qkvb, o_now, dqkv_now, pair_in, turn_in, chip_in, load_sem, pair_send, pair_recv,
                 turn_send, turn_recv, chip_send, chip_recv, all_send, all_recv, small_send, small_recv):
        self.__dict__.update({k: v for k, v in locals().items() if k != 'self'})
        self.partner = peer_of(me, PARTNER)
        self.chips = DEVICES // 2
        self.stage = (wo, wqkv)
        self.sizes = [ref.shape[1] // 2 for ref in self.stage]
        self.early = ob.shape[0] - o_now.shape[0]

    def slot(self, place):
        return (place + DEVICES) % (DEVICES + 1)

    def half_of(self, i, half):
        return pl.ds(half * self.sizes[i], self.sizes[i])

    def loads(self, place):
        rows = pl.ds(0, self.early)
        return [pltpu.make_async_copy(self.o_hbm.at[place], self.ob.at[rows], self.load_sem.at[0]),
                pltpu.make_async_copy(self.dqkv_hbm.at[place], self.qkvb.at[rows], self.load_sem.at[1])]

    def pair(self, order):
        return [remote(self.stage[i].at[self.slot(2 * order)], self.pair_in[i].at[order % 2],
                       self.pair_send.at[i, order], self.pair_recv.at[i, order], self.partner) for i in range(2)]

    def turn(self, half):
        return [remote(self.stage[i].at[self.slot(1), self.half_of(i, half)], self.turn_in[i].at[half],
                       self.turn_send.at[i, half], self.turn_recv.at[i, half], peer_of(self.me, (X, Y)[half])) for i in range(2)]

    def chip(self, axis, half):
        return [remote(self.stage[i].at[self.slot(2 * axis + 3), self.half_of(i, half)], self.chip_in[i].at[axis, self.half_of(i, half)],
                       self.chip_send.at[i, axis, half], self.chip_recv.at[i, axis, half], peer_of(self.me, (X, Y)[axis])) for i in range(2)]

    def join_turn(self, axis, half):
        wait_recv(self.turn(half))
        for i in range(2):
            part = self.stage[i].at[self.slot(2 * axis + 3), self.half_of(i, half)]
            part[...] = (part[...].astype(F32) + self.turn_in[i][half].astype(F32)).astype(BF16)
        start(self.chip(axis, half))

    def step(self, place):
        for copy in self.loads(place):
            copy.wait()
        self.ob[self.early:] = self.o_now[...]
        self.qkvb[self.early:] = self.dqkv_now[...]
        tokens = self.ob.shape[0]
        into = self.slot(place)
        self.stage[0][into] = dot(self.ob[...], self.dyb[...].reshape(tokens, self.dyb.shape[2]), TN).astype(BF16)
        self.stage[1][into] = dot(self.ht_ref[...], self.qkvb[...]).astype(BF16)
        order = place // 2

        @pl.when(place < DEVICES - 1)
        def _():
            start(self.loads(place + 1))

        @pl.when(place % 2 == 0)
        def _():
            start(self.pair(order))

        @pl.when(place % 2 == 1)
        def _():
            wait_recv(self.pair(order))
            for i in range(2):
                for half in range(2):
                    part = self.stage[i].at[into, self.half_of(i, half)]
                    part[...] = (part[...].astype(F32) + self.pair_in[i][order % 2, self.half_of(i, half)].astype(F32)).astype(BF16)

        @pl.when(place == 1)
        def _():
            start(self.turn(0))
            start(self.turn(1))

        @pl.when(place == 3)
        def _():
            start(self.chip(0, 0))

        @pl.when(place == 5)
        def _():
            start(self.chip(1, 1))
            self.join_turn(0, 1)
            self.join_turn(1, 0)

    def small_copy(self, step, arrival=False):
        peer = peer_of(self.me, step)
        return remote(self.small, self.smallb.at[peer if arrival else self.me], self.small_send.at[step], self.small_recv.at[step], peer)

    def spread(self, half, slot, arrival=False):
        me, partner = self.me, self.partner
        x, y, diag = (peer_of(me, step) for step in (X, Y, DIAG))
        target = (x, y, (y, x)[half], partner, partner, partner, partner)[slot]
        owner = (me, me, (x, y)[half], me, x, y, diag)[slot]
        sender = (x, y, diag, partner, peer_of(partner, X), peer_of(partner, Y), peer_of(partner, DIAG))[slot]
        copies = []
        for i in range(2):
            part = self.half_of(i, half)
            src = self.stage[i].at[self.slot(DEVICES - 1), part] if slot in (0, 1, 3) else self.gathered[i].at[owner, part]
            copies.append(remote(src, self.gathered[i].at[sender if arrival else owner, part],
                                 self.all_send.at[i, half, slot], self.all_recv.at[i, half, slot], target))
        return copies

    def finish(self):
        small, smallb, spread = self.small, self.smallb, self.spread
        small[...] = jnp.zeros_like(small)
        lanes = self.dqn_ref.shape[1]
        rows = self.dgin_ref.shape[1] // lanes
        for row in range(rows):
            small[row:row + 1] = self.dgin_ref[:, row * lanes:(row + 1) * lanes]
        small[rows:rows + 1] = self.dqn_ref[...]
        small[rows + 1:rows + 2] = self.dkn_ref[...]
        for step in range(1, DEVICES):
            self.small_copy(step).start()

        result = self.slot(DEVICES - 1)
        for half in range(2):
            for axis in range(2):
                wait_recv(self.chip(axis, half))
            for i in range(2):
                rows_half = self.half_of(i, half)
                part = self.stage[i].at[result, rows_half]
                total = part[...].astype(F32) + self.chip_in[i][0, rows_half].astype(F32) + self.chip_in[i][1, rows_half].astype(F32)
                part[...] = total.astype(BF16)
            for slot in ((0, 1, 3), (1, 0, 3))[half]:
                start(spread(half, slot))
        local = [pltpu.make_async_copy(self.stage[i].at[result], self.gathered[i].at[self.me], self.load_sem.at[i]) for i in range(2)]
        start(local)

        for step in range(1, DEVICES):
            self.small_copy(step, arrival=True).wait_recv()
        smallb[self.me] = small[...]
        sums = smallb[0]
        for device in range(1, DEVICES):
            sums = sums + smallb[device]
        self.small_out[...] = sums

        for half, slot, onward in ((0, 0, (2, 4)), (1, 1, (2, 5)), (1, 0, (4,)), (0, 1, (5,)), (0, 2, (6,)), (1, 2, (6,))):
            wait_recv(spread(half, slot, arrival=True))
            for forward in onward:
                start(spread(half, forward))
        for copy in local:
            copy.wait()
        for half in range(2):
            for slot in (3, 4, 5, 6):
                wait_recv(spread(half, slot, arrival=True))
            for slot in range(7):
                wait_send(spread(half, slot))
            wait_send(self.turn(half))
            for axis in range(2):
                wait_send(self.chip(axis, half))
        for order in range(self.chips):
            wait_send(self.pair(order))
        for step in range(1, DEVICES):
            self.small_copy(step).wait_send()


def block_call(x, dy, pos, gains, w_q, w_k, w_v, w_o, head_dim):
    batch, piece, model = x.shape
    seqs, seq_len = batch // DEVICES, piece * DEVICES
    q_width, kv_width = w_q.shape[1], w_k.shape[1]
    groups = kv_width // head_dim
    q_cols = q_width // groups
    tokens = seqs * seq_len
    width = q_cols + 2 * head_dim
    fixed = lambda s, g: (0, 0)
    bf = lambda *shape: jax.ShapeDtypeStruct(shape, BF16)
    f32 = lambda *shape: jax.ShapeDtypeStruct(shape, F32)
    anywhere = pl.BlockSpec(memory_space=pl.ANY)
    flops = 4 * tokens * model * (q_width * 2 + kv_width * 2) + 12 * tokens * seq_len * q_width
    vb = lambda *shape: pltpu.VMEM(shape, BF16)
    vf = lambda *shape: pltpu.VMEM(shape, F32)
    dma = lambda *shape: pltpu.SemaphoreType.DMA(shape)
    return pl.pallas_call(
        block_kernel,
        grid=(seqs, groups),
        in_specs=[
            anywhere, anywhere, anywhere, anywhere, anywhere, anywhere, anywhere,
            pl.BlockSpec(gains.shape, fixed),
        ],
        out_specs=[anywhere] * 6 + [pl.BlockSpec((16, head_dim), fixed)],
        out_shape=[
            bf(batch, piece, model), bf(batch, piece, model),
            bf(groups, q_cols, model), bf(groups, model, width),
            bf(groups, tokens - seq_len, q_cols), bf(groups, tokens - seq_len, width),
            f32(16, head_dim),
        ],
        scratch_shapes=[
            vb(seqs, seq_len, model), vb(seqs, seq_len, model), vb(2, seq_len, model),
            vf(seqs, DEVICES, 8, head_dim),
            vb(groups + 1, model, width), vb(groups + 1, q_cols, model),
            vb(seq_len, model), vb(model, tokens),
            vf(seq_len, head_dim), vf(seq_len, head_dim), vf(seq_len, head_dim), vf(seq_len, head_dim),
            vf(seq_len, model), vf(seq_len, model),
            vf(seq_len, q_cols), vf(seq_len, head_dim), vb(seq_len, head_dim), vb(seq_len, q_cols),
            vb(seq_len, head_dim), vb(seq_len, q_cols),
            vb(seq_len, q_cols), vb(seq_len, width), vb(seq_len, q_cols), vb(seq_len, width),
            vb(2, seq_len, q_cols), vb(2, seq_len, width),
            vf(1, model), vf(1, head_dim), vf(1, head_dim), vf(16, head_dim), vf(DEVICES, 16, head_dim),
            vb(tokens, q_cols), vb(tokens, width),
            vb(2, q_cols, model), vb(2, model, width),
            vb(2, q_cols // 2, model), vb(2, model // 2, width),
            vb(2, q_cols, model), vb(2, model, width),
            pltpu.SemaphoreType.DMA((4, groups)),
            pltpu.SemaphoreType.DMA((3, seqs, DEVICES)),
            pltpu.SemaphoreType.DMA((3, seqs, DEVICES)),
            pltpu.SemaphoreType.DMA((2, seqs, DEVICES)),
            pltpu.SemaphoreType.DMA((2, seqs, DEVICES)),
            dma(2, 2), dma(2), dma(2, 4), dma(2, 4), dma(2, 2), dma(2, 2), dma(2, 2, 2), dma(2, 2, 2),
            dma(2, 2, 7), dma(2, 2, 7), dma(DEVICES), dma(DEVICES),
        ],
        compiler_params=pltpu.CompilerParams(
            dimension_semantics=("arbitrary", "arbitrary"), vmem_limit_bytes=67_000_000,
            collective_id=0, has_side_effects=True),
        cost_estimate=pl.CostEstimate(flops=flops, bytes_accessed=50_000_000, transcendentals=tokens * seq_len * 8),
        name="block",
    )(x, dy, pos, w_q, w_k, w_v, w_o, gains)


def widen_kernel(ga_ref, gb_ref, small_ref, wq_ref, wk_ref, wv_ref, wo_ref, dgin_ref, dqn_ref, dkn_ref):
    @pl.when(pl.program_id(0) == 0)
    def _():
        lanes = small_ref.shape[1]
        rows = dgin_ref.shape[1] // lanes
        for row in range(rows):
            dgin_ref[:, row * lanes:(row + 1) * lanes] = small_ref[row:row + 1]
        dqn_ref[...] = small_ref[rows:rows + 1]
        dkn_ref[...] = small_ref[rows + 1:rows + 2]

    q_cols, head_dim = wq_ref.shape[1], wk_ref.shape[1]
    wo_ref[...] = ga_ref[0].astype(F32)
    wq_ref[...] = gb_ref[0, :, :q_cols].astype(F32)
    wk_ref[...] = gb_ref[0, :, q_cols:q_cols + head_dim].astype(F32)
    wv_ref[...] = gb_ref[0, :, q_cols + head_dim:].astype(F32)


def widen_call(ga, gb, small):
    groups, q_cols, model = ga.shape
    head_dim = (gb.shape[2] - q_cols) // 2
    f32 = lambda *shape: jax.ShapeDtypeStruct(shape, F32)
    across = lambda g: (0, g)
    return pl.pallas_call(
        widen_kernel,
        grid=(groups,),
        in_specs=[pl.BlockSpec((1, q_cols, model), lambda g: (g, 0, 0)),
                  pl.BlockSpec((1, model, gb.shape[2]), lambda g: (g, 0, 0)),
                  pl.BlockSpec(small.shape, lambda g: (0, 0))],
        out_specs=[pl.BlockSpec((model, q_cols), across), pl.BlockSpec((model, head_dim), across),
                   pl.BlockSpec((model, head_dim), across), pl.BlockSpec((q_cols, model), lambda g: (g, 0))]
        + [pl.BlockSpec((1, n), lambda g: (0, 0)) for n in (model, head_dim, head_dim)],
        out_shape=[f32(model, groups * q_cols), f32(model, groups * head_dim), f32(model, groups * head_dim),
                   f32(groups * q_cols, model), f32(1, model), f32(1, head_dim), f32(1, head_dim)],
        compiler_params=pltpu.CompilerParams(dimension_semantics=("arbitrary",)),
        name="widen",
    )(ga, gb, small)


def solution(mesh):
    seq_spec = P(None, 'sp', None)
    replicated = P()

    def shard_body(hidden_in, grad_out, positions, w_q, w_k, w_v, w_o, g_in, q_norm, k_norm):
        batch, seq_dev, model_dim = hidden_in.shape
        head_dim = q_norm.shape[0]
        exponents = jnp.arange(0, head_dim, 2).astype(F32) / head_dim
        inv_freq = jnp.power(ROPE_THETA, -exponents)
        gains = jnp.concatenate([g_in.astype(F32), q_norm.astype(F32), k_norm.astype(F32), inv_freq, inv_freq])[None]
        pos = jnp.broadcast_to(jnp.pad(positions.astype(F32), ((0, 0), (0, head_dim - seq_dev)))[:, None, :], (batch, 8, head_dim))
        hidden_out, grad_in, ga, gb, _, _, small = block_call(hidden_in, grad_out, pos, gains, w_q, w_k, w_v, w_o, head_dim)
        grad_wq, grad_wk, grad_wv, grad_wo, dgin, dqn, dkn = widen_call(ga, gb, small)
        return hidden_out, grad_in, grad_wq, grad_wk, grad_wv, grad_wo, dgin[0], dqn[0], dkn[0]

    return jax.shard_map(shard_body, mesh=mesh,
                         in_specs=(seq_spec, seq_spec, P(None, 'sp'), replicated, replicated, replicated, replicated, replicated, replicated, replicated),
                         out_specs=(seq_spec, seq_spec, replicated, replicated, replicated, replicated, replicated, replicated, replicated),
                         check_vma=False)
```

```python
import functools
import jax
import jax.numpy as jnp
from jax import lax
from jax.experimental import pallas as pl
from jax.experimental.pallas import tpu as pltpu
from jax.sharding import PartitionSpec as P

EPSILON = 1e-6
ROPE_THETA = 1000000.0
NEG_LARGE = -1e30
LOG2_E = 1.4426950408889634
NT = (((1,), (1,)), ((), ()))
TN = (((0,), (0,)), ((), ()))
ROW_BLOCK = 256
DEVICES = 8
BF16 = jnp.bfloat16
F32 = jnp.float32


def dot(a, b, dims=(((1,), (0,)), ((), ()))):
    return lax.dot_general(a, b, dims, preferred_element_type=F32)


def peer_of(me, step):
    core, x, y = me % 2, (me // 2) % 2, me // 4
    return ((y + step // 4) % 2) * 4 + ((x + (step // 2) % 2) % 2) * 2 + (core + step % 2) % 2


X, Y, DIAG, PARTNER = 2, 4, 6, 1


def chip_peer(me, order):
    return peer_of(me, (1 - order // 2) * X + ((order + 1) % 2) * Y)


def group_at(me, place):
    return peer_of(chip_peer(me, place // 2), 1 - place % 2)


def entry_barrier(me):
    barrier = pltpu.get_barrier_semaphore()
    for step in range(1, DEVICES):
        pl.semaphore_signal(barrier, inc=1, device_id=(peer_of(me, step),), device_id_type=pl.DeviceIdType.MESH)
    pl.semaphore_wait(barrier, DEVICES - 1)


def remote(src, dst, send, recv, device):
    return pltpu.make_async_remote_copy(src_ref=src, dst_ref=dst, send_sem=send, recv_sem=recv,
                                        device_id=(device,), device_id_type=pl.DeviceIdType.MESH)


def block_kernel(x_hbm, dy_hbm, pos_hbm, wq_hbm, wk_hbm, wv_hbm, wo_hbm, gains_ref,
                 out_hbm, gi_hbm, ga_hbm, gb_hbm, o_hbm, dqkv_hbm, small_out,
                 xb, dyb, gib, posb, wqkv, wo, h_ref, ht_ref, rope_cos, rope_sin, next_cos, next_sin, out_acc, dh_acc,
                 q_next, k_next, v_next, do_next, v_now, do_now, o_now, dqkv_now, o_last, dqkv_last, o_stage, dqkv_stage,
                 dgin_ref, dqn_ref, dkn_ref, small, smallb, ob, qkvb, l1a, l1b, t_a, t_b, l2a, l2b,
                 weight_sem, in_send, in_recv, out_send, out_recv, store_sem, load_sem, pair_send, pair_recv,
                 turn_send, turn_recv, chip_send, chip_recv, all_send, all_recv, small_send, small_recv):
    seq, group = pl.program_id(0), pl.program_id(1)
    seqs, groups = pl.num_programs(0), pl.num_programs(1)
    me = lax.axis_index('sp')
    head_dim, model = dqn_ref.shape[1], dgin_ref.shape[1]
    gin_ref = gains_ref.at[:, pl.ds(0, model)]
    qn_ref, kn_ref, freq_ref = (gains_ref.at[:, pl.ds(model + i * head_dim, head_dim)] for i in range(3))
    q_cols = o_now.shape[1]
    per_kv = q_cols // head_dim
    seq_len = xb.shape[1]
    piece = seq_len // DEVICES
    scale = head_dim ** -0.5
    half = head_dim // 2
    tiles = [slice(i, i + ROW_BLOCK) for i in range(0, seq_len, ROW_BLOCK)]

    def rows_of(device):
        return pl.ds(pl.multiple_of(device * piece, piece), piece)

    def incoming(kind, s, step, arrival=False):
        peer = peer_of(me, step)
        src = (x_hbm, dy_hbm, pos_hbm)[kind].at[DEVICES * s + peer]

        def landing(device):
            return posb.at[s, device] if kind == 2 else (xb, dyb)[kind].at[s, rows_of(device)]

        if step == 0:
            return pltpu.make_async_copy(src, landing(me), in_recv.at[kind, s, 0])
        return remote(src, landing(peer if arrival else me), in_send.at[kind, s, step], in_recv.at[kind, s, step], peer)

    def outgoing(kind, s, step, arrival=False):
        peer = peer_of(me, step)
        src = xb.at[s, rows_of(peer)] if kind == 0 else gib.at[s % 2, rows_of(peer)]
        dst = (out_hbm, gi_hbm)[kind]
        if step == 0:
            return pltpu.make_async_copy(src, dst.at[DEVICES * s + me], out_recv.at[kind, s, 0])
        return remote(src, dst.at[DEVICES * s + (peer if arrival else me)],
                      out_send.at[kind, s, step], out_recv.at[kind, s, step], peer)

    def sent(kind, s):
        outgoing(kind, s, 0).wait()
        for step in range(1, DEVICES):
            outgoing(kind, s, step).wait_send()

    def weight_loads():
        copies = []
        for place in range(DEVICES):
            g = group_at(me, place)
            wide = pl.ds(pl.multiple_of(g * q_cols, q_cols), q_cols)
            narrow = pl.ds(pl.multiple_of(g * head_dim, head_dim), head_dim)
            parts = ((wq_hbm.at[:, wide], wqkv.at[place, :, pl.ds(0, q_cols)]),
                     (wk_hbm.at[:, narrow], wqkv.at[place, :, pl.ds(q_cols, head_dim)]),
                     (wv_hbm.at[:, narrow], wqkv.at[place, :, pl.ds(q_cols + head_dim, head_dim)]),
                     (wo_hbm.at[wide], wo.at[place]))
            copies += [pltpu.make_async_copy(src, dst, weight_sem.at[i, place]) for i, (src, dst) in enumerate(parts)]
        return copies

    def arrive(kind, s):
        for step in range(DEVICES):
            if step == 0:
                incoming(kind, s, 0).wait()
            else:
                incoming(kind, s, step, arrival=True).wait_recv()

    def prepare(s):
        arrive(2, s)
        on_diag = lax.broadcasted_iota(jnp.int32, (piece, head_dim), 0) == lax.broadcasted_iota(jnp.int32, (piece, head_dim), 1)
        low = lax.broadcasted_iota(jnp.int32, (piece, head_dim), 1) < half
        half_count = DEVICES // 2

        def column(device):
            row = jnp.broadcast_to(posb[s, device, 0:1, :], (piece, head_dim))
            return jnp.sum(jnp.where(on_diag, row, 0.0), axis=-1, keepdims=True)

        for device in range(half_count):
            angles = jnp.where(low, column(device), column(device + half_count)) * freq_ref[...]
            cos, sin = jnp.cos(angles), jnp.sin(angles)
            cos_turned, sin_turned = pltpu.roll(cos, half, 1), pltpu.roll(sin, half, 1)
            first = slice(device * piece, (device + 1) * piece)
            second = slice((device + half_count) * piece, (device + half_count + 1) * piece)
            next_cos[first, :] = jnp.where(low, cos, cos_turned)
            next_sin[first, :] = jnp.where(low, -sin, sin_turned)
            next_cos[second, :] = jnp.where(low, cos_turned, cos)
            next_sin[second, :] = jnp.where(low, -sin_turned, sin)
        arrive(0, s)
        x = xb[s].astype(F32)
        inv = lax.rsqrt(jnp.mean(x * x, axis=-1, keepdims=True) + EPSILON)
        h_ref[...] = (x * inv * gin_ref[...]).astype(BF16)
        arrive(1, s)

    def project(s, g):
        def q_rows(rows):
            q_next[rows] = dot(h_ref[rows], wqkv[g, :, :q_cols])

        def kv_rows(rows):
            kv = dot(h_ref[rows], wqkv[g, :, q_cols:])
            k_next[rows] = kv[:, :head_dim]
            v_next[rows] = kv[:, head_dim:].astype(BF16)

        def do_rows(rows):
            do_next[rows] = dot(dyb[s, rows], wo[g], NT).astype(BF16)

        return [functools.partial(f, rows) for f in (q_rows, kv_rows, do_rows) for rows in tiles]

    def accumulate(g):
        def out_cols(cols):
            out_acc[:, cols] += dot(o_last[...], wo[g, :, cols])

        def dh_cols(cols):
            dh_acc[:, cols] += dot(dqkv_last[...], wqkv[g, cols, :], NT)

        columns = [slice(c, c + 256) for c in range(0, out_acc.shape[1], 256)]
        return [functools.partial(f, cols) for f in (out_cols, dh_cols) for cols in columns]

    def run(products):
        for product in products:
            product()

    def finish(s):
        x = xb[s].astype(F32)
        inv = lax.rsqrt(jnp.mean(x * x, axis=-1, keepdims=True) + EPSILON)
        unit = x * inv
        xb[s] = (x + out_acc[...]).astype(BF16)
        d_norm = dh_acc[...]
        dgin_ref[...] += jnp.sum(d_norm * unit, axis=0, keepdims=True)
        d_unit = d_norm * gin_ref[...]
        grad = inv * (d_unit - unit * jnp.mean(d_unit * unit, axis=-1, keepdims=True))

        @pl.when(s >= 2)
        def _():
            sent(1, s - 2)

        gib[s % 2] = (dyb[s].astype(F32) + grad).astype(BF16)
        for kind in range(2):
            for step in (2, 4, 6, 3, 5, 7, 1, 0):
                outgoing(kind, s, step).start()

    @pl.when((seq == 0) & (group == 0))
    def _():
        entry_barrier(me)

        def send_all(s, carry):
            for kind in (2, 0, 1):
                for step in (2, 4, 6, 3, 5, 7, 1, 0):
                    incoming(kind, s, step).start()
            return carry

        lax.fori_loop(0, seqs, send_all, 0)
        for copy in weight_loads():
            copy.start()
        dgin_ref[...] = jnp.zeros_like(dgin_ref)
        dqn_ref[...] = jnp.zeros_like(dqn_ref)
        dkn_ref[...] = jnp.zeros_like(dkn_ref)
        o_now[...] = jnp.zeros_like(o_now)
        dqkv_now[...] = jnp.zeros_like(dqkv_now)
        out_acc[...] = jnp.zeros_like(out_acc)
        dh_acc[...] = jnp.zeros_like(dh_acc)
        for copy in weight_loads():
            copy.wait()
        prepare(0)
        run(project(0, 0))

    @pl.when(group == 0)
    def _():
        rope_cos[...] = next_cos[...]
        rope_sin[...] = next_sin[...]
        ht_ref[:, pl.ds(pl.multiple_of(seq * seq_len, seq_len), seq_len)] = h_ref[...].T

    last_group = group == groups - 1

    @pl.when(last_group & (seq < seqs - 1))
    def _():
        prepare(seq + 1)

    cos, sin = rope_cos[...], rope_sin[...]

    def norm_rotate(t, gain):
        inv = lax.rsqrt(jnp.mean(t * t, axis=-1, keepdims=True) + EPSILON)
        unit = t * inv
        scaled = unit * gain
        return (scaled * cos + pltpu.roll(scaled, half, 1) * sin).astype(BF16), unit, inv

    def norm_rotate_back(grad, unit, inv, gain):
        d_scaled = grad * cos - pltpu.roll(grad, half, 1) * sin
        d_gain = jnp.sum(d_scaled * unit, axis=0, keepdims=True)
        d_unit = d_scaled * gain
        return inv * (d_unit - unit * jnp.mean(d_unit * unit, axis=-1, keepdims=True)), d_gain

    step_id = seq * groups + group
    slot = step_id % 2

    def stores(step):
        g, rows = step % groups, pl.ds(pl.multiple_of((step // groups) * seq_len, seq_len), seq_len)
        return [pltpu.make_async_copy(o_stage.at[step % 2], o_hbm.at[g, rows], store_sem.at[0, step % 2]),
                pltpu.make_async_copy(dqkv_stage.at[step % 2], dqkv_hbm.at[g, rows], store_sem.at[1, step % 2])]

    stored = (seqs - 1) * groups

    @pl.when((step_id >= 2) & (step_id - 2 < stored))
    def _():
        for copy in stores(step_id - 2):
            copy.wait()

    @pl.when((step_id >= 1) & (step_id - 1 < stored))
    def _():
        for copy in stores(step_id - 1):
            copy.start()

    v_now[...] = v_next[...]
    do_now[...] = do_next[...]
    o_last[...] = o_now[...]
    dqkv_last[...] = dqkv_now[...]

    ahead = project(jnp.minimum(seq + last_group.astype(jnp.int32), seqs - 1), (group + 1) % groups)
    behind = accumulate((group + groups - 1) % groups)
    lanes = [slice(head * head_dim, (head + 1) * head_dim) for head in range(per_kv)]
    stacked = per_kv * ROW_BLOCK
    key_id = lax.broadcasted_iota(jnp.int32, (ROW_BLOCK, stacked), 0)
    causal = key_id <= lax.broadcasted_iota(jnp.int32, (ROW_BLOCK, stacked), 1) % ROW_BLOCK
    blocks = len(tiles)

    run(behind[:6])
    k_rot, k_unit, k_inv = norm_rotate(k_next[...], kn_ref[...])
    q_parts = [norm_rotate(q_next[:, lane], qn_ref[...]) for lane in lanes]
    q_tile = [jnp.concatenate([part[0][tile] for part in q_parts], axis=0) for tile in tiles]
    do_tile = [jnp.concatenate([do_now[tile, lane] for lane in lanes], axis=0) for tile in tiles]
    v_cols, k_cols = v_now[...].T, k_rot.T
    fill = [ahead[0:2], behind[6:7], behind[7:8] + ahead[2:3], ahead[3:4]]
    dp_all = [dot(v_now[:(i + 1) * ROW_BLOCK], do_tile[i], NT) for i in range(blocks)]
    s_all = [dot(k_rot[:(i + 1) * ROW_BLOCK], q_tile[i], NT) for i in range(blocks)]

    def masked(i):
        diagonal = jnp.where(causal, s_all[i][i * ROW_BLOCK:], NEG_LARGE)
        return diagonal if i == 0 else jnp.concatenate([s_all[i][:i * ROW_BLOCK], diagonal], axis=0)

    def store_output(i, o_i):
        for head, lane in enumerate(lanes):
            o_head = o_i[head * ROW_BLOCK:(head + 1) * ROW_BLOCK]
            o_stage[slot, tiles[i], lane] = o_head
            o_now[tiles[i], lane] = o_head

    def add_rows(total, part):
        keys = part.shape[0]
        if total is None:
            return part
        return jnp.concatenate([total + part[:total.shape[0]], part[total.shape[0]:keys]], axis=0)

    dk_all, dv_all, dq_tile = None, None, []
    for i in range(blocks):
        keys = (i + 1) * ROW_BLOCK
        s = masked(i)
        e = jnp.exp2((s - jnp.max(s, axis=0, keepdims=True)) * (scale * LOG2_E))
        p = e * (1.0 / jnp.sum(e, axis=0, keepdims=True))
        p_bf16 = p.astype(BF16)
        run(fill[2 * i])
        store_output(i, dot(v_cols[:, :keys], p_bf16).astype(BF16).T)
        dv_all = add_rows(dv_all, dot(p_bf16, do_tile[i]))
        delta = jnp.sum(p * dp_all[i], axis=0, keepdims=True)
        ds = (p * (dp_all[i] - delta)).astype(BF16)
        run(fill[2 * i + 1])
        dq_tile.append(dot(k_cols[:, :keys], ds).T)
        dk_all = add_rows(dk_all, dot(ds, q_tile[i]))
    run(ahead[4:])
    for head, lane in enumerate(lanes):
        dq_head = jnp.concatenate([dq[head * ROW_BLOCK:(head + 1) * ROW_BLOCK] for dq in dq_tile], axis=0)
        dq_head, d_gain = norm_rotate_back(dq_head * scale, q_parts[head][1], q_parts[head][2], qn_ref[...])
        dqn_ref[...] += d_gain
        dq_head = dq_head.astype(BF16)
        dqkv_stage[slot, :, lane] = dq_head
        dqkv_now[:, lane] = dq_head
    dk_head, d_gain = norm_rotate_back(dk_all * scale, k_unit, k_inv, kn_ref[...])
    dkn_ref[...] += d_gain
    dk_head = dk_head.astype(BF16)
    dqkv_stage[slot, :, q_cols:q_cols + head_dim] = dk_head
    dqkv_now[:, q_cols:q_cols + head_dim] = dk_head
    dv_head = dv_all.astype(BF16)
    dqkv_stage[slot, :, q_cols + head_dim:] = dv_head
    dqkv_now[:, q_cols + head_dim:] = dv_head

    @pl.when((group == 0) & (seq > 0))
    def _():
        finish(seq - 1)
        out_acc[...] = jnp.zeros_like(out_acc)
        dh_acc[...] = jnp.zeros_like(dh_acc)

    reducer = GradientReducer(me, (ga_hbm, gb_hbm), o_hbm, dqkv_hbm, small_out, dyb, ht_ref, wo, wqkv,
                              dgin_ref, dqn_ref, dkn_ref, small, smallb, ob, qkvb, o_now, dqkv_now, (l1a, l1b), (t_a, t_b), (l2a, l2b),
                              load_sem, pair_send, pair_recv, turn_send, turn_recv, chip_send, chip_recv,
                              all_send, all_recv, small_send, small_recv)
    last_seq = seq == seqs - 1

    @pl.when(last_seq & (group == 0))
    def _():
        start(reducer.loads(0))

    @pl.when(last_seq & (group < groups - 1))
    def _():
        reducer.step(group)

    @pl.when(last_seq & last_group)
    def _():
        o_last[...] = o_now[...]
        dqkv_last[...] = dqkv_now[...]
        run(accumulate(groups - 1))
        finish(seqs - 1)
        reducer.step(groups - 1)
        reducer.finish()

        def drain(s, carry):
            for step in range(1, DEVICES):
                for kind in range(3):
                    incoming(kind, s, step).wait_send()
                for kind in range(2):
                    outgoing(kind, s, step, arrival=True).wait_recv()
            sent(0, s)
            return carry

        lax.fori_loop(0, seqs, drain, 0)
        for s in range(2):
            sent(1, seqs - 2 + s)


def start(copies):
    for copy in copies:
        copy.start()


def wait_send(copies):
    for copy in copies:
        copy.wait_send()


def wait_recv(copies):
    for copy in copies:
        copy.wait_recv()


class GradientReducer:
    def __init__(self, me, gathered, o_hbm, dqkv_hbm, small_out, dyb, ht_ref, wo, wqkv, dgin_ref, dqn_ref, dkn_ref,
                 small, smallb, ob, qkvb, o_now, dqkv_now, pair_in, turn_in, chip_in, load_sem, pair_send, pair_recv,
                 turn_send, turn_recv, chip_send, chip_recv, all_send, all_recv, small_send, small_recv):
        self.__dict__.update({k: v for k, v in locals().items() if k != 'self'})
        self.partner = peer_of(me, PARTNER)
        self.chips = DEVICES // 2
        self.stage = (wo, wqkv)
        self.sizes = [ref.shape[1] // 2 for ref in self.stage]
        self.early = ob.shape[0] - o_now.shape[0]

    def slot(self, place):
        return (place + DEVICES) % (DEVICES + 1)

    def half_of(self, i, half):
        return pl.ds(half * self.sizes[i], self.sizes[i])

    def loads(self, place):
        rows = pl.ds(0, self.early)
        return [pltpu.make_async_copy(self.o_hbm.at[place], self.ob.at[rows], self.load_sem.at[0]),
                pltpu.make_async_copy(self.dqkv_hbm.at[place], self.qkvb.at[rows], self.load_sem.at[1])]

    def pair(self, order):
        return [remote(self.stage[i].at[self.slot(2 * order)], self.pair_in[i].at[order % 2],
                       self.pair_send.at[i, order], self.pair_recv.at[i, order], self.partner) for i in range(2)]

    def turn(self, half):
        return [remote(self.stage[i].at[self.slot(1), self.half_of(i, half)], self.turn_in[i].at[half],
                       self.turn_send.at[i, half], self.turn_recv.at[i, half], peer_of(self.me, (X, Y)[half])) for i in range(2)]

    def chip(self, axis, half):
        return [remote(self.stage[i].at[self.slot(2 * axis + 3), self.half_of(i, half)], self.chip_in[i].at[axis, self.half_of(i, half)],
                       self.chip_send.at[i, axis, half], self.chip_recv.at[i, axis, half], peer_of(self.me, (X, Y)[axis])) for i in range(2)]

    def join_turn(self, axis, half):
        wait_recv(self.turn(half))
        for i in range(2):
            part = self.stage[i].at[self.slot(2 * axis + 3), self.half_of(i, half)]
            part[...] = (part[...].astype(F32) + self.turn_in[i][half].astype(F32)).astype(BF16)
        start(self.chip(axis, half))

    def step(self, place):
        for copy in self.loads(place):
            copy.wait()
        self.ob[self.early:] = self.o_now[...]
        self.qkvb[self.early:] = self.dqkv_now[...]
        tokens = self.ob.shape[0]
        into = self.slot(place)
        self.stage[0][into] = dot(self.ob[...], self.dyb[...].reshape(tokens, self.dyb.shape[2]), TN).astype(BF16)
        self.stage[1][into] = dot(self.ht_ref[...], self.qkvb[...]).astype(BF16)
        order = place // 2

        @pl.when(place < DEVICES - 1)
        def _():
            start(self.loads(place + 1))

        @pl.when(place % 2 == 0)
        def _():
            start(self.pair(order))

        @pl.when(place % 2 == 1)
        def _():
            wait_recv(self.pair(order))
            for i in range(2):
                for half in range(2):
                    part = self.stage[i].at[into, self.half_of(i, half)]
                    part[...] = (part[...].astype(F32) + self.pair_in[i][order % 2, self.half_of(i, half)].astype(F32)).astype(BF16)

        @pl.when(place == 1)
        def _():
            start(self.turn(0))
            start(self.turn(1))

        @pl.when(place == 3)
        def _():
            start(self.chip(0, 0))

        @pl.when(place == 5)
        def _():
            start(self.chip(1, 1))
            self.join_turn(0, 1)
            self.join_turn(1, 0)

    def small_copy(self, step, arrival=False):
        peer = peer_of(self.me, step)
        return remote(self.small, self.smallb.at[peer if arrival else self.me], self.small_send.at[step], self.small_recv.at[step], peer)

    def spread(self, half, slot, arrival=False):
        me, partner = self.me, self.partner
        x, y, diag = (peer_of(me, step) for step in (X, Y, DIAG))
        target = (x, y, (y, x)[half], partner, partner, partner, partner)[slot]
        owner = (me, me, (x, y)[half], me, x, y, diag)[slot]
        sender = (x, y, diag, partner, peer_of(partner, X), peer_of(partner, Y), peer_of(partner, DIAG))[slot]
        copies = []
        for i in range(2):
            part = self.half_of(i, half)
            src = self.stage[i].at[self.slot(DEVICES - 1), part] if slot in (0, 1, 3) else self.gathered[i].at[owner, part]
            copies.append(remote(src, self.gathered[i].at[sender if arrival else owner, part],
                                 self.all_send.at[i, half, slot], self.all_recv.at[i, half, slot], target))
        return copies

    def finish(self):
        small, smallb, spread = self.small, self.smallb, self.spread
        small[...] = jnp.zeros_like(small)
        lanes = self.dqn_ref.shape[1]
        rows = self.dgin_ref.shape[1] // lanes
        for row in range(rows):
            small[row:row + 1] = self.dgin_ref[:, row * lanes:(row + 1) * lanes]
        small[rows:rows + 1] = self.dqn_ref[...]
        small[rows + 1:rows + 2] = self.dkn_ref[...]
        for step in range(1, DEVICES):
            self.small_copy(step).start()

        result = self.slot(DEVICES - 1)
        for half in range(2):
            for axis in range(2):
                wait_recv(self.chip(axis, half))
            for i in range(2):
                rows_half = self.half_of(i, half)
                part = self.stage[i].at[result, rows_half]
                total = part[...].astype(F32) + self.chip_in[i][0, rows_half].astype(F32) + self.chip_in[i][1, rows_half].astype(F32)
                part[...] = total.astype(BF16)
            for slot in ((0, 1, 3), (1, 0, 3))[half]:
                start(spread(half, slot))
        local = [pltpu.make_async_copy(self.stage[i].at[result], self.gathered[i].at[self.me], self.load_sem.at[i]) for i in range(2)]
        start(local)

        for step in range(1, DEVICES):
            self.small_copy(step, arrival=True).wait_recv()
        smallb[self.me] = small[...]
        sums = smallb[0]
        for device in range(1, DEVICES):
            sums = sums + smallb[device]
        self.small_out[...] = sums

        for half, slot, onward in ((0, 0, (2, 4)), (1, 1, (2, 5)), (1, 0, (4,)), (0, 1, (5,)), (0, 2, (6,)), (1, 2, (6,))):
            wait_recv(spread(half, slot, arrival=True))
            for forward in onward:
                start(spread(half, forward))
        for copy in local:
            copy.wait()
        for half in range(2):
            for slot in (3, 4, 5, 6):
                wait_recv(spread(half, slot, arrival=True))
            for slot in range(7):
                wait_send(spread(half, slot))
            wait_send(self.turn(half))
            for axis in range(2):
                wait_send(self.chip(axis, half))
        for order in range(self.chips):
            wait_send(self.pair(order))
        for step in range(1, DEVICES):
            self.small_copy(step).wait_send()


def block_call(x, dy, pos, gains, w_q, w_k, w_v, w_o, head_dim):
    batch, piece, model = x.shape
    seqs, seq_len = batch // DEVICES, piece * DEVICES
    q_width, kv_width = w_q.shape[1], w_k.shape[1]
    groups = kv_width // head_dim
    q_cols = q_width // groups
    tokens = seqs * seq_len
    width = q_cols + 2 * head_dim
    fixed = lambda s, g: (0, 0)
    bf = lambda *shape: jax.ShapeDtypeStruct(shape, BF16)
    f32 = lambda *shape: jax.ShapeDtypeStruct(shape, F32)
    anywhere = pl.BlockSpec(memory_space=pl.ANY)
    flops = 4 * tokens * model * (q_width * 2 + kv_width * 2) + 12 * tokens * seq_len * q_width
    vb = lambda *shape: pltpu.VMEM(shape, BF16)
    vf = lambda *shape: pltpu.VMEM(shape, F32)
    dma = lambda *shape: pltpu.SemaphoreType.DMA(shape)
    return pl.pallas_call(
        block_kernel,
        grid=(seqs, groups),
        in_specs=[
            anywhere, anywhere, anywhere, anywhere, anywhere, anywhere, anywhere,
            pl.BlockSpec(gains.shape, fixed),
        ],
        out_specs=[anywhere] * 6 + [pl.BlockSpec((16, head_dim), fixed)],
        out_shape=[
            bf(batch, piece, model), bf(batch, piece, model),
            bf(groups, q_cols, model), bf(groups, model, width),
            bf(groups, tokens - seq_len, q_cols), bf(groups, tokens - seq_len, width),
            f32(16, head_dim),
        ],
        scratch_shapes=[
            vb(seqs, seq_len, model), vb(seqs, seq_len, model), vb(2, seq_len, model),
            vf(seqs, DEVICES, 8, head_dim),
            vb(groups + 1, model, width), vb(groups + 1, q_cols, model),
            vb(seq_len, model), vb(model, tokens),
            vf(seq_len, head_dim), vf(seq_len, head_dim), vf(seq_len, head_dim), vf(seq_len, head_dim),
            vf(seq_len, model), vf(seq_len, model),
            vf(seq_len, q_cols), vf(seq_len, head_dim), vb(seq_len, head_dim), vb(seq_len, q_cols),
            vb(seq_len, head_dim), vb(seq_len, q_cols),
            vb(seq_len, q_cols), vb(seq_len, width), vb(seq_len, q_cols), vb(seq_len, width),
            vb(2, seq_len, q_cols), vb(2, seq_len, width),
            vf(1, model), vf(1, head_dim), vf(1, head_dim), vf(16, head_dim), vf(DEVICES, 16, head_dim),
            vb(tokens, q_cols), vb(tokens, width),
            vb(2, q_cols, model), vb(2, model, width),
            vb(2, q_cols // 2, model), vb(2, model // 2, width),
            vb(2, q_cols, model), vb(2, model, width),
            pltpu.SemaphoreType.DMA((4, groups)),
            pltpu.SemaphoreType.DMA((3, seqs, DEVICES)),
            pltpu.SemaphoreType.DMA((3, seqs, DEVICES)),
            pltpu.SemaphoreType.DMA((2, seqs, DEVICES)),
            pltpu.SemaphoreType.DMA((2, seqs, DEVICES)),
            dma(2, 2), dma(2), dma(2, 4), dma(2, 4), dma(2, 2), dma(2, 2), dma(2, 2, 2), dma(2, 2, 2),
            dma(2, 2, 7), dma(2, 2, 7), dma(DEVICES), dma(DEVICES),
        ],
        compiler_params=pltpu.CompilerParams(
            dimension_semantics=("arbitrary", "arbitrary"), vmem_limit_bytes=67_000_000,
            collective_id=0, has_side_effects=True),
        cost_estimate=pl.CostEstimate(flops=flops, bytes_accessed=50_000_000, transcendentals=tokens * seq_len * 8),
        name="block",
    )(x, dy, pos, w_q, w_k, w_v, w_o, gains)


def widen_kernel(ga_ref, gb_ref, small_ref, wq_ref, wk_ref, wv_ref, wo_ref, dgin_ref, dqn_ref, dkn_ref):
    @pl.when(pl.program_id(0) == 0)
    def _():
        lanes = small_ref.shape[1]
        rows = dgin_ref.shape[1] // lanes
        for row in range(rows):
            dgin_ref[:, row * lanes:(row + 1) * lanes] = small_ref[row:row + 1]
        dqn_ref[...] = small_ref[rows:rows + 1]
        dkn_ref[...] = small_ref[rows + 1:rows + 2]

    q_cols, head_dim = wq_ref.shape[1], wk_ref.shape[1]
    wo_ref[...] = ga_ref[0].astype(F32)
    wq_ref[...] = gb_ref[0, :, :q_cols].astype(F32)
    wk_ref[...] = gb_ref[0, :, q_cols:q_cols + head_dim].astype(F32)
    wv_ref[...] = gb_ref[0, :, q_cols + head_dim:].astype(F32)


def widen_call(ga, gb, small):
    groups, q_cols, model = ga.shape
    head_dim = (gb.shape[2] - q_cols) // 2
    f32 = lambda *shape: jax.ShapeDtypeStruct(shape, F32)
    across = lambda g: (0, g)
    return pl.pallas_call(
        widen_kernel,
        grid=(groups,),
        in_specs=[pl.BlockSpec((1, q_cols, model), lambda g: (g, 0, 0)),
                  pl.BlockSpec((1, model, gb.shape[2]), lambda g: (g, 0, 0)),
                  pl.BlockSpec(small.shape, lambda g: (0, 0))],
        out_specs=[pl.BlockSpec((model, q_cols), across), pl.BlockSpec((model, head_dim), across),
                   pl.BlockSpec((model, head_dim), across), pl.BlockSpec((q_cols, model), lambda g: (g, 0))]
        + [pl.BlockSpec((1, n), lambda g: (0, 0)) for n in (model, head_dim, head_dim)],
        out_shape=[f32(model, groups * q_cols), f32(model, groups * head_dim), f32(model, groups * head_dim),
                   f32(groups * q_cols, model), f32(1, model), f32(1, head_dim), f32(1, head_dim)],
        compiler_params=pltpu.CompilerParams(dimension_semantics=("arbitrary",)),
        name="widen",
    )(ga, gb, small)


def solution(mesh):
    seq_spec = P(None, 'sp', None)
    replicated = P()

    def shard_body(hidden_in, grad_out, positions, w_q, w_k, w_v, w_o, g_in, q_norm, k_norm):
        batch, seq_dev, model_dim = hidden_in.shape
        head_dim = q_norm.shape[0]
        exponents = jnp.arange(0, head_dim, 2).astype(F32) / head_dim
        inv_freq = jnp.power(ROPE_THETA, -exponents)
        gains = jnp.concatenate([g_in.astype(F32), q_norm.astype(F32), k_norm.astype(F32), inv_freq, inv_freq])[None]
        pos = jnp.broadcast_to(jnp.pad(positions.astype(F32), ((0, 0), (0, head_dim - seq_dev)))[:, None, :], (batch, 8, head_dim))
        hidden_out, grad_in, ga, gb, _, _, small = block_call(hidden_in, grad_out, pos, gains, w_q, w_k, w_v, w_o, head_dim)
        grad_wq, grad_wk, grad_wv, grad_wo, dgin, dqn, dkn = widen_call(ga, gb, small)
        return hidden_out, grad_in, grad_wq, grad_wk, grad_wv, grad_wo, dgin[0], dqn[0], dkn[0]

    return jax.shard_map(shard_body, mesh=mesh,
                         in_specs=(seq_spec, seq_spec, P(None, 'sp'), replicated, replicated, replicated, replicated, replicated, replicated, replicated),
                         out_specs=(seq_spec, seq_spec, replicated, replicated, replicated, replicated, replicated, replicated, replicated),
                         check_vma=False)
```

```python
import functools
import jax
import jax.numpy as jnp
from jax import lax
from jax.experimental import pallas as pl
from jax.experimental.pallas import tpu as pltpu
from jax.sharding import PartitionSpec as P

EPSILON = 1e-6
ROPE_THETA = 1000000.0
NEG_LARGE = -1e30
LOG2_E = 1.4426950408889634
NT = (((1,), (1,)), ((), ()))
TN = (((0,), (0,)), ((), ()))
ROW_BLOCK = 256
DEVICES = 8
BF16 = jnp.bfloat16
F32 = jnp.float32


def dot(a, b, dims=(((1,), (0,)), ((), ()))):
    return lax.dot_general(a, b, dims, preferred_element_type=F32)


def peer_of(me, step):
    core, x, y = me % 2, (me // 2) % 2, me // 4
    return ((y + step // 4) % 2) * 4 + ((x + (step // 2) % 2) % 2) * 2 + (core + step % 2) % 2


X, Y, DIAG, PARTNER = 2, 4, 6, 1


def chip_peer(me, order):
    return peer_of(me, (1 - order // 2) * X + ((order + 1) % 2) * Y)


def group_at(me, place):
    return peer_of(chip_peer(me, place // 2), 1 - place % 2)


def entry_barrier(me):
    barrier = pltpu.get_barrier_semaphore()
    for step in range(1, DEVICES):
        pl.semaphore_signal(barrier, inc=1, device_id=(peer_of(me, step),), device_id_type=pl.DeviceIdType.MESH)
    pl.semaphore_wait(barrier, DEVICES - 1)


def remote(src, dst, send, recv, device):
    return pltpu.make_async_remote_copy(src_ref=src, dst_ref=dst, send_sem=send, recv_sem=recv,
                                        device_id=(device,), device_id_type=pl.DeviceIdType.MESH)


def block_kernel(x_hbm, dy_hbm, pos_hbm, wq_hbm, wk_hbm, wv_hbm, wo_hbm, gin_ref, qn_ref, kn_ref, freq_ref,
                 out_hbm, gi_hbm, ga_hbm, gb_hbm, o_hbm, dqkv_hbm, small_out,
                 xb, dyb, gib, posb, wqkv, wo, h_ref, ht_ref, rope_cos, rope_sin, next_cos, next_sin, out_acc, dh_acc,
                 q_next, k_next, v_next, do_next, v_now, do_now, o_now, dqkv_now, o_last, dqkv_last, o_stage, dqkv_stage,
                 dgin_ref, dqn_ref, dkn_ref, small, smallb, ob, qkvb, l1a, l1b, t_a, t_b, l2a, l2b,
                 weight_sem, in_send, in_recv, out_send, out_recv, store_sem, load_sem, pair_send, pair_recv,
                 turn_send, turn_recv, chip_send, chip_recv, all_send, all_recv, small_send, small_recv):
    seq, group = pl.program_id(0), pl.program_id(1)
    seqs, groups = pl.num_programs(0), pl.num_programs(1)
    me = lax.axis_index('sp')
    head_dim, model = dqn_ref.shape[1], dgin_ref.shape[1]
    q_gain, k_gain, in_gain = (ref[...].astype(F32) for ref in (qn_ref, kn_ref, gin_ref))
    q_cols = o_now.shape[1]
    per_kv = q_cols // head_dim
    seq_len = xb.shape[1]
    piece = seq_len // DEVICES
    scale = head_dim ** -0.5
    half = head_dim // 2
    tiles = [slice(i, i + ROW_BLOCK) for i in range(0, seq_len, ROW_BLOCK)]

    def rows_of(device):
        return pl.ds(pl.multiple_of(device * piece, piece), piece)

    def incoming(kind, s, step, arrival=False):
        peer = peer_of(me, step)
        src = (x_hbm, dy_hbm, pos_hbm)[kind].at[DEVICES * s + peer]

        def landing(device):
            return posb.at[s, device] if kind == 2 else (xb, dyb)[kind].at[s, rows_of(device)]

        if step == 0:
            return pltpu.make_async_copy(src, landing(me), in_recv.at[kind, s, 0])
        return remote(src, landing(peer if arrival else me), in_send.at[kind, s, step], in_recv.at[kind, s, step], peer)

    def outgoing(kind, s, step, arrival=False):
        peer = peer_of(me, step)
        src = xb.at[s, rows_of(peer)] if kind == 0 else gib.at[s % 2, rows_of(peer)]
        dst = (out_hbm, gi_hbm)[kind]
        if step == 0:
            return pltpu.make_async_copy(src, dst.at[DEVICES * s + me], out_recv.at[kind, s, 0])
        return remote(src, dst.at[DEVICES * s + (peer if arrival else me)],
                      out_send.at[kind, s, step], out_recv.at[kind, s, step], peer)

    def sent(kind, s):
        outgoing(kind, s, 0).wait()
        for step in range(1, DEVICES):
            outgoing(kind, s, step).wait_send()

    def weight_loads():
        copies = []
        for place in range(DEVICES):
            g = group_at(me, place)
            wide = pl.ds(pl.multiple_of(g * q_cols, q_cols), q_cols)
            narrow = pl.ds(pl.multiple_of(g * head_dim, head_dim), head_dim)
            parts = ((wq_hbm.at[:, wide], wqkv.at[place, :, pl.ds(0, q_cols)]),
                     (wk_hbm.at[:, narrow], wqkv.at[place, :, pl.ds(q_cols, head_dim)]),
                     (wv_hbm.at[:, narrow], wqkv.at[place, :, pl.ds(q_cols + head_dim, head_dim)]),
                     (wo_hbm.at[wide], wo.at[place]))
            copies += [pltpu.make_async_copy(src, dst, weight_sem.at[i, place]) for i, (src, dst) in enumerate(parts)]
        return copies

    def arrive(kind, s):
        for step in range(DEVICES):
            if step == 0:
                incoming(kind, s, 0).wait()
            else:
                incoming(kind, s, step, arrival=True).wait_recv()

    def prepare(s):
        arrive(2, s)
        on_diag = lax.broadcasted_iota(jnp.int32, (piece, head_dim), 0) == lax.broadcasted_iota(jnp.int32, (piece, head_dim), 1)
        low = lax.broadcasted_iota(jnp.int32, (piece, head_dim), 1) < half
        half_count = DEVICES // 2

        def column(device):
            row = jnp.broadcast_to(posb[s, device, 0:1, :], (piece, head_dim))
            return jnp.sum(jnp.where(on_diag, row, 0.0), axis=-1, keepdims=True)

        for device in range(half_count):
            angles = jnp.where(low, column(device), column(device + half_count)) * freq_ref[...]
            cos, sin = jnp.cos(angles), jnp.sin(angles)
            cos_turned, sin_turned = pltpu.roll(cos, half, 1), pltpu.roll(sin, half, 1)
            first = slice(device * piece, (device + 1) * piece)
            second = slice((device + half_count) * piece, (device + half_count + 1) * piece)
            next_cos[first, :] = jnp.where(low, cos, cos_turned)
            next_sin[first, :] = jnp.where(low, -sin, sin_turned)
            next_cos[second, :] = jnp.where(low, cos_turned, cos)
            next_sin[second, :] = jnp.where(low, -sin_turned, sin)
        arrive(0, s)
        x = xb[s].astype(F32)
        inv = lax.rsqrt(jnp.mean(x * x, axis=-1, keepdims=True) + EPSILON)
        h_ref[...] = (x * inv * in_gain).astype(BF16)

    def project(s, g):
        def q_rows(rows):
            q_next[rows] = dot(h_ref[rows], wqkv[g, :, :q_cols])

        def kv_rows(rows):
            kv = dot(h_ref[rows], wqkv[g, :, q_cols:])
            k_next[rows] = kv[:, :head_dim]
            v_next[rows] = kv[:, head_dim:].astype(BF16)

        def do_rows(rows):
            do_next[rows] = dot(dyb[s, rows], wo[g], NT).astype(BF16)

        return [functools.partial(f, rows) for f in (q_rows, kv_rows, do_rows) for rows in tiles]

    def accumulate(g):
        def out_cols(cols):
            out_acc[:, cols] += dot(o_last[...], wo[g, :, cols])

        def dh_cols(cols):
            dh_acc[:, cols] += dot(dqkv_last[...], wqkv[g, cols, :], NT)

        columns = [slice(c, c + 256) for c in range(0, out_acc.shape[1], 256)]
        return [functools.partial(f, cols) for f in (out_cols, dh_cols) for cols in columns]

    def run(products):
        for product in products:
            product()

    def finish(s):
        x = xb[s].astype(F32)
        inv = lax.rsqrt(jnp.mean(x * x, axis=-1, keepdims=True) + EPSILON)
        unit = x * inv
        xb[s] = (x + out_acc[...]).astype(BF16)
        d_norm = dh_acc[...]
        dgin_ref[...] += jnp.sum(d_norm * unit, axis=0, keepdims=True)
        d_unit = d_norm * in_gain
        grad = inv * (d_unit - unit * jnp.mean(d_unit * unit, axis=-1, keepdims=True))

        @pl.when(s >= 2)
        def _():
            sent(1, s - 2)

        gib[s % 2] = (dyb[s].astype(F32) + grad).astype(BF16)
        for kind in range(2):
            for step in (2, 4, 6, 3, 5, 7, 1, 0):
                outgoing(kind, s, step).start()

    @pl.when((seq == 0) & (group == 0))
    def _():
        entry_barrier(me)

        def send_all(s, carry):
            for kind in (2, 0, 1):
                for step in (2, 4, 6, 3, 5, 7, 1, 0):
                    incoming(kind, s, step).start()
            return carry

        lax.fori_loop(0, seqs, send_all, 0)
        for copy in weight_loads():
            copy.start()
        dgin_ref[...] = jnp.zeros_like(dgin_ref)
        dqn_ref[...] = jnp.zeros_like(dqn_ref)
        dkn_ref[...] = jnp.zeros_like(dkn_ref)
        o_now[...] = jnp.zeros_like(o_now)
        dqkv_now[...] = jnp.zeros_like(dqkv_now)
        out_acc[...] = jnp.zeros_like(out_acc)
        dh_acc[...] = jnp.zeros_like(dh_acc)
        for copy in weight_loads():
            copy.wait()
        prepare(0)
        first = project(0, 0)
        run(first[:4])
        arrive(1, 0)
        run(first[4:])

    @pl.when(group == 0)
    def _():
        rope_cos[...] = next_cos[...]
        rope_sin[...] = next_sin[...]
        ht_ref[:, pl.ds(pl.multiple_of(seq * seq_len, seq_len), seq_len)] = h_ref[...].T

    last_group = group == groups - 1

    @pl.when(last_group & (seq < seqs - 1))
    def _():
        prepare(seq + 1)
        arrive(1, seq + 1)

    cos, sin = rope_cos[...], rope_sin[...]

    def norm_rotate(t, gain):
        inv = lax.rsqrt(jnp.mean(t * t, axis=-1, keepdims=True) + EPSILON)
        unit = t * inv
        scaled = unit * gain
        return (scaled * cos + pltpu.roll(scaled, half, 1) * sin).astype(BF16), unit, inv

    def norm_rotate_back(grad, unit, inv, gain):
        d_scaled = grad * cos - pltpu.roll(grad, half, 1) * sin
        d_gain = jnp.sum(d_scaled * unit, axis=0, keepdims=True)
        d_unit = d_scaled * gain
        return inv * (d_unit - unit * jnp.mean(d_unit * unit, axis=-1, keepdims=True)), d_gain

    step_id = seq * groups + group
    slot = step_id % 2

    def stores(step):
        g, rows = step % groups, pl.ds(pl.multiple_of((step // groups) * seq_len, seq_len), seq_len)
        return [pltpu.make_async_copy(o_stage.at[step % 2], o_hbm.at[g, rows], store_sem.at[0, step % 2]),
                pltpu.make_async_copy(dqkv_stage.at[step % 2], dqkv_hbm.at[g, rows], store_sem.at[1, step % 2])]

    stored = (seqs - 1) * groups

    @pl.when((step_id >= 2) & (step_id - 2 < stored))
    def _():
        for copy in stores(step_id - 2):
            copy.wait()

    @pl.when((step_id >= 1) & (step_id - 1 < stored))
    def _():
        for copy in stores(step_id - 1):
            copy.start()

    v_now[...] = v_next[...]
    do_now[...] = do_next[...]
    o_last[...] = o_now[...]
    dqkv_last[...] = dqkv_now[...]

    ahead = project(jnp.minimum(seq + last_group.astype(jnp.int32), seqs - 1), (group + 1) % groups)
    behind = accumulate((group + groups - 1) % groups)
    lanes = [slice(head * head_dim, (head + 1) * head_dim) for head in range(per_kv)]
    stacked = per_kv * ROW_BLOCK
    key_id = lax.broadcasted_iota(jnp.int32, (ROW_BLOCK, stacked), 0)
    causal = key_id <= lax.broadcasted_iota(jnp.int32, (ROW_BLOCK, stacked), 1) % ROW_BLOCK
    blocks = len(tiles)

    run(behind[:6])
    k_rot, k_unit, k_inv = norm_rotate(k_next[...], k_gain)
    q_parts = [norm_rotate(q_next[:, lane], q_gain) for lane in lanes]
    q_tile = [jnp.concatenate([part[0][tile] for part in q_parts], axis=0) for tile in tiles]
    do_tile = [jnp.concatenate([do_now[tile, lane] for lane in lanes], axis=0) for tile in tiles]
    v_cols, k_cols = v_now[...].T, k_rot.T
    fill = [ahead[0:2], behind[6:7], behind[7:8] + ahead[2:3], ahead[3:4]]
    dp_all = [dot(v_now[:(i + 1) * ROW_BLOCK], do_tile[i], NT) for i in range(blocks)]
    s_all = [dot(k_rot[:(i + 1) * ROW_BLOCK], q_tile[i], NT) for i in range(blocks)]

    def masked(i):
        diagonal = jnp.where(causal, s_all[i][i * ROW_BLOCK:], NEG_LARGE)
        return diagonal if i == 0 else jnp.concatenate([s_all[i][:i * ROW_BLOCK], diagonal], axis=0)

    def store_output(i, o_i):
        for head, lane in enumerate(lanes):
            o_head = o_i[head * ROW_BLOCK:(head + 1) * ROW_BLOCK]
            o_stage[slot, tiles[i], lane] = o_head
            o_now[tiles[i], lane] = o_head

    def add_rows(total, part):
        keys = part.shape[0]
        if total is None:
            return part
        return jnp.concatenate([total + part[:total.shape[0]], part[total.shape[0]:keys]], axis=0)

    dk_all, dv_all, dq_tile = None, None, []
    for i in range(blocks):
        keys = (i + 1) * ROW_BLOCK
        s = masked(i)
        e = jnp.exp2((s - jnp.max(s, axis=0, keepdims=True)) * (scale * LOG2_E))
        p = e * (1.0 / jnp.sum(e, axis=0, keepdims=True))
        p_bf16 = p.astype(BF16)
        run(fill[2 * i])
        store_output(i, dot(v_cols[:, :keys], p_bf16).astype(BF16).T)
        dv_all = add_rows(dv_all, dot(p_bf16, do_tile[i]))
        delta = jnp.sum(p * dp_all[i], axis=0, keepdims=True)
        ds = (p * (dp_all[i] - delta)).astype(BF16)
        run(fill[2 * i + 1])
        dq_tile.append(dot(k_cols[:, :keys], ds).T)
        dk_all = add_rows(dk_all, dot(ds, q_tile[i]))
    run(ahead[4:])
    for head, lane in enumerate(lanes):
        dq_head = jnp.concatenate([dq[head * ROW_BLOCK:(head + 1) * ROW_BLOCK] for dq in dq_tile], axis=0)
        dq_head, d_gain = norm_rotate_back(dq_head * scale, q_parts[head][1], q_parts[head][2], q_gain)
        dqn_ref[...] += d_gain
        dq_head = dq_head.astype(BF16)
        dqkv_stage[slot, :, lane] = dq_head
        dqkv_now[:, lane] = dq_head
    dk_head, d_gain = norm_rotate_back(dk_all * scale, k_unit, k_inv, k_gain)
    dkn_ref[...] += d_gain
    dk_head = dk_head.astype(BF16)
    dqkv_stage[slot, :, q_cols:q_cols + head_dim] = dk_head
    dqkv_now[:, q_cols:q_cols + head_dim] = dk_head
    dv_head = dv_all.astype(BF16)
    dqkv_stage[slot, :, q_cols + head_dim:] = dv_head
    dqkv_now[:, q_cols + head_dim:] = dv_head

    @pl.when((group == 0) & (seq > 0))
    def _():
        finish(seq - 1)
        out_acc[...] = jnp.zeros_like(out_acc)
        dh_acc[...] = jnp.zeros_like(dh_acc)

    reducer = GradientReducer(me, (ga_hbm, gb_hbm), o_hbm, dqkv_hbm, small_out, dyb, ht_ref, wo, wqkv,
                              dgin_ref, dqn_ref, dkn_ref, small, smallb, ob, qkvb, o_now, dqkv_now, (l1a, l1b), (t_a, t_b), (l2a, l2b),
                              load_sem, pair_send, pair_recv, turn_send, turn_recv, chip_send, chip_recv,
                              all_send, all_recv, small_send, small_recv)
    last_seq = seq == seqs - 1

    @pl.when(last_seq & (group == 0))
    def _():
        start(reducer.loads(0))

    @pl.when(last_seq & (group < groups - 1))
    def _():
        reducer.step(group)

    @pl.when(last_seq & last_group)
    def _():
        o_last[...] = o_now[...]
        dqkv_last[...] = dqkv_now[...]
        run(accumulate(groups - 1))
        finish(seqs - 1)
        reducer.step(groups - 1)
        reducer.finish()

        def drain(s, carry):
            for step in range(1, DEVICES):
                for kind in range(3):
                    incoming(kind, s, step).wait_send()
                for kind in range(2):
                    outgoing(kind, s, step, arrival=True).wait_recv()
            sent(0, s)
            return carry

        lax.fori_loop(0, seqs, drain, 0)
        for s in range(2):
            sent(1, seqs - 2 + s)


def start(copies):
    for copy in copies:
        copy.start()


def wait_send(copies):
    for copy in copies:
        copy.wait_send()


def wait_recv(copies):
    for copy in copies:
        copy.wait_recv()


class GradientReducer:
    def __init__(self, me, gathered, o_hbm, dqkv_hbm, small_out, dyb, ht_ref, wo, wqkv, dgin_ref, dqn_ref, dkn_ref,
                 small, smallb, ob, qkvb, o_now, dqkv_now, pair_in, turn_in, chip_in, load_sem, pair_send, pair_recv,
                 turn_send, turn_recv, chip_send, chip_recv, all_send, all_recv, small_send, small_recv):
        self.__dict__.update({k: v for k, v in locals().items() if k != 'self'})
        self.partner = peer_of(me, PARTNER)
        self.chips = DEVICES // 2
        self.stage = (wo, wqkv)
        self.sizes = [ref.shape[1] // 2 for ref in self.stage]
        self.early = ob.shape[0] - o_now.shape[0]

    def slot(self, place):
        return (place + DEVICES) % (DEVICES + 1)

    def half_of(self, i, half):
        return pl.ds(half * self.sizes[i], self.sizes[i])

    def loads(self, place):
        rows = pl.ds(0, self.early)
        return [pltpu.make_async_copy(self.o_hbm.at[place], self.ob.at[rows], self.load_sem.at[0]),
                pltpu.make_async_copy(self.dqkv_hbm.at[place], self.qkvb.at[rows], self.load_sem.at[1])]

    def pair(self, order):
        return [remote(self.stage[i].at[self.slot(2 * order)], self.pair_in[i].at[order % 2],
                       self.pair_send.at[i, order], self.pair_recv.at[i, order], self.partner) for i in range(2)]

    def turn(self, half):
        return [remote(self.stage[i].at[self.slot(1), self.half_of(i, half)], self.turn_in[i].at[half],
                       self.turn_send.at[i, half], self.turn_recv.at[i, half], peer_of(self.me, (X, Y)[half])) for i in range(2)]

    def chip(self, axis, half):
        return [remote(self.stage[i].at[self.slot(2 * axis + 3), self.half_of(i, half)], self.chip_in[i].at[axis, self.half_of(i, half)],
                       self.chip_send.at[i, axis, half], self.chip_recv.at[i, axis, half], peer_of(self.me, (X, Y)[axis])) for i in range(2)]

    def join_turn(self, axis, half):
        wait_recv(self.turn(half))
        for i in range(2):
            part = self.stage[i].at[self.slot(2 * axis + 3), self.half_of(i, half)]
            part[...] = (part[...].astype(F32) + self.turn_in[i][half].astype(F32)).astype(BF16)
        start(self.chip(axis, half))

    def step(self, place):
        for copy in self.loads(place):
            copy.wait()
        self.ob[self.early:] = self.o_now[...]
        self.qkvb[self.early:] = self.dqkv_now[...]
        tokens = self.ob.shape[0]
        into = self.slot(place)
        self.stage[0][into] = dot(self.ob[...], self.dyb[...].reshape(tokens, self.dyb.shape[2]), TN).astype(BF16)
        self.stage[1][into] = dot(self.ht_ref[...], self.qkvb[...]).astype(BF16)
        order = place // 2

        @pl.when(place < DEVICES - 1)
        def _():
            start(self.loads(place + 1))

        @pl.when(place % 2 == 0)
        def _():
            start(self.pair(order))

        @pl.when(place % 2 == 1)
        def _():
            wait_recv(self.pair(order))
            for i in range(2):
                for half in range(2):
                    part = self.stage[i].at[into, self.half_of(i, half)]
                    part[...] = (part[...].astype(F32) + self.pair_in[i][order % 2, self.half_of(i, half)].astype(F32)).astype(BF16)

        @pl.when(place == 1)
        def _():
            start(self.turn(0))
            start(self.turn(1))

        @pl.when(place == 3)
        def _():
            start(self.chip(0, 0))

        @pl.when(place == 5)
        def _():
            start(self.chip(1, 1))
            self.join_turn(0, 1)
            self.join_turn(1, 0)

    def small_copy(self, step, arrival=False):
        peer = peer_of(self.me, step)
        return remote(self.small, self.smallb.at[peer if arrival else self.me], self.small_send.at[step], self.small_recv.at[step], peer)

    def spread(self, half, slot, arrival=False):
        me, partner = self.me, self.partner
        x, y, diag = (peer_of(me, step) for step in (X, Y, DIAG))
        target = (x, y, (y, x)[half], partner, partner, partner, partner)[slot]
        owner = (me, me, (x, y)[half], me, x, y, diag)[slot]
        sender = (x, y, diag, partner, peer_of(partner, X), peer_of(partner, Y), peer_of(partner, DIAG))[slot]
        copies = []
        for i in range(2):
            part = self.half_of(i, half)
            src = self.stage[i].at[self.slot(DEVICES - 1), part] if slot in (0, 1, 3) else self.gathered[i].at[owner, part]
            copies.append(remote(src, self.gathered[i].at[sender if arrival else owner, part],
                                 self.all_send.at[i, half, slot], self.all_recv.at[i, half, slot], target))
        return copies

    def finish(self):
        small, smallb, spread = self.small, self.smallb, self.spread
        small[...] = jnp.zeros_like(small)
        lanes = self.dqn_ref.shape[1]
        rows = self.dgin_ref.shape[1] // lanes
        for row in range(rows):
            small[row:row + 1] = self.dgin_ref[:, row * lanes:(row + 1) * lanes]
        small[rows:rows + 1] = self.dqn_ref[...]
        small[rows + 1:rows + 2] = self.dkn_ref[...]
        for step in range(1, DEVICES):
            self.small_copy(step).start()

        result = self.slot(DEVICES - 1)
        for half in range(2):
            for axis in range(2):
                wait_recv(self.chip(axis, half))
            for i in range(2):
                rows_half = self.half_of(i, half)
                part = self.stage[i].at[result, rows_half]
                total = part[...].astype(F32) + self.chip_in[i][0, rows_half].astype(F32) + self.chip_in[i][1, rows_half].astype(F32)
                part[...] = total.astype(BF16)
            for slot in ((0, 1, 3), (1, 0, 3))[half]:
                start(spread(half, slot))
        local = [pltpu.make_async_copy(self.stage[i].at[result], self.gathered[i].at[self.me], self.load_sem.at[i]) for i in range(2)]
        start(local)

        for step in range(1, DEVICES):
            self.small_copy(step, arrival=True).wait_recv()
        smallb[self.me] = small[...]
        sums = smallb[0]
        for device in range(1, DEVICES):
            sums = sums + smallb[device]
        self.small_out[...] = sums

        for half, slot, onward in ((0, 0, (2, 4)), (1, 1, (2, 5)), (1, 0, (4,)), (0, 1, (5,)), (0, 2, (6,)), (1, 2, (6,))):
            wait_recv(spread(half, slot, arrival=True))
            for forward in onward:
                start(spread(half, forward))
        for copy in local:
            copy.wait()
        for half in range(2):
            for slot in (3, 4, 5, 6):
                wait_recv(spread(half, slot, arrival=True))
            for slot in range(7):
                wait_send(spread(half, slot))
            wait_send(self.turn(half))
            for axis in range(2):
                wait_send(self.chip(axis, half))
        for order in range(self.chips):
            wait_send(self.pair(order))
        for step in range(1, DEVICES):
            self.small_copy(step).wait_send()


def block_call(x, dy, pos, gains, w_q, w_k, w_v, w_o, head_dim):
    batch, piece, model = x.shape
    seqs, seq_len = batch // DEVICES, piece * DEVICES
    q_width, kv_width = w_q.shape[1], w_k.shape[1]
    groups = kv_width // head_dim
    q_cols = q_width // groups
    tokens = seqs * seq_len
    width = q_cols + 2 * head_dim
    fixed = lambda s, g: (0, 0)
    bf = lambda *shape: jax.ShapeDtypeStruct(shape, BF16)
    f32 = lambda *shape: jax.ShapeDtypeStruct(shape, F32)
    anywhere = pl.BlockSpec(memory_space=pl.ANY)
    flops = 4 * tokens * model * (q_width * 2 + kv_width * 2) + 12 * tokens * seq_len * q_width
    vb = lambda *shape: pltpu.VMEM(shape, BF16)
    vf = lambda *shape: pltpu.VMEM(shape, F32)
    dma = lambda *shape: pltpu.SemaphoreType.DMA(shape)
    return pl.pallas_call(
        block_kernel,
        grid=(seqs, groups),
        in_specs=[
            anywhere, anywhere, anywhere, anywhere, anywhere, anywhere, anywhere,
        ] + [pl.BlockSpec(t.shape, fixed) for t in gains],
        out_specs=[anywhere] * 6 + [pl.BlockSpec((16, head_dim), fixed)],
        out_shape=[
            bf(batch, piece, model), bf(batch, piece, model),
            bf(groups, q_cols, model), bf(groups, model, width),
            bf(groups, tokens - seq_len, q_cols), bf(groups, tokens - seq_len, width),
            f32(16, head_dim),
        ],
        scratch_shapes=[
            vb(seqs, seq_len, model), vb(seqs, seq_len, model), vb(2, seq_len, model),
            vf(seqs, DEVICES, 8, head_dim),
            vb(groups + 1, model, width), vb(groups + 1, q_cols, model),
            vb(seq_len, model), vb(model, tokens),
            vf(seq_len, head_dim), vf(seq_len, head_dim), vf(seq_len, head_dim), vf(seq_len, head_dim),
            vf(seq_len, model), vf(seq_len, model),
            vf(seq_len, q_cols), vf(seq_len, head_dim), vb(seq_len, head_dim), vb(seq_len, q_cols),
            vb(seq_len, head_dim), vb(seq_len, q_cols),
            vb(seq_len, q_cols), vb(seq_len, width), vb(seq_len, q_cols), vb(seq_len, width),
            vb(2, seq_len, q_cols), vb(2, seq_len, width),
            vf(1, model), vf(1, head_dim), vf(1, head_dim), vf(16, head_dim), vf(DEVICES, 16, head_dim),
            vb(tokens, q_cols), vb(tokens, width),
            vb(2, q_cols, model), vb(2, model, width),
            vb(2, q_cols // 2, model), vb(2, model // 2, width),
            vb(2, q_cols, model), vb(2, model, width),
            pltpu.SemaphoreType.DMA((4, groups)),
            pltpu.SemaphoreType.DMA((3, seqs, DEVICES)),
            pltpu.SemaphoreType.DMA((3, seqs, DEVICES)),
            pltpu.SemaphoreType.DMA((2, seqs, DEVICES)),
            pltpu.SemaphoreType.DMA((2, seqs, DEVICES)),
            dma(2, 2), dma(2), dma(2, 4), dma(2, 4), dma(2, 2), dma(2, 2), dma(2, 2, 2), dma(2, 2, 2),
            dma(2, 2, 7), dma(2, 2, 7), dma(DEVICES), dma(DEVICES),
        ],
        compiler_params=pltpu.CompilerParams(
            dimension_semantics=("arbitrary", "arbitrary"), vmem_limit_bytes=67_000_000,
            collective_id=0, has_side_effects=True),
        cost_estimate=pl.CostEstimate(flops=flops, bytes_accessed=50_000_000, transcendentals=tokens * seq_len * 8),
        name="block",
    )(x, dy, pos, w_q, w_k, w_v, w_o, *gains)


def widen_kernel(ga_ref, gb_ref, small_ref, out_in, gi_in, wq_ref, wk_ref, wv_ref, wo_ref, dgin_ref, dqn_ref, dkn_ref, out_ref, gi_ref):
    @pl.when(pl.program_id(0) == 0)
    def _():
        lanes = small_ref.shape[1]
        rows = dgin_ref.shape[1] // lanes
        for row in range(rows):
            dgin_ref[:, row * lanes:(row + 1) * lanes] = small_ref[row:row + 1]
        dqn_ref[...] = small_ref[rows:rows + 1]
        dkn_ref[...] = small_ref[rows + 1:rows + 2]

    q_cols, head_dim = wq_ref.shape[1], wk_ref.shape[1]
    wo_ref[...] = ga_ref[0].astype(F32)
    wq_ref[...] = gb_ref[0, :, :q_cols].astype(F32)
    wk_ref[...] = gb_ref[0, :, q_cols:q_cols + head_dim].astype(F32)
    wv_ref[...] = gb_ref[0, :, q_cols + head_dim:].astype(F32)
    out_ref[...] = out_in[...]
    gi_ref[...] = gi_in[...]


def widen_call(ga, gb, small, out, gi):
    groups, q_cols, model = ga.shape
    width = gb.shape[2]
    head_dim = (width - q_cols) // 2
    parts = 2
    batch, piece, _ = out.shape
    f32 = lambda *shape: jax.ShapeDtypeStruct(shape, F32)
    across = lambda i: (i % parts, i // parts)
    fixed = lambda i: (0, 0)
    act = pl.BlockSpec((batch // (groups * parts), piece, model), lambda i: (i, 0, 0))
    return pl.pallas_call(
        widen_kernel,
        grid=(groups * parts,),
        in_specs=[pl.BlockSpec((1, q_cols // parts, model), lambda i: (i // parts, i % parts, 0)),
                  pl.BlockSpec((1, model // parts, width), lambda i: (i // parts, i % parts, 0)),
                  pl.BlockSpec(small.shape, fixed), act, act],
        out_specs=[pl.BlockSpec((model // parts, q_cols), across), pl.BlockSpec((model // parts, head_dim), across),
                   pl.BlockSpec((model // parts, head_dim), across), pl.BlockSpec((q_cols // parts, model), lambda i: (i, 0))]
        + [pl.BlockSpec((1, n), fixed) for n in (model, head_dim, head_dim)] + [act, act],
        out_shape=[f32(model, groups * q_cols), f32(model, groups * head_dim), f32(model, groups * head_dim),
                   f32(groups * q_cols, model), f32(1, model), f32(1, head_dim), f32(1, head_dim),
                   jax.ShapeDtypeStruct(out.shape, out.dtype), jax.ShapeDtypeStruct(gi.shape, gi.dtype)],
        compiler_params=pltpu.CompilerParams(dimension_semantics=("arbitrary",)),
        name="widen",
    )(ga, gb, small, out, gi)


def solution(mesh):
    seq_spec = P(None, 'sp', None)
    replicated = P()

    def shard_body(hidden_in, grad_out, positions, w_q, w_k, w_v, w_o, g_in, q_norm, k_norm):
        batch, seq_dev, model_dim = hidden_in.shape
        head_dim = q_norm.shape[0]
        exponents = jnp.arange(0, head_dim, 2).astype(F32) / head_dim
        inv_freq = jnp.power(ROPE_THETA, -exponents)
        gains = (g_in[None], q_norm[None], k_norm[None], jnp.concatenate([inv_freq, inv_freq])[None])
        pos = jnp.broadcast_to(jnp.pad(positions.astype(F32), ((0, 0), (0, head_dim - seq_dev)))[:, None, :], (batch, 8, head_dim))
        hidden_out, grad_in, ga, gb, _, _, small = block_call(hidden_in, grad_out, pos, gains, w_q, w_k, w_v, w_o, head_dim)
        grad_wq, grad_wk, grad_wv, grad_wo, dgin, dqn, dkn, hidden_out, grad_in = widen_call(ga, gb, small, hidden_out, grad_in)
        return hidden_out, grad_in, grad_wq, grad_wk, grad_wv, grad_wo, dgin[0], dqn[0], dkn[0]

    return jax.shard_map(shard_body, mesh=mesh,
                         in_specs=(seq_spec, seq_spec, P(None, 'sp'), replicated, replicated, replicated, replicated, replicated, replicated, replicated),
                         out_specs=(seq_spec, seq_spec, replicated, replicated, replicated, replicated, replicated, replicated, replicated),
                         check_vma=False)
```

```python
import functools
import jax
import jax.numpy as jnp
from jax import lax
from jax.experimental import pallas as pl
from jax.experimental.pallas import tpu as pltpu
from jax.sharding import PartitionSpec as P

EPSILON = 1e-6
ROPE_THETA = 1000000.0
NEG_LARGE = -1e30
LOG2_E = 1.4426950408889634
NN, NT, TN = ((((a,), (b,)), ((), ())) for a, b in ((1, 0), (1, 1), (0, 0)))
ROW_BLOCK = 256
DEVICES = 8
BF16 = jnp.bfloat16
F32 = jnp.float32


def dot(a, b, dims=NN):
    return lax.dot_general(a, b, dims, preferred_element_type=F32)


def peer_of(me, step):
    core, x, y = me % 2, (me // 2) % 2, me // 4
    return ((y + step // 4) % 2) * 4 + ((x + (step // 2) % 2) % 2) * 2 + (core + step % 2) % 2


X, Y, DIAG, PARTNER = 2, 4, 6, 1
SEND_ORDER = (2, 4, 6, 3, 5, 7, 1, 0)


def chip_peer(me, order):
    return peer_of(me, (1 - order // 2) * X + ((order + 1) % 2) * Y)


def group_at(me, place):
    return peer_of(chip_peer(me, place // 2), 1 - place % 2)


def entry_barrier(me):
    barrier = pltpu.get_barrier_semaphore()
    for step in range(1, DEVICES):
        pl.semaphore_signal(barrier, inc=1, device_id=(peer_of(me, step),), device_id_type=pl.DeviceIdType.MESH)
    pl.semaphore_wait(barrier, DEVICES - 1)


def remote(src, dst, send, recv, device):
    return pltpu.make_async_remote_copy(src_ref=src, dst_ref=dst, send_sem=send, recv_sem=recv,
                                        device_id=(device,), device_id_type=pl.DeviceIdType.MESH)


def block_kernel(x_hbm, dy_hbm, pos_hbm, wq_hbm, wk_hbm, wv_hbm, wo_hbm, gin_ref, qn_ref, kn_ref, freq_ref,
                 out_hbm, gi_hbm, ga_hbm, gb_hbm, o_hbm, dqkv_hbm, small_out,
                 xb, dyb, gib, posb, wqkv, wo, h_ref, ht_ref, rope_cos, rope_sin, next_cos, next_sin, out_acc, dh_acc,
                 q_next, k_next, v_next, do_next, v_now, do_now, o_now, dqkv_now, o_last, dqkv_last, o_stage, dqkv_stage,
                 dgin_ref, dqn_ref, dkn_ref, small, smallb, ob, qkvb, l1a, l1b, t_a, t_b, l2a, l2b,
                 weight_sem, in_send, in_recv, out_send, out_recv, store_sem, load_sem, pair_send, pair_recv,
                 turn_send, turn_recv, chip_send, chip_recv, all_send, all_recv, small_send, small_recv):
    seq, group = pl.program_id(0), pl.program_id(1)
    seqs, groups = pl.num_programs(0), pl.num_programs(1)
    me = lax.axis_index('sp')
    head_dim, model = dqn_ref.shape[1], dgin_ref.shape[1]
    q_gain, k_gain, in_gain = (ref[...].astype(F32) for ref in (qn_ref, kn_ref, gin_ref))
    q_cols = o_now.shape[1]
    per_kv = q_cols // head_dim
    seq_len = xb.shape[1]
    piece = seq_len // DEVICES
    scale = head_dim ** -0.5
    half = head_dim // 2
    tiles = [slice(i, i + ROW_BLOCK) for i in range(0, seq_len, ROW_BLOCK)]

    def rows_of(device):
        return pl.ds(pl.multiple_of(device * piece, piece), piece)

    def incoming(kind, s, step, arrival=False):
        peer = peer_of(me, step)
        src = (x_hbm, dy_hbm, pos_hbm)[kind].at[DEVICES * s + peer]

        def landing(device):
            return posb.at[s, device] if kind == 2 else (xb, dyb)[kind].at[s, rows_of(device)]

        if step == 0:
            return pltpu.make_async_copy(src, landing(me), in_recv.at[kind, s, 0])
        return remote(src, landing(peer if arrival else me), in_send.at[kind, s, step], in_recv.at[kind, s, step], peer)

    def outgoing(kind, s, step, arrival=False):
        peer = peer_of(me, step)
        src = xb.at[s, rows_of(peer)] if kind == 0 else gib.at[s % 2, rows_of(peer)]
        dst = (out_hbm, gi_hbm)[kind]
        if step == 0:
            return pltpu.make_async_copy(src, dst.at[DEVICES * s + me], out_recv.at[kind, s, 0])
        return remote(src, dst.at[DEVICES * s + (peer if arrival else me)],
                      out_send.at[kind, s, step], out_recv.at[kind, s, step], peer)

    def sent(kind, s):
        outgoing(kind, s, 0).wait()
        for step in range(1, DEVICES):
            outgoing(kind, s, step).wait_send()

    def weight_loads():
        copies = []
        for place in range(DEVICES):
            g = group_at(me, place)
            wide = pl.ds(pl.multiple_of(g * q_cols, q_cols), q_cols)
            narrow = pl.ds(pl.multiple_of(g * head_dim, head_dim), head_dim)
            parts = ((wq_hbm.at[:, wide], wqkv.at[place, :, pl.ds(0, q_cols)]),
                     (wk_hbm.at[:, narrow], wqkv.at[place, :, pl.ds(q_cols, head_dim)]),
                     (wv_hbm.at[:, narrow], wqkv.at[place, :, pl.ds(q_cols + head_dim, head_dim)]),
                     (wo_hbm.at[wide], wo.at[place]))
            copies += [pltpu.make_async_copy(src, dst, weight_sem.at[i, place]) for i, (src, dst) in enumerate(parts)]
        return copies

    def arrive(kind, s):
        for step in range(DEVICES):
            if step == 0:
                incoming(kind, s, 0).wait()
            else:
                incoming(kind, s, step, arrival=True).wait_recv()

    def prepare(s):
        arrive(2, s)
        on_diag = lax.broadcasted_iota(jnp.int32, (piece, head_dim), 0) == lax.broadcasted_iota(jnp.int32, (piece, head_dim), 1)
        low = lax.broadcasted_iota(jnp.int32, (piece, head_dim), 1) < half
        half_count = DEVICES // 2

        def column(device):
            row = jnp.broadcast_to(posb[s, device, 0:1, :], (piece, head_dim))
            return jnp.sum(jnp.where(on_diag, row, 0.0), axis=-1, keepdims=True)

        for device in range(half_count):
            angles = jnp.where(low, column(device), column(device + half_count)) * freq_ref[...]
            cos, sin = jnp.cos(angles), jnp.sin(angles)
            cos_turned, sin_turned = pltpu.roll(cos, half, 1), pltpu.roll(sin, half, 1)
            first = slice(device * piece, (device + 1) * piece)
            second = slice((device + half_count) * piece, (device + half_count + 1) * piece)
            next_cos[first, :] = jnp.where(low, cos, cos_turned)
            next_sin[first, :] = jnp.where(low, -sin, sin_turned)
            next_cos[second, :] = jnp.where(low, cos_turned, cos)
            next_sin[second, :] = jnp.where(low, -sin_turned, sin)
        arrive(0, s)
        x = xb[s].astype(F32)
        inv = lax.rsqrt(jnp.mean(x * x, axis=-1, keepdims=True) + EPSILON)
        h_ref[...] = (x * inv * in_gain).astype(BF16)

    def project(s, g):
        def q_rows(rows):
            q_next[rows] = dot(h_ref[rows], wqkv[g, :, :q_cols])

        def kv_rows(rows):
            kv = dot(h_ref[rows], wqkv[g, :, q_cols:])
            k_next[rows] = kv[:, :head_dim]
            v_next[rows] = kv[:, head_dim:].astype(BF16)

        def do_rows(rows):
            do_next[rows] = dot(dyb[s, rows], wo[g], NT).astype(BF16)

        return [functools.partial(f, rows) for f in (q_rows, kv_rows, do_rows) for rows in tiles]

    def accumulate(g):
        def out_cols(cols):
            out_acc[:, cols] += dot(o_last[...], wo[g, :, cols])

        def dh_cols(cols):
            dh_acc[:, cols] += dot(dqkv_last[...], wqkv[g, cols, :], NT)

        columns = [slice(c, c + 256) for c in range(0, out_acc.shape[1], 256)]
        return [functools.partial(f, cols) for f in (out_cols, dh_cols) for cols in columns]

    def run(products):
        for product in products:
            product()

    def finish(s):
        x = xb[s].astype(F32)
        inv = lax.rsqrt(jnp.mean(x * x, axis=-1, keepdims=True) + EPSILON)
        unit = x * inv
        xb[s] = (x + out_acc[...]).astype(BF16)
        d_norm = dh_acc[...]
        dgin_ref[...] += jnp.sum(d_norm * unit, axis=0, keepdims=True)
        d_unit = d_norm * in_gain
        grad = inv * (d_unit - unit * jnp.mean(d_unit * unit, axis=-1, keepdims=True))

        @pl.when(s >= 2)
        def _():
            sent(1, s - 2)

        gib[s % 2] = (dyb[s].astype(F32) + grad).astype(BF16)
        for kind in range(2):
            for step in SEND_ORDER:
                outgoing(kind, s, step).start()

    @pl.when((seq == 0) & (group == 0))
    def _():
        entry_barrier(me)

        def send_all(s, carry):
            for kind in (2, 0, 1):
                for step in SEND_ORDER:
                    incoming(kind, s, step).start()
            return carry

        lax.fori_loop(0, seqs, send_all, 0)
        for copy in weight_loads():
            copy.start()
        dgin_ref[...] = jnp.zeros_like(dgin_ref)
        dqn_ref[...] = jnp.zeros_like(dqn_ref)
        dkn_ref[...] = jnp.zeros_like(dkn_ref)
        o_now[...] = jnp.zeros_like(o_now)
        dqkv_now[...] = jnp.zeros_like(dqkv_now)
        out_acc[...] = jnp.zeros_like(out_acc)
        dh_acc[...] = jnp.zeros_like(dh_acc)
        for copy in weight_loads():
            copy.wait()
        prepare(0)
        first = project(0, 0)
        run(first[:4])
        arrive(1, 0)
        run(first[4:])

    @pl.when(group == 0)
    def _():
        rope_cos[...] = next_cos[...]
        rope_sin[...] = next_sin[...]
        ht_ref[:, pl.ds(pl.multiple_of(seq * seq_len, seq_len), seq_len)] = h_ref[...].T

    last_group = group == groups - 1

    @pl.when(last_group & (seq < seqs - 1))
    def _():
        prepare(seq + 1)
        arrive(1, seq + 1)

    cos, sin = rope_cos[...], rope_sin[...]

    def norm_rotate(t, gain):
        inv = lax.rsqrt(jnp.mean(t * t, axis=-1, keepdims=True) + EPSILON)
        unit = t * inv
        scaled = unit * gain
        return (scaled * cos + pltpu.roll(scaled, half, 1) * sin).astype(BF16), unit, inv

    def norm_rotate_back(grad, unit, inv, gain):
        d_scaled = grad * cos - pltpu.roll(grad, half, 1) * sin
        d_gain = jnp.sum(d_scaled * unit, axis=0, keepdims=True)
        d_unit = d_scaled * gain
        return inv * (d_unit - unit * jnp.mean(d_unit * unit, axis=-1, keepdims=True)), d_gain

    step_id = seq * groups + group
    slot = step_id % 2

    def stores(step):
        g, rows = step % groups, pl.ds(pl.multiple_of((step // groups) * seq_len, seq_len), seq_len)
        return [pltpu.make_async_copy(o_stage.at[step % 2], o_hbm.at[g, rows], store_sem.at[0, step % 2]),
                pltpu.make_async_copy(dqkv_stage.at[step % 2], dqkv_hbm.at[g, rows], store_sem.at[1, step % 2])]

    stored = (seqs - 1) * groups

    @pl.when((step_id >= 2) & (step_id - 2 < stored))
    def _():
        for copy in stores(step_id - 2):
            copy.wait()

    @pl.when((step_id >= 1) & (step_id - 1 < stored))
    def _():
        for copy in stores(step_id - 1):
            copy.start()

    v_now[...] = v_next[...]
    do_now[...] = do_next[...]
    o_last[...] = o_now[...]
    dqkv_last[...] = dqkv_now[...]

    ahead = project(jnp.minimum(seq + last_group.astype(jnp.int32), seqs - 1), (group + 1) % groups)
    behind = accumulate((group + groups - 1) % groups)
    lanes = [slice(head * head_dim, (head + 1) * head_dim) for head in range(per_kv)]
    stacked = per_kv * ROW_BLOCK
    key_id = lax.broadcasted_iota(jnp.int32, (ROW_BLOCK, stacked), 0)
    causal = key_id <= lax.broadcasted_iota(jnp.int32, (ROW_BLOCK, stacked), 1) % ROW_BLOCK
    blocks = len(tiles)

    run(behind[:6])
    k_rot, k_unit, k_inv = norm_rotate(k_next[...], k_gain)
    q_parts = [norm_rotate(q_next[:, lane], q_gain) for lane in lanes]
    q_tile = [jnp.concatenate([part[0][tile] for part in q_parts], axis=0) for tile in tiles]
    do_tile = [jnp.concatenate([do_now[tile, lane] for lane in lanes], axis=0) for tile in tiles]
    v_cols, k_cols = v_now[...].T, k_rot.T
    fill = [ahead[0:2], behind[6:7], behind[7:8] + ahead[2:3], ahead[3:4]]
    dp_all = [dot(v_now[:(i + 1) * ROW_BLOCK], do_tile[i], NT) for i in range(blocks)]
    s_all = [dot(k_rot[:(i + 1) * ROW_BLOCK], q_tile[i], NT) for i in range(blocks)]

    def masked(i):
        diagonal = jnp.where(causal, s_all[i][i * ROW_BLOCK:], NEG_LARGE)
        return diagonal if i == 0 else jnp.concatenate([s_all[i][:i * ROW_BLOCK], diagonal], axis=0)

    def store_output(i, o_i):
        for head, lane in enumerate(lanes):
            o_head = o_i[head * ROW_BLOCK:(head + 1) * ROW_BLOCK]
            o_stage[slot, tiles[i], lane] = o_head
            o_now[tiles[i], lane] = o_head

    def add_rows(total, part):
        keys = part.shape[0]
        if total is None:
            return part
        return jnp.concatenate([total + part[:total.shape[0]], part[total.shape[0]:keys]], axis=0)

    dk_all, dv_all, dq_tile = None, None, []
    for i in range(blocks):
        keys = (i + 1) * ROW_BLOCK
        s = masked(i)
        e = jnp.exp2((s - jnp.max(s, axis=0, keepdims=True)) * (scale * LOG2_E))
        p = e * (1.0 / jnp.sum(e, axis=0, keepdims=True))
        p_bf16 = p.astype(BF16)
        run(fill[2 * i])
        store_output(i, dot(v_cols[:, :keys], p_bf16).astype(BF16).T)
        dv_all = add_rows(dv_all, dot(p_bf16, do_tile[i]))
        delta = jnp.sum(p * dp_all[i], axis=0, keepdims=True)
        ds = (p * (dp_all[i] - delta)).astype(BF16)
        run(fill[2 * i + 1])
        dq_tile.append(dot(k_cols[:, :keys], ds).T)
        dk_all = add_rows(dk_all, dot(ds, q_tile[i]))
    run(ahead[4:])
    for head, lane in enumerate(lanes):
        dq_head = jnp.concatenate([dq[head * ROW_BLOCK:(head + 1) * ROW_BLOCK] for dq in dq_tile], axis=0)
        dq_head, d_gain = norm_rotate_back(dq_head * scale, q_parts[head][1], q_parts[head][2], q_gain)
        dqn_ref[...] += d_gain
        dq_head = dq_head.astype(BF16)
        dqkv_stage[slot, :, lane] = dq_head
        dqkv_now[:, lane] = dq_head
    dk_head, d_gain = norm_rotate_back(dk_all * scale, k_unit, k_inv, k_gain)
    dkn_ref[...] += d_gain
    dk_head = dk_head.astype(BF16)
    dqkv_stage[slot, :, q_cols:q_cols + head_dim] = dk_head
    dqkv_now[:, q_cols:q_cols + head_dim] = dk_head
    dv_head = dv_all.astype(BF16)
    dqkv_stage[slot, :, q_cols + head_dim:] = dv_head
    dqkv_now[:, q_cols + head_dim:] = dv_head

    @pl.when((group == 0) & (seq > 0))
    def _():
        finish(seq - 1)
        out_acc[...] = jnp.zeros_like(out_acc)
        dh_acc[...] = jnp.zeros_like(dh_acc)

    reducer = GradientReducer(me, (ga_hbm, gb_hbm), o_hbm, dqkv_hbm, small_out, dyb, ht_ref, wo, wqkv,
                              dgin_ref, dqn_ref, dkn_ref, small, smallb, ob, qkvb, o_now, dqkv_now, (l1a, l1b), (t_a, t_b), (l2a, l2b),
                              load_sem, pair_send, pair_recv, turn_send, turn_recv, chip_send, chip_recv,
                              all_send, all_recv, small_send, small_recv)
    last_seq = seq == seqs - 1

    @pl.when(last_seq & (group == 0))
    def _():
        start(reducer.loads(0))

    @pl.when(last_seq & (group < groups - 1))
    def _():
        reducer.step(group)

    @pl.when(last_seq & last_group)
    def _():
        o_last[...] = o_now[...]
        dqkv_last[...] = dqkv_now[...]
        run(accumulate(groups - 1))
        finish(seqs - 1)
        reducer.step(groups - 1)
        reducer.finish()

        def drain(s, carry):
            for step in range(1, DEVICES):
                for kind in range(3):
                    incoming(kind, s, step).wait_send()
                for kind in range(2):
                    outgoing(kind, s, step, arrival=True).wait_recv()
            sent(0, s)
            return carry

        lax.fori_loop(0, seqs, drain, 0)
        for s in range(2):
            sent(1, seqs - 2 + s)


def start(copies):
    for copy in copies:
        copy.start()


def wait_send(copies):
    for copy in copies:
        copy.wait_send()


def wait_recv(copies):
    for copy in copies:
        copy.wait_recv()


class GradientReducer:
    def __init__(self, me, gathered, o_hbm, dqkv_hbm, small_out, dyb, ht_ref, wo, wqkv, dgin_ref, dqn_ref, dkn_ref,
                 small, smallb, ob, qkvb, o_now, dqkv_now, pair_in, turn_in, chip_in, load_sem, pair_send, pair_recv,
                 turn_send, turn_recv, chip_send, chip_recv, all_send, all_recv, small_send, small_recv):
        self.__dict__.update({k: v for k, v in locals().items() if k != 'self'})
        self.partner = peer_of(me, PARTNER)
        self.chips = DEVICES // 2
        self.stage = (wo, wqkv)
        self.sizes = [ref.shape[1] // 2 for ref in self.stage]
        self.early = ob.shape[0] - o_now.shape[0]

    def slot(self, place):
        return (place + DEVICES) % (DEVICES + 1)

    def half_of(self, i, half):
        return pl.ds(half * self.sizes[i], self.sizes[i])

    def loads(self, place):
        rows = pl.ds(0, self.early)
        return [pltpu.make_async_copy(self.o_hbm.at[place], self.ob.at[rows], self.load_sem.at[0]),
                pltpu.make_async_copy(self.dqkv_hbm.at[place], self.qkvb.at[rows], self.load_sem.at[1])]

    def pair(self, order):
        return [remote(self.stage[i].at[self.slot(2 * order)], self.pair_in[i].at[order % 2],
                       self.pair_send.at[i, order], self.pair_recv.at[i, order], self.partner) for i in range(2)]

    def turn(self, half):
        return [remote(self.stage[i].at[self.slot(1), self.half_of(i, half)], self.turn_in[i].at[half],
                       self.turn_send.at[i, half], self.turn_recv.at[i, half], peer_of(self.me, (X, Y)[half])) for i in range(2)]

    def chip(self, axis, half):
        return [remote(self.stage[i].at[self.slot(2 * axis + 3), self.half_of(i, half)], self.chip_in[i].at[axis, self.half_of(i, half)],
                       self.chip_send.at[i, axis, half], self.chip_recv.at[i, axis, half], peer_of(self.me, (X, Y)[axis])) for i in range(2)]

    def join_turn(self, axis, half):
        wait_recv(self.turn(half))
        for i in range(2):
            part = self.stage[i].at[self.slot(2 * axis + 3), self.half_of(i, half)]
            part[...] = (part[...].astype(F32) + self.turn_in[i][half].astype(F32)).astype(BF16)
        start(self.chip(axis, half))

    def step(self, place):
        for copy in self.loads(place):
            copy.wait()
        self.ob[self.early:] = self.o_now[...]
        self.qkvb[self.early:] = self.dqkv_now[...]
        tokens = self.ob.shape[0]
        into = self.slot(place)
        self.stage[0][into] = dot(self.ob[...], self.dyb[...].reshape(tokens, self.dyb.shape[2]), TN).astype(BF16)
        self.stage[1][into] = dot(self.ht_ref[...], self.qkvb[...]).astype(BF16)
        order = place // 2

        @pl.when(place < DEVICES - 1)
        def _():
            start(self.loads(place + 1))

        @pl.when(place % 2 == 0)
        def _():
            start(self.pair(order))

        @pl.when(place % 2 == 1)
        def _():
            wait_recv(self.pair(order))
            for i in range(2):
                for half in range(2):
                    part = self.stage[i].at[into, self.half_of(i, half)]
                    part[...] = (part[...].astype(F32) + self.pair_in[i][order % 2, self.half_of(i, half)].astype(F32)).astype(BF16)

        @pl.when(place == 1)
        def _():
            start(self.turn(0))
            start(self.turn(1))

        @pl.when(place == 3)
        def _():
            start(self.chip(0, 0))

        @pl.when(place == 5)
        def _():
            start(self.chip(1, 1))
            self.join_turn(0, 1)
            self.join_turn(1, 0)

    def small_copy(self, step, arrival=False):
        peer = peer_of(self.me, step)
        return remote(self.small, self.smallb.at[peer if arrival else self.me], self.small_send.at[step], self.small_recv.at[step], peer)

    def spread(self, half, slot, arrival=False):
        me, partner = self.me, self.partner
        x, y, diag = (peer_of(me, step) for step in (X, Y, DIAG))
        target = (x, y, (y, x)[half], partner, partner, partner, partner)[slot]
        owner = (me, me, (x, y)[half], me, x, y, diag)[slot]
        sender = (x, y, diag, partner, peer_of(partner, X), peer_of(partner, Y), peer_of(partner, DIAG))[slot]
        copies = []
        for i in range(2):
            part = self.half_of(i, half)
            src = self.stage[i].at[self.slot(DEVICES - 1), part] if slot in (0, 1, 3) else self.gathered[i].at[owner, part]
            copies.append(remote(src, self.gathered[i].at[sender if arrival else owner, part],
                                 self.all_send.at[i, half, slot], self.all_recv.at[i, half, slot], target))
        return copies

    def finish(self):
        small, smallb, spread = self.small, self.smallb, self.spread
        small[...] = jnp.zeros_like(small)
        lanes = self.dqn_ref.shape[1]
        rows = self.dgin_ref.shape[1] // lanes
        for row in range(rows):
            small[row:row + 1] = self.dgin_ref[:, row * lanes:(row + 1) * lanes]
        small[rows:rows + 1] = self.dqn_ref[...]
        small[rows + 1:rows + 2] = self.dkn_ref[...]
        for step in range(1, DEVICES):
            self.small_copy(step).start()

        result = self.slot(DEVICES - 1)
        for half in range(2):
            for axis in range(2):
                wait_recv(self.chip(axis, half))
            for i in range(2):
                rows_half = self.half_of(i, half)
                part = self.stage[i].at[result, rows_half]
                total = part[...].astype(F32) + self.chip_in[i][0, rows_half].astype(F32) + self.chip_in[i][1, rows_half].astype(F32)
                part[...] = total.astype(BF16)
            for slot in ((0, 1, 3), (1, 0, 3))[half]:
                start(spread(half, slot))
        local = [pltpu.make_async_copy(self.stage[i].at[result], self.gathered[i].at[self.me], self.load_sem.at[i]) for i in range(2)]
        start(local)

        for step in range(1, DEVICES):
            self.small_copy(step, arrival=True).wait_recv()
        smallb[self.me] = small[...]
        sums = smallb[0]
        for device in range(1, DEVICES):
            sums = sums + smallb[device]
        self.small_out[...] = sums

        for half, slot, onward in ((0, 0, (2, 4)), (1, 1, (2, 5)), (1, 0, (4,)), (0, 1, (5,)), (0, 2, (6,)), (1, 2, (6,))):
            wait_recv(spread(half, slot, arrival=True))
            for forward in onward:
                start(spread(half, forward))
        for copy in local:
            copy.wait()
        for half in range(2):
            for slot in (3, 4, 5, 6):
                wait_recv(spread(half, slot, arrival=True))
            for slot in range(7):
                wait_send(spread(half, slot))
            wait_send(self.turn(half))
            for axis in range(2):
                wait_send(self.chip(axis, half))
        for order in range(self.chips):
            wait_send(self.pair(order))
        for step in range(1, DEVICES):
            self.small_copy(step).wait_send()


def block_call(x, dy, pos, gains, w_q, w_k, w_v, w_o, head_dim):
    batch, piece, model = x.shape
    seqs, seq_len = batch // DEVICES, piece * DEVICES
    q_width, kv_width = w_q.shape[1], w_k.shape[1]
    groups = kv_width // head_dim
    q_cols = q_width // groups
    tokens = seqs * seq_len
    width = q_cols + 2 * head_dim
    fixed = lambda s, g: (0, 0)
    bf = lambda *shape: jax.ShapeDtypeStruct(shape, BF16)
    f32 = lambda *shape: jax.ShapeDtypeStruct(shape, F32)
    anywhere = pl.BlockSpec(memory_space=pl.ANY)
    flops = 4 * tokens * model * (q_width * 2 + kv_width * 2) + 12 * tokens * seq_len * q_width
    vb = lambda *shape: pltpu.VMEM(shape, BF16)
    vf = lambda *shape: pltpu.VMEM(shape, F32)
    dma = lambda *shape: pltpu.SemaphoreType.DMA(shape)
    twice = lambda shape: [shape] * 2
    return pl.pallas_call(
        block_kernel,
        grid=(seqs, groups),
        in_specs=[
            anywhere, anywhere, anywhere, anywhere, anywhere, anywhere, anywhere,
        ] + [pl.BlockSpec(t.shape, fixed) for t in gains],
        out_specs=[anywhere] * 6 + [pl.BlockSpec((16, head_dim), fixed)],
        out_shape=[
            bf(batch, piece, model), bf(batch, piece, model),
            bf(groups, q_cols, model), bf(groups, model, width),
            bf(groups, tokens - seq_len, q_cols), bf(groups, tokens - seq_len, width),
            f32(16, head_dim),
        ],
        scratch_shapes=[
            vb(seqs, seq_len, model), vb(seqs, seq_len, model), vb(2, seq_len, model),
            vf(seqs, DEVICES, 8, head_dim),
            vb(groups + 1, model, width), vb(groups + 1, q_cols, model),
            vb(seq_len, model), vb(model, tokens),
            vf(seq_len, head_dim), vf(seq_len, head_dim), vf(seq_len, head_dim), vf(seq_len, head_dim),
            vf(seq_len, model), vf(seq_len, model),
            vf(seq_len, q_cols), vf(seq_len, head_dim), vb(seq_len, head_dim), vb(seq_len, q_cols),
            vb(seq_len, head_dim), vb(seq_len, q_cols),
            vb(seq_len, q_cols), vb(seq_len, width), vb(seq_len, q_cols), vb(seq_len, width),
            vb(2, seq_len, q_cols), vb(2, seq_len, width),
            vf(1, model), vf(1, head_dim), vf(1, head_dim), vf(16, head_dim), vf(DEVICES, 16, head_dim),
            vb(tokens, q_cols), vb(tokens, width),
            vb(2, q_cols, model), vb(2, model, width),
            vb(2, q_cols // 2, model), vb(2, model // 2, width),
            vb(2, q_cols, model), vb(2, model, width),
            dma(4, groups), *twice(dma(3, seqs, DEVICES)), *twice(dma(2, seqs, DEVICES)),
            dma(2, 2), dma(2), *twice(dma(2, DEVICES // 2)), *twice(dma(2, 2)), *twice(dma(2, 2, 2)),
            *twice(dma(2, 2, DEVICES)), *twice(dma(DEVICES)),
        ],
        compiler_params=pltpu.CompilerParams(
            dimension_semantics=("arbitrary", "arbitrary"), vmem_limit_bytes=67_000_000,
            collective_id=0, has_side_effects=True),
        cost_estimate=pl.CostEstimate(flops=flops, bytes_accessed=50_000_000, transcendentals=tokens * seq_len * 8),
        name="block",
    )(x, dy, pos, w_q, w_k, w_v, w_o, *gains)


def widen_kernel(ga_ref, gb_ref, small_ref, out_in, gi_in, wq_ref, wk_ref, wv_ref, wo_ref, dgin_ref, dqn_ref, dkn_ref, out_ref, gi_ref):
    @pl.when(pl.program_id(0) == 0)
    def _():
        lanes = small_ref.shape[1]
        rows = dgin_ref.shape[1] // lanes
        for row in range(rows):
            dgin_ref[:, row * lanes:(row + 1) * lanes] = small_ref[row:row + 1]
        dqn_ref[...] = small_ref[rows:rows + 1]
        dkn_ref[...] = small_ref[rows + 1:rows + 2]

    q_cols, head_dim = wq_ref.shape[1], wk_ref.shape[1]
    wo_ref[...] = ga_ref[0].astype(F32)
    wq_ref[...] = gb_ref[0, :, :q_cols].astype(F32)
    wk_ref[...] = gb_ref[0, :, q_cols:q_cols + head_dim].astype(F32)
    wv_ref[...] = gb_ref[0, :, q_cols + head_dim:].astype(F32)
    out_ref[...] = out_in[...]
    gi_ref[...] = gi_in[...]


def widen_call(ga, gb, small, out, gi):
    groups, q_cols, model = ga.shape
    width = gb.shape[2]
    head_dim = (width - q_cols) // 2
    parts = 2
    batch, piece, _ = out.shape
    f32 = lambda *shape: jax.ShapeDtypeStruct(shape, F32)
    across = lambda i: (i % parts, i // parts)
    fixed = lambda i: (0, 0)
    act = pl.BlockSpec((batch // (groups * parts), piece, model), lambda i: (i, 0, 0))
    return pl.pallas_call(
        widen_kernel,
        grid=(groups * parts,),
        in_specs=[pl.BlockSpec((1, q_cols // parts, model), lambda i: (i // parts, i % parts, 0)),
                  pl.BlockSpec((1, model // parts, width), lambda i: (i // parts, i % parts, 0)),
                  pl.BlockSpec(small.shape, fixed), act, act],
        out_specs=[pl.BlockSpec((model // parts, q_cols), across), pl.BlockSpec((model // parts, head_dim), across),
                   pl.BlockSpec((model // parts, head_dim), across), pl.BlockSpec((q_cols // parts, model), lambda i: (i, 0))]
        + [pl.BlockSpec((1, n), fixed) for n in (model, head_dim, head_dim)] + [act, act],
        out_shape=[f32(model, groups * q_cols), f32(model, groups * head_dim), f32(model, groups * head_dim),
                   f32(groups * q_cols, model), f32(1, model), f32(1, head_dim), f32(1, head_dim),
                   jax.ShapeDtypeStruct(out.shape, out.dtype), jax.ShapeDtypeStruct(gi.shape, gi.dtype)],
        compiler_params=pltpu.CompilerParams(dimension_semantics=("arbitrary",)),
        name="widen",
    )(ga, gb, small, out, gi)


def solution(mesh):
    seq_spec = P(None, 'sp', None)
    replicated = P()

    def shard_body(hidden_in, grad_out, positions, w_q, w_k, w_v, w_o, g_in, q_norm, k_norm):
        batch, seq_dev, model_dim = hidden_in.shape
        head_dim = q_norm.shape[0]
        exponents = jnp.arange(0, head_dim, 2).astype(F32) / head_dim
        inv_freq = jnp.power(ROPE_THETA, -exponents)
        gains = (g_in[None], q_norm[None], k_norm[None], jnp.concatenate([inv_freq, inv_freq])[None])
        pos = jnp.broadcast_to(jnp.pad(positions.astype(F32), ((0, 0), (0, head_dim - seq_dev)))[:, None, :], (batch, 8, head_dim))
        hidden_out, grad_in, ga, gb, _, _, small = block_call(hidden_in, grad_out, pos, gains, w_q, w_k, w_v, w_o, head_dim)
        grad_wq, grad_wk, grad_wv, grad_wo, dgin, dqn, dkn, hidden_out, grad_in = widen_call(ga, gb, small, hidden_out, grad_in)
        return hidden_out, grad_in, grad_wq, grad_wk, grad_wv, grad_wo, dgin[0], dqn[0], dkn[0]

    return jax.shard_map(shard_body, mesh=mesh,
                         in_specs=(seq_spec, seq_spec, P(None, 'sp'), replicated, replicated, replicated, replicated, replicated, replicated, replicated),
                         out_specs=(seq_spec, seq_spec, replicated, replicated, replicated, replicated, replicated, replicated, replicated),
                         check_vma=False)
```
